32 devices in a mesh: gx: 4 (over x, core), gy: 4 (over z), gz: 2 (over y).
Axes of the slice: x: 2, y: 2, z: 4, core: 2. Of those that a mesh axis runs over, the one named last changes fastest.
Arguments:
- right_side: float32 [16, 16, 8, 4, 256], P('gx', 'gy', 'gz'), may hold values from -80 to 80
- bond_blocks: float32 [13, 4, 4, 16, 16, 8], P(None, None, None, 'gx', 'gy', 'gz'), may hold values from -0.012 to 0.012
- bond_open: int32 [13, 16, 16, 8], P(None, 'gx', 'gy', 'gz'), may hold values 0 or 1
- onsite_blocks: float32 [4, 4, 16, 16, 8], P(None, None, 'gx', 'gy', 'gz'), may hold values from -0.012 to 0.012
- orbital_levels: float32 [4, 16, 16, 8], P(None, 'gx', 'gy', 'gz'), may hold values from 1.3 to 2.6
- column_shift: float32 [256], replicated, may hold values from 0.05 to 1
Outputs:
- solution: float32 [16, 16, 8, 4, 256], P('gx', 'gy', 'gz')
- residual: float32 [16, 16, 8, 4, 256], P('gx', 'gy', 'gz')
The draws below stay inside these ranges and needn't reach their ends.
All inputs are finite; a program needn't handle non-finite values. No bound on the sum of `bond_open` on one device may be relied on, other than what follows from the above.
Results may differ from the reference program's by a relative error of at most 0.0003.
Values sent between devices are 32-bit elements; how exact they have to be, the bound alone decides.
A program may use at most 192 MiB of HBM per device.

```python
import math
import jax
import jax.numpy as jnp
from jax import lax

ORB = 4
COLS = 256
BONDS = 13
ITERS = 3
NX = 16
NY = 16
NZ = 8


def draw_right_side(key, part):
    subkeys = jax.random.split(key, 3)
    full_shape = (NX, NY, NZ, ORB, COLS)
    along_x = jnp.arange(NX, dtype=jnp.float32) / NX
    along_y = jnp.arange(NY, dtype=jnp.float32) / NY
    along_z = jnp.arange(NZ, dtype=jnp.float32) / NZ
    position_ramp = jnp.exp(0.37 * (along_x[:, None, None] + along_y[None, :, None] + along_z[None, None, :]))
    atom_scale = jnp.exp(jax.random.uniform(subkeys[1], (NX, NY, NZ, ORB, 1), jnp.float32, math.log(0.3), math.log(3.0)))
    values = jnp.clip(jax.random.normal(subkeys[0], full_shape, jnp.float32), -4.0, 4.0)
    column_scale = jnp.exp(jax.random.uniform(subkeys[2], (COLS,), jnp.float32, math.log(0.5), math.log(5.0)))
    return (0.3 * values * atom_scale * column_scale * position_ramp[:, :, :, None, None]).astype(jnp.float32)


def set_ends(array, rng, least, largest):
    shape = array.shape
    place = [jax.random.randint(jax.random.fold_in(rng, axis), (), 0, shape[axis]) for axis in range(len(shape))]
    array = array.at[tuple(place)].set(least)
    longest = shape.index(max(shape))
    place[longest] = (place[longest] + 1) % shape[longest]
    return array.at[tuple(place)].set(largest)


def level_of(key, extent, pieces, smallest, high):
    factor_of, own = 1.0, jax.random.fold_in(key, 6)
    for axis_at, shards_of in pieces:
        steps = jnp.exp(jax.random.uniform(jax.random.fold_in(own, axis_at), (shards_of,), jnp.float32, smallest / len(pieces), high / len(pieces)))
        factor_of = factor_of * jnp.repeat(steps, extent[axis_at] // shards_of).reshape([-1 if axis == axis_at else 1 for axis in range(len(extent))])
    return factor_of


def setup_inputs(seed: int = 0) -> dict:
    keys = jax.random.split(jax.random.key(seed), 7)
    return {
        "right_side": draw_right_side(jax.random.fold_in(keys[6], 71), 0),
        "bond_blocks": jnp.clip(jax.random.uniform(keys[1], (BONDS, ORB, ORB, NX, NY, NZ), jnp.float32, -0.012, 0.012) * level_of(keys[1], (BONDS, ORB, ORB, NX, NY, NZ), ((3, 4), (4, 4), (5, 2)), -0.4, 0.0), -0.012, 0.012),
        "bond_open": set_ends((jax.random.randint(keys[2], (BONDS, NX, NY, NZ), 0, 4) < 3).astype(jnp.int32), jax.random.fold_in(keys[2], 1), 0, 1),
        "onsite_blocks": jnp.clip(jax.random.uniform(keys[3], (ORB, ORB, NX, NY, NZ), jnp.float32, -0.012, 0.012) * level_of(keys[3], (ORB, ORB, NX, NY, NZ), ((2, 4), (3, 4), (4, 2)), -0.4, 0.0), -0.012, 0.012),
        "orbital_levels": jnp.clip(jnp.exp(math.log(2.6) - 0.6931472 * jax.random.uniform(keys[4], (ORB, NX, NY, NZ), jnp.float32) ** level_of(keys[4], (ORB, NX, NY, NZ), ((1, 4), (2, 4), (3, 2)), -0.2, 0.2)), 1.3, 2.6),
        "column_shift": jnp.clip(jnp.exp(jax.random.uniform(keys[5], (COLS,), jnp.float32, math.log(0.05), math.log(1.0))), 0.05, 1.0),
    }


half_offsets = [(first, second, third) for first in (-1, 0, 1) for second in (-1, 0, 1) for third in (-1, 0, 1) if (first, second, third) > (0, 0, 0)]


def hop(blocks, vector):
    return jnp.einsum('ijxyz,xyzjc->xyzic', blocks.astype(jnp.float32), vector.astype(jnp.float32), precision=lax.Precision.HIGHEST)


def operate(vector, coupled, onsite_sym, atom_levels, column_shift):
    result = hop(onsite_sym, vector) + (atom_levels[..., None] + column_shift) * vector
    for bond_index, offset in enumerate(half_offsets):
        ahead = jnp.roll(vector, (-offset[0], -offset[1], -offset[2]), axis=(0, 1, 2))
        behind = jnp.roll(vector, offset, axis=(0, 1, 2))
        mirrored = jnp.roll(coupled[bond_index], offset, axis=(2, 3, 4))
        result = result + hop(coupled[bond_index], ahead) + hop(jnp.swapaxes(mirrored, 0, 1), behind)
    return result


def reference(right_side, bond_blocks, bond_open, onsite_blocks, orbital_levels, column_shift):
    coupled = bond_blocks * bond_open[:, None, None].astype(jnp.float32)
    onsite_sym = 0.5 * (onsite_blocks + jnp.swapaxes(onsite_blocks, 0, 1))
    atom_levels = jnp.transpose(orbital_levels, (1, 2, 3, 0))
    solution = jnp.zeros_like(right_side)
    residual = right_side
    direction = right_side
    norm_now = jnp.sum(residual * residual, axis=(0, 1, 2, 3))
    for iteration in range(ITERS):
        image = operate(direction, coupled, onsite_sym, atom_levels, column_shift)
        alpha = norm_now / jnp.sum(direction * image, axis=(0, 1, 2, 3))
        solution = solution + alpha * direction
        residual = residual - alpha * image
        norm_next = jnp.sum(residual * residual, axis=(0, 1, 2, 3))
        direction = residual + (norm_next / norm_now) * direction
        norm_now = norm_next
    return (solution, residual)
```

```python
import functools
import itertools

import jax
import jax.numpy as jnp
from jax import lax
from jax.experimental import pallas as pl
from jax.experimental.pallas import tpu as pltpu
from jax.sharding import PartitionSpec as P

ITERS = 3
LANES = 128
ROWS = 8
AXES = ("gx", "gy", "gz")
MESH = pl.DeviceIdType.MESH

bonds = [o for o in itertools.product((-1, 0, 1), repeat=3) if o > (0, 0, 0)]
NB = len(bonds)
ahead_runs = [(1, 3), (10, 3)]
behind_runs = [(4, 3)]
assert all(bonds[k][1] == 1 for at, n in ahead_runs for k in range(at, at + n))
assert all(bonds[k][1] == -1 for at, n in behind_runs for k in range(at, at + n))


class Plan:
    def __init__(self, block, orb, cols, peers):
        self.X, self.Y, self.Z = block
        self.O, self.cols = orb, cols
        self.nx, self.ny, self.nz = peers
        self.S = self.nx * self.nz
        self.l = self.X * self.Z
        self.L = self.S * self.l
        self.G = LANES // self.l
        self.Cw = cols // self.S
        self.YO = self.Y * orb
        self.HL = self.YO * self.l
        self.HT = self.HL // LANES
        self.H = cols // LANES
        self.JT = LANES // (self.Y * self.l)
        self.tiles = orb * orb // self.JT
        self.CR = (NB + 1) * self.tiles
        self.OC = orb * self.Cw
        assert self.tiles == ROWS and self.S % self.G == 0 and self.Cw % ROWS == 0


def kernel(plan, rs_hbm, bb_hbm, open_ref, onsite_ref, level_ref, shift_ref, sol_hbm, res_hbm,
           RS, BB, T, RB, CS, CR, M, MB, V, VS, SB, YB, MG, TG, WQ, OS,
           in_sem, a_s, a_r, c_s, c_r, hv_s, hv_r, hm_s, hm_r, th_s, th_r, y_s, y_r, mo_s, mo_r, w_s, w_r):
    p = plan
    X, Y, Z, O, S, L, l, G, Cw, H, OC = p.X, p.Y, p.Z, p.O, p.S, p.L, p.l, p.G, p.Cw, p.H, p.OC
    f32 = jnp.float32
    ax, ay, az = (lax.axis_index(name) for name in AXES)
    me = ax * p.nz + az
    pending = []

    def mate(r):
        d = lax.rem(me + r, S)
        return d, (lax.div(d, p.nz), ay, lax.rem(d, p.nz))

    def source(r):
        return lax.rem(me + (S - r), S)

    def along(r):
        return (ax, lax.rem(ay + (r % p.ny), p.ny), az)

    def send(src, dst, ssem, rsem, device):
        copy = pltpu.make_async_remote_copy(
            src_ref=src, dst_ref=dst, send_sem=ssem, recv_sem=rsem, device_id=device, device_id_type=MESH
        )
        copy.start()
        pending.append(copy)
        return copy

    loads = []
    for x in range(X):
        for y in range(Y):
            n = Z * H * O
            copy = pltpu.make_async_copy(
                rs_hbm.at[x, y], RS.at[pl.ds((y * X + x) * n, n)], in_sem.at[x * Y + y])
            copy.start()
            loads.append(copy)
    bond_load = pltpu.make_async_copy(bb_hbm, BB, in_sem.at[X * Y])
    bond_load.start()

    barrier = pltpu.get_barrier_semaphore()
    for r in range(1, S):
        pl.semaphore_signal(barrier, inc=1, device_id=mate(r)[1], device_id_type=MESH)
    for r in range(1, p.ny):
        pl.semaphore_signal(barrier, inc=1, device_id=along(r), device_id_type=MESH)

    lane = lax.broadcasted_iota(jnp.int32, (1, L), 1)
    lane128 = lax.broadcasted_iota(jnp.int32, (1, LANES), 1)

    def roll(v, by):
        by = by % v.shape[1]
        return v if by == 0 else pltpu.roll(v, by, 1)

    zl = lane & (Z - 1)
    xl = (lane // Z) & (X - 1)
    gz = (lane // l) & (p.nz - 1)

    def shift_z(v, s):
        if s == 0:
            return v
        edge, outer = (zl == Z - 1, gz == p.nz - 1) if s > 0 else (zl == 0, gz == 0)
        far = l - (Z - 1)
        out = jnp.where(edge, roll(v, -s * far), roll(v, -s))
        return jnp.where(edge & outer, roll(v, -s * (far - p.nz * l)), out)

    def shift_x(v, s):
        if s == 0:
            return v
        edge = (xl == X - 1) if s > 0 else (xl == 0)
        far = p.nz * l - (X - 1) * Z
        return jnp.where(edge, roll(v, -s * far), roll(v, -s * Z))

    block_of = lane128 // l

    def butterfly(arrays):
        arrays = list(arrays)
        m = 1
        while m < G:
            low = (block_of & m) == 0
            for a in range(G):
                if a & m == 0:
                    b = a | m
                    first, second = arrays[a], arrays[b]
                    arrays[a] = jnp.where(low, first, roll(second, m * l))
                    arrays[b] = jnp.where(low, roll(first, -m * l), second)
            m *= 2
        return arrays

    for copy in loads:
        copy.wait()
    step = H * O
    for h in range(H):
        rows = jnp.concatenate([
            RS[pl.ds(y * X * Z * step + h * O + o, l, stride=step), :] for y in range(Y) for o in range(O)
        ], axis=0)
        T[h * LANES:(h + 1) * LANES, :] = jnp.transpose(rows)
    pl.semaphore_wait(barrier, S - 1 + p.ny - 1)
    field_copies = []
    for r in range(1, S):
        d, device = mate(r)
        field_copies.append(send(
            T.at[pl.ds(pl.multiple_of(d * Cw, ROWS), Cw)], RB.at[me], a_s.at[r - 1], a_r.at[r - 1], device))
    RB[me] = T[pl.ds(pl.multiple_of(me * Cw, ROWS), Cw), :]

    def spread_z(block):
        n = block.shape[0]
        out = jnp.zeros((n, LANES), f32)
        for z in range(Z):
            out = jnp.where((lane128 & (Z - 1)) == z, block[:, z:z + 1], out)
        row = lax.broadcasted_iota(jnp.int32, (n, LANES), 0)
        col = lax.broadcasted_iota(jnp.int32, (n, LANES), 1)
        x_row, y_row = (row // Y) & (X - 1), row & (Y - 1)
        x_col, y_col = (col // Z) & (X - 1), (col // l) & (Y - 1)
        return jnp.where((x_row == x_col) & (y_row == y_col), out, 0.0)

    onsite = spread_z(onsite_ref[...])
    level = spread_z(level_ref[...])
    XY = X * Y
    pair = [jnp.sum(onsite[n * XY:(n + 1) * XY], axis=0, keepdims=True) for n in range(O * O)]
    diagonal = [jnp.sum(level[n * XY:(n + 1) * XY], axis=0, keepdims=True) for n in range(O)]
    j_low = lane128 // (Y * l)
    for i in range(O):
        for jh in range(O // p.JT):
            line = jnp.zeros((1, LANES), f32)
            for jl in range(p.JT):
                j = jh * p.JT + jl
                term = 0.5 * (pair[i * O + j] + pair[j * O + i])
                if i == j:
                    term = term + diagonal[i]
                line = jnp.where(j_low == jl, term, line)
            row = NB * ROWS + i * (O // p.JT) + jh
            CS[row:row + 1, :] = line

    bond_load.wait()
    is_open = open_ref[...].astype(f32)
    is_open = jnp.concatenate([is_open] * p.JT, axis=0)
    x_of, y_of = (lane128 // (Y * Z)) & (X - 1), (lane128 // Z) & (Y - 1)
    x_to, y_to = (lane128 // Z) & (X - 1), (lane128 // (X * Z)) & (Y - 1)
    source_lane = (lane128 & (Z - 1)) + x_to * (Y * Z) + y_to * Z + j_low * (Y * l)
    gaps = sorted({(x * Y * Z + y * Z) - (y * X * Z + x * Z) for x in range(X) for y in range(Y)})
    for t in range(p.tiles):
        block = BB[t * LANES:(t + 1) * LANES, :] * is_open
        block = jnp.concatenate([block, jnp.zeros((LANES, LANES - NB), f32)], axis=1)
        block = jnp.transpose(block)[0:2 * ROWS, :]
        out = block
        for gap in gaps:
            if gap:
                out = jnp.where(source_lane - lane128 == gap, roll(block, -gap), out)
        CS[pl.ds(t, NB, stride=ROWS), :] = out[0:NB, :]
    coef_copies = []
    for r in range(1, S):
        d, device = mate(r)
        coef_copies.append(send(CS, CR.at[me], c_s.at[r - 1], c_r.at[r - 1], device))
    CR[me] = CS[...]

    def halo_field(m):
        return [
            send(V.at[m, 1], V.at[m, Y + 1], hv_s.at[m, 0], hv_r.at[m, 0], along(-1)),
            send(V.at[m, Y], V.at[m, 0], hv_s.at[m, 1], hv_r.at[m, 1], along(1)),
        ]

    def arrived(copies):
        for copy in copies:
            copy.wait_recv()

    arrived(field_copies)
    for t in range(p.HT):
        for first in range(0, S, G):
            blocks = butterfly([RB[first + n, :, t * LANES:(t + 1) * LANES] for n in range(G)])
            at = first // G * LANES
            for n in range(G):
                y, o = divmod(t * G + n, O)
                V[0, y + 1, o * Cw:(o + 1) * Cw, at:at + LANES] = blocks[n]
    halo = halo_field(0)

    arrived(coef_copies)
    for first in range(0, S, G):
        blocks = butterfly([CR[first + n] for n in range(G)])
        at = first // G * LANES
        for n in range(G):
            jl, y = divmod(n, Y)
            M[jl, y + 1, :, at:at + LANES] = blocks[n]
    coef_halo = []
    for n, (run, y_from, y_to_slot, way) in enumerate(
            [(run, Y, 0, 1) for run in ahead_runs] + [(run, 1, Y + 1, -1) for run in behind_runs]):
        rows = pl.ds(run[0] * ROWS, run[1] * ROWS)
        coef_halo.append(send(
            M.at[:, y_from, rows], M.at[:, y_to_slot, rows], hm_s.at[n], hm_r.at[n], along(way)))

    HALFJ = O // p.JT
    diag_rows = [(i % p.JT, NB * ROWS + i * HALFJ + i // p.JT) for i in range(O)]
    part = jnp.zeros((1, L), f32)
    for y in range(1, Y + 1):
        for jl, row in diag_rows:
            part = part + M[jl, y, row:row + 1, :]
    TG[ay] = jnp.broadcast_to(jnp.sum(part, axis=1, keepdims=True), (ROWS, LANES))
    theta_copies = [
        send(TG.at[ay], TG.at[ay], th_s.at[r - 1], th_r.at[r - 1], along(r)) for r in range(1, p.ny)]

    def mirror(k, y):
        o = bonds[k]
        for jl in range(p.JT):
            block = M[jl, y + 1 - o[1], k * ROWS:(k + 1) * ROWS, :]
            MB[k, jl, y] = shift_x(shift_z(block, -o[2]), -o[0])

    def inside(y):
        return 0 <= y < Y

    for k in range(NB):
        for y in range(Y):
            if inside(y - bonds[k][1]):
                mirror(k, y)

    def place(sx, sz):
        n = (sx + 1) * 3 + sz + 1
        return n - (n > 4)

    def spread_field(m, slot):
        for o in range(O):
            rows = slice(o * Cw, (o + 1) * Cw)
            base = V[m, slot, rows, :]
            for sz in (-1, 0, 1):
                turned = shift_z(base, sz)
                for sx in (-1, 0, 1):
                    if (sx, sz) != (0, 0):
                        VS[place(sx, sz), slot, rows, :] = shift_x(turned, sx)

    def add_bonds(acc, m, y, steps):
        for k, o in enumerate(bonds):
            for sign in (1, -1):
                if sign * o[1] not in steps:
                    continue
                slot = y + 1 + sign * o[1]
                sx, sz = sign * o[0], sign * o[2]
                for j in range(O):
                    rows = slice(j * Cw, (j + 1) * Cw)
                    v = V[m, slot, rows, :] if (sx, sz) == (0, 0) else VS[place(sx, sz), slot, rows, :]
                    for i in range(O):
                        if sign > 0:
                            row = k * ROWS + i * HALFJ + j // p.JT
                            c = M[j % p.JT, y + 1, row:row + 1, :]
                        else:
                            row = j * HALFJ + i // p.JT
                            c = MB[k, i % p.JT, y, row:row + 1, :]
                        acc[i] = acc[i] + c * v

    def add_onsite(acc, m, y, theta):
        for j in range(O):
            v = V[m, y + 1, j * Cw:(j + 1) * Cw, :]
            for i in range(O):
                row = NB * ROWS + i * HALFJ + j // p.JT
                c = M[j % p.JT, y + 1, row:row + 1, :]
                if i == j:
                    c = c - theta
                acc[i] = acc[i] + c * v

    def put(acc, m, y):
        for i in range(O):
            V[m, y + 1, i * Cw:(i + 1) * Cw, :] = acc[i]

    def take(m, y):
        return [V[m, y + 1, i * Cw:(i + 1) * Cw, :] for i in range(O)]

    def zeros():
        return [jnp.zeros((Cw, L), f32) for _ in range(O)]

    def moment(a, b):
        total = jnp.zeros((Cw, L), f32)
        for y in range(Y):
            for i in range(O):
                rows = slice(i * Cw, (i + 1) * Cw)
                total = total + V[a, y + 1, rows, :] * V[b, y + 1, rows, :]
        return jnp.sum(total, axis=1, keepdims=True)

    moments = []
    home_copies = []

    def go_home(m):
        for t in range(p.HT):
            for first in range(0, S, G):
                at = first // G * LANES
                blocks = []
                for n in range(G):
                    y, o = divmod(t * G + n, O)
                    blocks.append(V[m, y + 1, o * Cw:(o + 1) * Cw, at:at + LANES])
                blocks = butterfly(blocks)
                for n in range(G):
                    SB[m - 1, first + n, :, t * LANES:(t + 1) * LANES] = blocks[n]
        mine = pl.ds(pl.multiple_of(me * Cw, ROWS), Cw)
        for r in range(1, S):
            d, device = mate(r)
            home_copies.append(send(
                SB.at[m - 1, d], YB.at[m - 1, mine], y_s.at[m - 1, r - 1], y_r.at[m - 1, r - 1], device))
        YB[m - 1, mine] = SB[m - 1, me]

    theta = None
    for m in range(ITERS):
        for slot in range(1, Y + 1):
            spread_field(m, slot)
        for y in range(Y):
            acc = zeros()
            add_bonds(acc, m, y, [s for s in (-1, 0, 1) if inside(y + s)])
            put(acc, m + 1, y)
        if m == 0:
            moments.append(moment(0, 0))
            arrived(theta_copies)
            theta = TG[0][0:1, 0:1]
            for n in range(1, p.ny):
                theta = theta + TG[n][0:1, 0:1]
            theta = theta * (1.0 / (p.ny * Y * L * O))
        arrived(halo)
        if m == 0:
            arrived(coef_halo)
            for k in range(NB):
                for y in range(Y):
                    if not inside(y - bonds[k][1]):
                        mirror(k, y)
        for slot, y, s in ((0, 0, -1), (Y + 1, Y - 1, 1)):
            spread_field(m, slot)
            acc = take(m + 1, y)
            add_bonds(acc, m, y, [s])
            add_onsite(acc, m, y, theta)
            put(acc, m + 1, y)
        if m + 1 < ITERS:
            halo = halo_field(m + 1)
        for y in range(1, Y - 1):
            acc = take(m + 1, y)
            add_onsite(acc, m, y, theta)
            put(acc, m + 1, y)
        go_home(m + 1)
        moments.append(moment(m, m + 1))
        if m + 1 < ITERS:
            moments.append(moment(m + 1, m + 1))

    table = jnp.zeros((Cw, LANES), f32)
    for n, value in enumerate(moments):
        table = jnp.where(lane128 == n, value, table)
    if Cw < LANES:
        table = jnp.concatenate([table, jnp.zeros((LANES - Cw, LANES), f32)], axis=0)
    MG[ay] = jnp.transpose(table)[0:ROWS, :]
    arrived([send(MG.at[ay], MG.at[ay], mo_s.at[r - 1], mo_r.at[r - 1], along(r)) for r in range(1, p.ny)])
    total = MG[0]
    for n in range(1, p.ny):
        total = total + MG[n]
    m_of = [total[n:n + 1, :] for n in range(2 * ITERS)]
    shift = jnp.zeros((1, LANES), f32)
    for d in range(S):
        h, at = divmod(d * Cw, LANES)
        shift = jnp.where(me == d, roll(shift_ref[:, h * LANES:(h + 1) * LANES], -at), shift)
    shift = shift + theta

    def inner(u, v):
        out = None
        for a, first in enumerate(u):
            for b, second in enumerate(v):
                term = first * second * m_of[a + b]
                out = term if out is None else out + term
        return out

    def plus(u, v, factor):
        n = max(len(u), len(v))
        out = []
        for a in range(n):
            if a < len(v):
                term = factor * v[a]
                out.append(u[a] + term if a < len(u) else term)
            else:
                out.append(u[a])
        return out

    one = jnp.ones((1, LANES), f32)
    answer, residual, direction, norm = [], [one], [one], m_of[0]
    for turn in range(ITERS):
        image = [shift * direction[0]]
        for a in range(1, len(direction)):
            image.append(direction[a - 1] + shift * direction[a])
        image.append(direction[-1])
        alpha = norm / inner(direction, image)
        answer = plus(answer, direction, alpha)
        residual = plus(residual, image, -alpha)
        if turn + 1 < ITERS:
            fresh = inner(residual, residual)
            direction = plus(residual, direction, fresh / norm)
            norm = fresh
    factors = answer + residual
    WQ[me] = jnp.concatenate(factors + [jnp.zeros((ROWS - len(factors), LANES), f32)], axis=0)
    factor_copies = []
    for r in range(1, S):
        d, device = mate(r)
        factor_copies.append(send(WQ.at[me], WQ.at[me], w_s.at[r - 1], w_r.at[r - 1], device))
    arrived(factor_copies)
    arrived(home_copies)

    outs = []
    for h in range(H):
        lines = jnp.zeros((ROWS, LANES), f32)
        per = LANES // Cw
        for n in range(per):
            d = h * per + n
            lines = jnp.where(lane128 // Cw == n, roll(WQ[d], n * Cw), lines)
        column = jnp.transpose(lines)
        rows = slice(h * LANES, (h + 1) * LANES)
        basis = [T[rows, :]] + [YB[n, rows, :] for n in range(ITERS)]
        for which, hbm in ((0, sol_hbm), (1, res_hbm)):
            at = which * ITERS
            field = column[:, at:at + 1] * basis[0]
            for n in range(1, ITERS + which):
                field = field + column[:, at + n:at + n + 1] * basis[n]
            field = jnp.transpose(field)
            for y in range(Y):
                for o in range(O):
                    n = (y * O + o) * l
                    OS[which, pl.ds(y * X * Z * step + h * O + o, l, stride=step), :] = field[n:n + l, :]
    for which, hbm in ((0, sol_hbm), (1, res_hbm)):
        for x in range(X):
            for y in range(Y):
                n = Z * H * O
                copy = pltpu.make_async_copy(
                    OS.at[which, pl.ds((y * X + x) * n, n)], hbm.at[x, y], in_sem.at[(which * X + x) * Y + y])
                copy.start()
                outs.append(copy)
    for copy in outs:
        copy.wait()
    for copy in pending:
        copy.wait_send()


def per_device(peers, right_side, bond_blocks, bond_open, onsite_blocks, orbital_levels, column_shift):
    block, orb, cols = right_side.shape[:3], right_side.shape[3], right_side.shape[4]
    p = Plan(block, orb, cols, peers)
    X, Y, Z, O, S, L, H = p.X, p.Y, p.Z, p.O, p.S, p.L, p.H
    f32 = jnp.float32
    right = right_side.reshape(X, Y, Z, O, H, LANES).transpose(0, 1, 2, 4, 3, 5).reshape(X, Y, Z * H * O, LANES)
    blocks = jnp.transpose(bond_blocks, (1, 2, 3, 4, 5, 0)).reshape(O * O * X * Y * Z, NB)
    opened = jnp.transpose(bond_open, (1, 2, 3, 0)).reshape(X * Y * Z, NB)
    onsite = onsite_blocks.reshape(O * O * X * Y, Z)
    levels = orbital_levels.reshape(O * X * Y, Z)
    dma = pltpu.SemaphoreType.DMA
    vmem, anywhere = pl.BlockSpec(memory_space=pltpu.VMEM), pl.BlockSpec(memory_space=pl.ANY)

    def scratch(*shape):
        return pltpu.VMEM(shape, f32)

    outs = pl.pallas_call(
        functools.partial(kernel, p),
        out_shape=(jax.ShapeDtypeStruct(right.shape, f32),) * 2,
        in_specs=[anywhere, anywhere] + [vmem] * 4,
        out_specs=(anywhere, anywhere),
        scratch_shapes=[
            scratch(X * Y * Z * H * O, LANES),
            scratch(O * O * X * Y * Z, NB),
            scratch(cols, p.HL),
            scratch(S, p.Cw, p.HL),
            scratch(p.CR, LANES),
            scratch(S, p.CR, LANES),
            scratch(p.JT, Y + 2, p.CR, L),
            scratch(NB, p.JT, Y, ROWS, L),
            scratch(ITERS + 1, Y + 2, p.OC, L),
            scratch(8, Y + 2, p.OC, L),
            scratch(ITERS, S, p.Cw, p.HL),
            scratch(ITERS, cols, p.HL),
            scratch(p.ny, ROWS, LANES),
            scratch(p.ny, ROWS, LANES),
            scratch(S, ROWS, LANES),
            scratch(2, X * Y * Z * H * O, LANES),
            dma((2 * X * Y,)),
            dma((S - 1,)), dma((S - 1,)), dma((S - 1,)), dma((S - 1,)),
            dma((ITERS, 2)), dma((ITERS, 2)), dma((3,)), dma((3,)),
            dma((p.ny - 1,)), dma((p.ny - 1,)),
            dma((ITERS, S - 1)), dma((ITERS, S - 1)),
            dma((p.ny - 1,)), dma((p.ny - 1,)), dma((S - 1,)), dma((S - 1,)),
        ],
        compiler_params=pltpu.CompilerParams(
            collective_id=0, has_side_effects=True, vmem_limit_bytes=60 * 1024 * 1024
        ),
    )(right, blocks, opened, onsite, levels, column_shift[None])

    def back(v):
        return v.reshape(X, Y, Z, H, O, LANES).transpose(0, 1, 2, 4, 3, 5).reshape(right_side.shape)

    return back(outs[0]), back(outs[1])


def solution(mesh):
    field = P("gx", "gy", "gz", None, None)
    placed = (
        field,
        P(None, None, None, "gx", "gy", "gz"),
        P(None, "gx", "gy", "gz"),
        P(None, None, "gx", "gy", "gz"),
        P(None, "gx", "gy", "gz"),
        P(),
    )
    return jax.shard_map(
        functools.partial(per_device, tuple(mesh.shape[name] for name in AXES)),
        mesh=mesh,
        in_specs=placed,
        out_specs=(field, field),
        check_vma=False,
    )
```

```python
import functools
import itertools

import jax
import jax.numpy as jnp
from jax import lax
from jax.experimental import pallas as pl
from jax.experimental.pallas import tpu as pltpu
from jax.sharding import PartitionSpec as P

ITERS = 3
LANES = 128
ROWS = 8
AXES = ("gx", "gy", "gz")
MESH = pl.DeviceIdType.MESH

bonds = [o for o in itertools.product((-1, 0, 1), repeat=3) if o > (0, 0, 0)]
NB = len(bonds)
ahead_runs = [(1, 3), (10, 3)]
behind_runs = [(4, 3)]
assert all(bonds[k][1] == 1 for at, n in ahead_runs for k in range(at, at + n))
assert all(bonds[k][1] == -1 for at, n in behind_runs for k in range(at, at + n))


class Plan:
    def __init__(self, block, orb, cols, peers):
        self.X, self.Y, self.Z = block
        self.O, self.cols = orb, cols
        self.nx, self.ny, self.nz = peers
        self.S = self.nx * self.nz
        self.l = self.X * self.Z
        self.L = self.S * self.l
        self.G = LANES // self.l
        self.Cw = cols // self.S
        self.YO = self.Y * orb
        self.HL = self.YO * self.l
        self.HT = self.HL // LANES
        self.H = cols // LANES
        self.JT = LANES // (self.Y * self.l)
        self.tiles = orb * orb // self.JT
        self.CR = (NB + 1) * self.tiles
        self.OC = orb * self.Cw
        assert self.tiles == ROWS and self.S % self.G == 0 and self.Cw % ROWS == 0


def kernel(plan, rs_hbm, bb_hbm, open_hbm, onsite_hbm, level_hbm, shift_hbm, sol_hbm, res_hbm,
           RS, BB, open_ref, onsite_ref, level_ref, shift_ref, PM, LH, T, RB, CS, CR, M, MB, V, VS, SB, YB, MG, TG, WQ, OS,
           in_sem, a_s, a_r, c_s, c_r, hv_s, hv_r, hm_s, hm_r, th_s, th_r, y_s, y_r, mo_s, mo_r, w_s, w_r):
    p = plan
    X, Y, Z, O, S, L, l, G, Cw, H, OC = p.X, p.Y, p.Z, p.O, p.S, p.L, p.l, p.G, p.Cw, p.H, p.OC
    f32 = jnp.float32
    ax, ay, az = (lax.axis_index(name) for name in AXES)
    me = ax * p.nz + az
    pending = []

    def mate(r):
        d = lax.rem(me + r, S)
        return d, (lax.div(d, p.nz), ay, lax.rem(d, p.nz))

    def source(r):
        return lax.rem(me + (S - r), S)

    def along(r):
        return (ax, lax.rem(ay + (r % p.ny), p.ny), az)

    def send(src, dst, ssem, rsem, device):
        copy = pltpu.make_async_remote_copy(
            src_ref=src, dst_ref=dst, send_sem=ssem, recv_sem=rsem, device_id=device, device_id_type=MESH
        )
        copy.start()
        pending.append(copy)
        return copy

    barrier = pltpu.get_barrier_semaphore()
    for r in range(1, S):
        pl.semaphore_signal(barrier, inc=1, device_id=mate(r)[1], device_id_type=MESH)
    for r in range(1, p.ny):
        pl.semaphore_signal(barrier, inc=1, device_id=along(r), device_id_type=MESH)

    loads = []
    for x in range(X):
        for y in range(Y):
            n = Z * H * O
            copy = pltpu.make_async_copy(
                rs_hbm.at[x, y], RS.at[pl.ds((y * X + x) * n, n)], in_sem.at[x * Y + y])
            copy.start()
            loads.append(copy)
    small_loads = []
    for n, (src, dst) in enumerate(((onsite_hbm, onsite_ref), (level_hbm, level_ref), (bb_hbm, BB),
                                    (open_hbm, open_ref), (shift_hbm, shift_ref))):
        copy = pltpu.make_async_copy(src, dst, in_sem.at[X * Y + n])
        copy.start()
        small_loads.append(copy)

    lane = lax.broadcasted_iota(jnp.int32, (1, L), 1)
    lane128 = lax.broadcasted_iota(jnp.int32, (1, LANES), 1)

    def roll(v, by):
        by = by % v.shape[1]
        return v if by == 0 else pltpu.roll(v, by, 1)

    zg = ((lane // l) & (p.nz - 1)) * Z + (lane & (Z - 1))
    xg = (lane // (l * p.nz)) * X + ((lane // Z) & (X - 1))
    row_of = lax.broadcasted_iota(jnp.int32, (L, L), 0)

    def place(sx, sz):
        n = (sx + 1) * 3 + sz + 1
        return n - (n > 4)

    def make_shifts():
        for sx in (-1, 0, 1):
            for sz in (-1, 0, 1):
                if (sx, sz) == (0, 0):
                    continue
                x_to, z_to = (xg + sx) & (p.nx * X - 1), (zg + sz) & (p.nz * Z - 1)
                from_lane = ((x_to // X) * p.nz + z_to // Z) * l + (x_to & (X - 1)) * Z + (z_to & (Z - 1))
                matrix = jnp.where(row_of == from_lane, 1.0, 0.0).astype(jnp.bfloat16)
                at = place(sx, sz) * L
                PM[0:L, at:at + L] = matrix
                PM[L:2 * L, at:at + L] = matrix

    def halves(v):
        high = v.astype(jnp.bfloat16)
        low = (v - high.astype(f32)).astype(jnp.bfloat16)
        return jnp.concatenate([high, low], axis=1)

    block_of = lane128 // l

    def butterfly(arrays):
        arrays = list(arrays)
        m = 1
        while m < G:
            low = (block_of & m) == 0
            for a in range(G):
                if a & m == 0:
                    b = a | m
                    first, second = arrays[a], arrays[b]
                    arrays[a] = jnp.where(low, first, roll(second, m * l))
                    arrays[b] = jnp.where(low, roll(first, -m * l), second)
            m *= 2
        return arrays

    for copy in loads:
        copy.wait()
    step = H * O
    for h in range(H):
        rows = jnp.concatenate([
            RS[pl.ds(y * X * Z * step + h * O + o, l, stride=step), :] for y in range(Y) for o in range(O)
        ], axis=0)
        T[h * LANES:(h + 1) * LANES, :] = jnp.transpose(rows)
    make_shifts()
    pl.semaphore_wait(barrier, S - 1 + p.ny - 1)
    field_copies = []
    for r in range(1, S):
        d, device = mate(r)
        field_copies.append(send(
            T.at[pl.ds(pl.multiple_of(d * Cw, ROWS), Cw)], RB.at[me], a_s.at[r - 1], a_r.at[r - 1], device))
    RB[me] = T[pl.ds(pl.multiple_of(me * Cw, ROWS), Cw), :]

    def spread_z(block):
        n = block.shape[0]
        out = jnp.zeros((n, LANES), f32)
        for z in range(Z):
            out = jnp.where((lane128 & (Z - 1)) == z, block[:, z:z + 1], out)
        row = lax.broadcasted_iota(jnp.int32, (n, LANES), 0)
        col = lax.broadcasted_iota(jnp.int32, (n, LANES), 1)
        x_row, y_row = (row // Y) & (X - 1), row & (Y - 1)
        x_col, y_col = (col // Z) & (X - 1), (col // l) & (Y - 1)
        return jnp.where((x_row == x_col) & (y_row == y_col), out, 0.0)

    for copy in small_loads[0:2]:
        copy.wait()
    onsite = spread_z(onsite_ref[...])
    level = spread_z(level_ref[...])
    XY = X * Y
    pair = [jnp.sum(onsite[n * XY:(n + 1) * XY], axis=0, keepdims=True) for n in range(O * O)]
    diagonal = [jnp.sum(level[n * XY:(n + 1) * XY], axis=0, keepdims=True) for n in range(O)]
    j_low = lane128 // (Y * l)
    for i in range(O):
        for jh in range(O // p.JT):
            line = jnp.zeros((1, LANES), f32)
            for jl in range(p.JT):
                j = jh * p.JT + jl
                term = 0.5 * (pair[i * O + j] + pair[j * O + i])
                if i == j:
                    term = term + diagonal[i]
                line = jnp.where(j_low == jl, term, line)
            row = NB * ROWS + i * (O // p.JT) + jh
            CS[row:row + 1, :] = line

    for copy in small_loads[2:]:
        copy.wait()
    is_open = open_ref[...].astype(f32)
    is_open = jnp.concatenate([is_open] * p.JT, axis=0)
    x_of, y_of = (lane128 // (Y * Z)) & (X - 1), (lane128 // Z) & (Y - 1)
    x_to, y_to = (lane128 // Z) & (X - 1), (lane128 // (X * Z)) & (Y - 1)
    source_lane = (lane128 & (Z - 1)) + x_to * (Y * Z) + y_to * Z + j_low * (Y * l)
    gaps = sorted({(x * Y * Z + y * Z) - (y * X * Z + x * Z) for x in range(X) for y in range(Y)})
    for t in range(p.tiles):
        block = BB[t * LANES:(t + 1) * LANES, :] * is_open
        block = jnp.concatenate([block, jnp.zeros((LANES, LANES - NB), f32)], axis=1)
        block = jnp.transpose(block)[0:2 * ROWS, :]
        out = block
        for gap in gaps:
            if gap:
                out = jnp.where(source_lane - lane128 == gap, roll(block, -gap), out)
        CS[pl.ds(t, NB, stride=ROWS), :] = out[0:NB, :]
    coef_copies = []
    for r in range(1, S):
        d, device = mate(r)
        coef_copies.append(send(CS, CR.at[me], c_s.at[r - 1], c_r.at[r - 1], device))
    CR[me] = CS[...]

    def halo_field(m):
        return [
            send(V.at[m, 1], V.at[m, Y + 1], hv_s.at[m, 0], hv_r.at[m, 0], along(-1)),
            send(V.at[m, Y], V.at[m, 0], hv_s.at[m, 1], hv_r.at[m, 1], along(1)),
        ]

    def arrived(copies):
        for copy in copies:
            copy.wait_recv()

    arrived(field_copies)
    for t in range(p.HT):
        for first in range(0, S, G):
            blocks = butterfly([RB[first + n, :, t * LANES:(t + 1) * LANES] for n in range(G)])
            at = first // G * LANES
            for n in range(G):
                y, o = divmod(t * G + n, O)
                V[0, y + 1, o * Cw:(o + 1) * Cw, at:at + LANES] = blocks[n]
    halo = halo_field(0)

    arrived(coef_copies)
    for first in range(0, S, G):
        blocks = butterfly([CR[first + n] for n in range(G)])
        at = first // G * LANES
        for n in range(G):
            jl, y = divmod(n, Y)
            M[jl, y + 1, :, at:at + LANES] = blocks[n]
    coef_halo = []
    for n, (run, y_from, y_to_slot, way) in enumerate(
            [(run, Y, 0, 1) for run in ahead_runs] + [(run, 1, Y + 1, -1) for run in behind_runs]):
        rows = pl.ds(run[0] * ROWS, run[1] * ROWS)
        coef_halo.append(send(
            M.at[:, y_from, rows], M.at[:, y_to_slot, rows], hm_s.at[n], hm_r.at[n], along(way)))

    HALFJ = O // p.JT
    diag_rows = [(i % p.JT, NB * ROWS + i * HALFJ + i // p.JT) for i in range(O)]
    part = jnp.zeros((1, L), f32)
    for y in range(1, Y + 1):
        for jl, row in diag_rows:
            part = part + M[jl, y, row:row + 1, :]
    TG[ay] = jnp.broadcast_to(jnp.sum(part, axis=1, keepdims=True), (ROWS, LANES))
    theta_copies = [
        send(TG.at[ay], TG.at[ay], th_s.at[r - 1], th_r.at[r - 1], along(r)) for r in range(1, p.ny)]

    def inside(y):
        return 0 <= y < Y

    def mirror(within):
        groups = {}
        for k, o in enumerate(bonds):
            for y in range(Y):
                if inside(y - o[1]) == within:
                    groups.setdefault((-o[0], -o[2]), []).extend((k, jl, y) for jl in range(p.JT))
        for (sx, sz), members in groups.items():
            blocks = [M[jl, y + 1 - bonds[k][1], k * ROWS:(k + 1) * ROWS, :] for k, jl, y in members]
            if (sx, sz) != (0, 0):
                at = place(sx, sz) * L
                moved = jnp.dot(halves(jnp.concatenate(blocks, axis=0)), PM[:, at:at + L], preferred_element_type=f32)
                blocks = [moved[n * ROWS:(n + 1) * ROWS] for n in range(len(members))]
            for (k, jl, y), block in zip(members, blocks):
                MB[k, jl, y] = block

    mirror(True)

    def spread_field(m, slots):
        rows = len(slots) * OC
        for n, slot in enumerate(slots):
            LH[n * OC:(n + 1) * OC, :] = halves(V[m, slot])
        for n in range(0, 8, 2):
            at = slice(n * L, (n + 2) * L)
            moved = jnp.dot(LH[0:rows, :], PM[:, at], preferred_element_type=f32)
            for q, slot in enumerate(slots):
                VS[slot, :, at] = moved[q * OC:(q + 1) * OC]

    def add_bonds(acc, m, y, steps):
        for k, o in enumerate(bonds):
            for sign in (1, -1):
                if sign * o[1] not in steps:
                    continue
                slot = y + 1 + sign * o[1]
                sx, sz = sign * o[0], sign * o[2]
                for j in range(O):
                    rows = slice(j * Cw, (j + 1) * Cw)
                    at = place(sx, sz) * L
                    v = V[m, slot, rows, :] if (sx, sz) == (0, 0) else VS[slot, rows, at:at + L]
                    for i in range(O):
                        if sign > 0:
                            row = k * ROWS + i * HALFJ + j // p.JT
                            c = M[j % p.JT, y + 1, row:row + 1, :]
                        else:
                            row = j * HALFJ + i // p.JT
                            c = MB[k, i % p.JT, y, row:row + 1, :]
                        acc[i] = acc[i] + c * v

    def add_onsite(acc, m, y, theta):
        for j in range(O):
            v = V[m, y + 1, j * Cw:(j + 1) * Cw, :]
            for i in range(O):
                row = NB * ROWS + i * HALFJ + j // p.JT
                c = M[j % p.JT, y + 1, row:row + 1, :]
                if i == j:
                    c = c - theta
                acc[i] = acc[i] + c * v

    def put(acc, m, y):
        for i in range(O):
            V[m, y + 1, i * Cw:(i + 1) * Cw, :] = acc[i]

    def take(m, y):
        return [V[m, y + 1, i * Cw:(i + 1) * Cw, :] for i in range(O)]

    def zeros():
        return [jnp.zeros((Cw, L), f32) for _ in range(O)]

    def moment(a, b):
        total = jnp.zeros((Cw, L), f32)
        for y in range(Y):
            for i in range(O):
                rows = slice(i * Cw, (i + 1) * Cw)
                total = total + V[a, y + 1, rows, :] * V[b, y + 1, rows, :]
        return jnp.sum(total, axis=1, keepdims=True)

    moments = []
    home_copies = []

    def go_home(m):
        for t in range(p.HT):
            for first in range(0, S, G):
                at = first // G * LANES
                blocks = []
                for n in range(G):
                    y, o = divmod(t * G + n, O)
                    blocks.append(V[m, y + 1, o * Cw:(o + 1) * Cw, at:at + LANES])
                blocks = butterfly(blocks)
                for n in range(G):
                    SB[m - 1, first + n, :, t * LANES:(t + 1) * LANES] = blocks[n]
        mine = pl.ds(pl.multiple_of(me * Cw, ROWS), Cw)
        for r in range(1, S):
            d, device = mate(r)
            home_copies.append(send(
                SB.at[m - 1, d], YB.at[m - 1, mine], y_s.at[m - 1, r - 1], y_r.at[m - 1, r - 1], device))
        YB[m - 1, mine] = SB[m - 1, me]

    theta = None
    for m in range(ITERS):
        spread_field(m, range(1, Y + 1))
        for y in range(Y):
            acc = zeros()
            add_bonds(acc, m, y, [s for s in (-1, 0, 1) if inside(y + s)])
            put(acc, m + 1, y)
        if m == 0:
            moments.append(moment(0, 0))
            arrived(theta_copies)
            theta = TG[0][0:1, 0:1]
            for n in range(1, p.ny):
                theta = theta + TG[n][0:1, 0:1]
            theta = theta * (1.0 / (p.ny * Y * L * O))
        arrived(halo)
        if m == 0:
            arrived(coef_halo)
            mirror(False)
        spread_field(m, (0, Y + 1))
        for y, s in ((0, -1), (Y - 1, 1)):
            acc = take(m + 1, y)
            add_bonds(acc, m, y, [s])
            add_onsite(acc, m, y, theta)
            put(acc, m + 1, y)
        if m + 1 < ITERS:
            halo = halo_field(m + 1)
        for y in range(1, Y - 1):
            acc = take(m + 1, y)
            add_onsite(acc, m, y, theta)
            put(acc, m + 1, y)
        go_home(m + 1)
        moments.append(moment(m, m + 1))
        if m + 1 < ITERS:
            moments.append(moment(m + 1, m + 1))

    table = jnp.zeros((Cw, LANES), f32)
    for n, value in enumerate(moments):
        table = jnp.where(lane128 == n, value, table)
    if Cw < LANES:
        table = jnp.concatenate([table, jnp.zeros((LANES - Cw, LANES), f32)], axis=0)
    MG[ay] = jnp.transpose(table)[0:ROWS, :]
    arrived([send(MG.at[ay], MG.at[ay], mo_s.at[r - 1], mo_r.at[r - 1], along(r)) for r in range(1, p.ny)])
    total = MG[0]
    for n in range(1, p.ny):
        total = total + MG[n]
    m_of = [total[n:n + 1, :] for n in range(2 * ITERS)]
    shift = jnp.zeros((1, LANES), f32)
    for d in range(S):
        h, at = divmod(d * Cw, LANES)
        shift = jnp.where(me == d, roll(shift_ref[:, h * LANES:(h + 1) * LANES], -at), shift)
    shift = shift + theta

    def inner(u, v):
        out = None
        for a, first in enumerate(u):
            for b, second in enumerate(v):
                term = first * second * m_of[a + b]
                out = term if out is None else out + term
        return out

    def plus(u, v, factor):
        n = max(len(u), len(v))
        out = []
        for a in range(n):
            if a < len(v):
                term = factor * v[a]
                out.append(u[a] + term if a < len(u) else term)
            else:
                out.append(u[a])
        return out

    one = jnp.ones((1, LANES), f32)
    answer, residual, direction, norm = [], [one], [one], m_of[0]
    for turn in range(ITERS):
        image = [shift * direction[0]]
        for a in range(1, len(direction)):
            image.append(direction[a - 1] + shift * direction[a])
        image.append(direction[-1])
        alpha = norm / inner(direction, image)
        answer = plus(answer, direction, alpha)
        residual = plus(residual, image, -alpha)
        if turn + 1 < ITERS:
            fresh = inner(residual, residual)
            direction = plus(residual, direction, fresh / norm)
            norm = fresh
    factors = answer + residual
    WQ[me] = jnp.concatenate(factors + [jnp.zeros((ROWS - len(factors), LANES), f32)], axis=0)
    factor_copies = []
    for r in range(1, S):
        d, device = mate(r)
        factor_copies.append(send(WQ.at[me], WQ.at[me], w_s.at[r - 1], w_r.at[r - 1], device))
    arrived(factor_copies)
    arrived(home_copies)

    outs = []
    for h in range(H):
        lines = jnp.zeros((ROWS, LANES), f32)
        per = LANES // Cw
        for n in range(per):
            d = h * per + n
            lines = jnp.where(lane128 // Cw == n, roll(WQ[d], n * Cw), lines)
        column = jnp.transpose(lines)
        rows = slice(h * LANES, (h + 1) * LANES)
        basis = [T[rows, :]] + [YB[n, rows, :] for n in range(ITERS)]
        for which, hbm in ((0, sol_hbm), (1, res_hbm)):
            at = which * ITERS
            field = column[:, at:at + 1] * basis[0]
            for n in range(1, ITERS + which):
                field = field + column[:, at + n:at + n + 1] * basis[n]
            field = jnp.transpose(field)
            for y in range(Y):
                for o in range(O):
                    n = (y * O + o) * l
                    OS[which, pl.ds(y * X * Z * step + h * O + o, l, stride=step), :] = field[n:n + l, :]
    for which, hbm in ((0, sol_hbm), (1, res_hbm)):
        for x in range(X):
            for y in range(Y):
                n = Z * H * O
                copy = pltpu.make_async_copy(
                    OS.at[which, pl.ds((y * X + x) * n, n)], hbm.at[x, y], in_sem.at[(which * X + x) * Y + y])
                copy.start()
                outs.append(copy)
    for copy in outs:
        copy.wait()
    for copy in pending:
        copy.wait_send()


def per_device(peers, right_side, bond_blocks, bond_open, onsite_blocks, orbital_levels, column_shift):
    block, orb, cols = right_side.shape[:3], right_side.shape[3], right_side.shape[4]
    p = Plan(block, orb, cols, peers)
    X, Y, Z, O, S, L, H = p.X, p.Y, p.Z, p.O, p.S, p.L, p.H
    f32 = jnp.float32
    right = right_side.reshape(X, Y, Z, O, H, LANES).transpose(0, 1, 2, 4, 3, 5).reshape(X, Y, Z * H * O, LANES)
    blocks = jnp.transpose(bond_blocks, (1, 2, 3, 4, 5, 0)).reshape(O * O * X * Y * Z, NB)
    opened = jnp.transpose(bond_open, (1, 2, 3, 0)).reshape(X * Y * Z, NB)
    onsite = onsite_blocks.reshape(O * O * X * Y, Z)
    levels = orbital_levels.reshape(O * X * Y, Z)
    dma = pltpu.SemaphoreType.DMA
    anywhere = pl.BlockSpec(memory_space=pl.ANY)

    def scratch(*shape):
        return pltpu.VMEM(shape, f32)

    outs = pl.pallas_call(
        functools.partial(kernel, p),
        out_shape=(jax.ShapeDtypeStruct(right.shape, f32),) * 2,
        in_specs=[anywhere] * 6,
        out_specs=(anywhere, anywhere),
        scratch_shapes=[
            scratch(X * Y * Z * H * O, LANES),
            scratch(O * O * X * Y * Z, NB),
            pltpu.VMEM(opened.shape, jnp.int32),
            scratch(*onsite.shape),
            scratch(*levels.shape),
            scratch(1, cols),
            pltpu.VMEM((2 * L, 8 * L), jnp.bfloat16),
            pltpu.VMEM((Y * p.OC, 2 * L), jnp.bfloat16),
            scratch(cols, p.HL),
            scratch(S, p.Cw, p.HL),
            scratch(p.CR, LANES),
            scratch(S, p.CR, LANES),
            scratch(p.JT, Y + 2, p.CR, L),
            scratch(NB, p.JT, Y, ROWS, L),
            scratch(ITERS + 1, Y + 2, p.OC, L),
            scratch(Y + 2, p.OC, 8 * L),
            scratch(ITERS, S, p.Cw, p.HL),
            scratch(ITERS, cols, p.HL),
            scratch(p.ny, ROWS, LANES),
            scratch(p.ny, ROWS, LANES),
            scratch(S, ROWS, LANES),
            scratch(2, X * Y * Z * H * O, LANES),
            dma((2 * X * Y,)),
            dma((S - 1,)), dma((S - 1,)), dma((S - 1,)), dma((S - 1,)),
            dma((ITERS, 2)), dma((ITERS, 2)), dma((3,)), dma((3,)),
            dma((p.ny - 1,)), dma((p.ny - 1,)),
            dma((ITERS, S - 1)), dma((ITERS, S - 1)),
            dma((p.ny - 1,)), dma((p.ny - 1,)), dma((S - 1,)), dma((S - 1,)),
        ],
        compiler_params=pltpu.CompilerParams(
            collective_id=0, has_side_effects=True, vmem_limit_bytes=60 * 1024 * 1024
        ),
    )(right, blocks, opened, onsite, levels, column_shift[None])

    def back(v):
        return v.reshape(X, Y, Z, H, O, LANES).transpose(0, 1, 2, 4, 3, 5).reshape(right_side.shape)

    return back(outs[0]), back(outs[1])


def solution(mesh):
    field = P("gx", "gy", "gz", None, None)
    placed = (
        field,
        P(None, None, None, "gx", "gy", "gz"),
        P(None, "gx", "gy", "gz"),
        P(None, None, "gx", "gy", "gz"),
        P(None, "gx", "gy", "gz"),
        P(),
    )
    return jax.shard_map(
        functools.partial(per_device, tuple(mesh.shape[name] for name in AXES)),
        mesh=mesh,
        in_specs=placed,
        out_specs=(field, field),
        check_vma=False,
    )
```

```python
import functools
import itertools

import jax
import jax.numpy as jnp
from jax import lax
from jax.experimental import pallas as pl
from jax.experimental.pallas import tpu as pltpu
from jax.sharding import PartitionSpec as P

ITERS = 3
LANES = 128
ROWS = 8
AXES = ("gx", "gy", "gz")
MESH = pl.DeviceIdType.MESH

bonds = [o for o in itertools.product((-1, 0, 1), repeat=3) if o > (0, 0, 0)]
NB = len(bonds)
ahead_runs = [(1, 3), (10, 3)]
behind_runs = [(4, 3)]
assert all(bonds[k][1] == 1 for at, n in ahead_runs for k in range(at, at + n))
assert all(bonds[k][1] == -1 for at, n in behind_runs for k in range(at, at + n))


class Plan:
    def __init__(self, block, orb, cols, peers):
        self.X, self.Y, self.Z = block
        self.O, self.cols = orb, cols
        self.nx, self.ny, self.nz = peers
        self.S = self.nx * self.nz
        self.l = self.X * self.Z
        self.L = self.S * self.l
        self.G = LANES // self.l
        self.Cw = cols // self.S
        self.YO = self.Y * orb
        self.HL = self.YO * self.l
        self.HT = self.HL // LANES
        self.H = cols // LANES
        self.JT = LANES // (self.Y * self.l)
        self.tiles = orb * orb // self.JT
        self.CR = (NB + 1) * self.tiles
        self.OC = orb * self.Cw
        assert self.tiles == ROWS and self.S % self.G == 0 and self.Cw % ROWS == 0


def kernel(plan, rs_hbm, bb_hbm, open_hbm, onsite_hbm, level_hbm, shift_hbm, sol_hbm, res_hbm,
           RS, BB, open_ref, onsite_ref, level_ref, shift_ref, PM, LH, T, RB, CS, CR, M, MB, V, VS, SB, YB, EM, SR, TG, OS,
           in_sem, a_s, a_r, c_s, c_r, hv_s, hv_r, hm_s, hm_r, th_s, th_r, y_s, y_r, e_s, e_r):
    p = plan
    X, Y, Z, O, S, L, l, G, Cw, H, OC = p.X, p.Y, p.Z, p.O, p.S, p.L, p.l, p.G, p.Cw, p.H, p.OC
    f32 = jnp.float32
    ax, ay, az = (lax.axis_index(name) for name in AXES)
    me = ax * p.nz + az
    pending = []

    def mate(r):
        d = lax.rem(me + r, S)
        return d, (lax.div(d, p.nz), ay, lax.rem(d, p.nz))

    def source(r):
        return lax.rem(me + (S - r), S)

    def along(r):
        return (ax, lax.rem(ay + (r % p.ny), p.ny), az)

    def send(src, dst, ssem, rsem, device):
        copy = pltpu.make_async_remote_copy(
            src_ref=src, dst_ref=dst, send_sem=ssem, recv_sem=rsem, device_id=device, device_id_type=MESH
        )
        copy.start()
        pending.append(copy)
        return copy

    barrier = pltpu.get_barrier_semaphore()
    for r in range(1, S):
        pl.semaphore_signal(barrier, inc=1, device_id=mate(r)[1], device_id_type=MESH)
    for r in range(1, p.ny):
        pl.semaphore_signal(barrier, inc=1, device_id=along(r), device_id_type=MESH)

    loads = []
    for x in range(X):
        for y in range(Y):
            n = Z * H * O
            copy = pltpu.make_async_copy(
                rs_hbm.at[x, y], RS.at[pl.ds((y * X + x) * n, n)], in_sem.at[x * Y + y])
            copy.start()
            loads.append(copy)
    small_loads = []
    for n, (src, dst) in enumerate(((onsite_hbm, onsite_ref), (level_hbm, level_ref), (bb_hbm, BB),
                                    (open_hbm, open_ref), (shift_hbm, shift_ref))):
        copy = pltpu.make_async_copy(src, dst, in_sem.at[X * Y + n])
        copy.start()
        small_loads.append(copy)

    lane = lax.broadcasted_iota(jnp.int32, (1, L), 1)
    lane128 = lax.broadcasted_iota(jnp.int32, (1, LANES), 1)

    def roll(v, by):
        by = by % v.shape[1]
        return v if by == 0 else pltpu.roll(v, by, 1)

    zg = ((lane // l) & (p.nz - 1)) * Z + (lane & (Z - 1))
    xg = (lane // (l * p.nz)) * X + ((lane // Z) & (X - 1))
    row_of = lax.broadcasted_iota(jnp.int32, (L, L), 0)

    def place(sx, sz):
        n = (sx + 1) * 3 + sz + 1
        return n - (n > 4)

    def make_shifts():
        for sx in (-1, 0, 1):
            for sz in (-1, 0, 1):
                if (sx, sz) == (0, 0):
                    continue
                x_to, z_to = (xg + sx) & (p.nx * X - 1), (zg + sz) & (p.nz * Z - 1)
                from_lane = ((x_to // X) * p.nz + z_to // Z) * l + (x_to & (X - 1)) * Z + (z_to & (Z - 1))
                matrix = jnp.where(row_of == from_lane, 1.0, 0.0).astype(jnp.bfloat16)
                at = place(sx, sz) * L
                PM[0:L, at:at + L] = matrix
                PM[L:2 * L, at:at + L] = matrix

    def halves(v):
        high = v.astype(jnp.bfloat16)
        low = (v - high.astype(f32)).astype(jnp.bfloat16)
        return jnp.concatenate([high, low], axis=1)

    block_of = lane128 // l

    def butterfly(arrays):
        arrays = list(arrays)
        m = 1
        while m < G:
            low = (block_of & m) == 0
            for a in range(G):
                if a & m == 0:
                    b = a | m
                    first, second = arrays[a], arrays[b]
                    arrays[a] = jnp.where(low, first, roll(second, m * l))
                    arrays[b] = jnp.where(low, roll(first, -m * l), second)
            m *= 2
        return arrays

    for copy in loads:
        copy.wait()
    step = H * O
    for h in range(H):
        rows = jnp.concatenate([
            RS[pl.ds(y * X * Z * step + h * O + o, l, stride=step), :] for y in range(Y) for o in range(O)
        ], axis=0)
        T[h * LANES:(h + 1) * LANES, :] = jnp.transpose(rows)
    make_shifts()
    pl.semaphore_wait(barrier, S - 1 + p.ny - 1)
    field_copies = []
    for r in range(1, S):
        d, device = mate(r)
        field_copies.append(send(
            T.at[pl.ds(pl.multiple_of(d * Cw, ROWS), Cw)], RB.at[me], a_s.at[r - 1], a_r.at[r - 1], device))
    RB[me] = T[pl.ds(pl.multiple_of(me * Cw, ROWS), Cw), :]

    def spread_z(block):
        n = block.shape[0]
        out = jnp.zeros((n, LANES), f32)
        for z in range(Z):
            out = jnp.where((lane128 & (Z - 1)) == z, block[:, z:z + 1], out)
        row = lax.broadcasted_iota(jnp.int32, (n, LANES), 0)
        col = lax.broadcasted_iota(jnp.int32, (n, LANES), 1)
        x_row, y_row = (row // Y) & (X - 1), row & (Y - 1)
        x_col, y_col = (col // Z) & (X - 1), (col // l) & (Y - 1)
        return jnp.where((x_row == x_col) & (y_row == y_col), out, 0.0)

    for copy in small_loads[0:2]:
        copy.wait()
    onsite = spread_z(onsite_ref[...])
    level = spread_z(level_ref[...])
    XY = X * Y
    pair = [jnp.sum(onsite[n * XY:(n + 1) * XY], axis=0, keepdims=True) for n in range(O * O)]
    diagonal = [jnp.sum(level[n * XY:(n + 1) * XY], axis=0, keepdims=True) for n in range(O)]
    j_low = lane128 // (Y * l)
    for i in range(O):
        for jh in range(O // p.JT):
            line = jnp.zeros((1, LANES), f32)
            for jl in range(p.JT):
                j = jh * p.JT + jl
                term = 0.5 * (pair[i * O + j] + pair[j * O + i])
                if i == j:
                    term = term + diagonal[i]
                line = jnp.where(j_low == jl, term, line)
            row = NB * ROWS + i * (O // p.JT) + jh
            CS[row:row + 1, :] = line

    for copy in small_loads[2:]:
        copy.wait()
    is_open = open_ref[...].astype(f32)
    is_open = jnp.concatenate([is_open] * p.JT, axis=0)
    x_of, y_of = (lane128 // (Y * Z)) & (X - 1), (lane128 // Z) & (Y - 1)
    x_to, y_to = (lane128 // Z) & (X - 1), (lane128 // (X * Z)) & (Y - 1)
    source_lane = (lane128 & (Z - 1)) + x_to * (Y * Z) + y_to * Z + j_low * (Y * l)
    gaps = sorted({(x * Y * Z + y * Z) - (y * X * Z + x * Z) for x in range(X) for y in range(Y)})
    for t in range(p.tiles):
        block = BB[t * LANES:(t + 1) * LANES, :] * is_open
        block = jnp.concatenate([block, jnp.zeros((LANES, LANES - NB), f32)], axis=1)
        block = jnp.transpose(block)[0:2 * ROWS, :]
        out = block
        for gap in gaps:
            if gap:
                out = jnp.where(source_lane - lane128 == gap, roll(block, -gap), out)
        CS[pl.ds(t, NB, stride=ROWS), :] = out[0:NB, :]
    coef_copies = []
    for r in range(1, S):
        d, device = mate(r)
        coef_copies.append(send(CS, CR.at[me], c_s.at[r - 1], c_r.at[r - 1], device))
    CR[me] = CS[...]

    def halo_field(m):
        return [
            send(V.at[m, 1], V.at[m, Y + 1], hv_s.at[m, 0], hv_r.at[m, 0], along(-1)),
            send(V.at[m, Y], V.at[m, 0], hv_s.at[m, 1], hv_r.at[m, 1], along(1)),
        ]

    def arrived(copies):
        for copy in copies:
            copy.wait_recv()

    arrived(field_copies)
    for t in range(p.HT):
        for first in range(0, S, G):
            blocks = butterfly([RB[first + n, :, t * LANES:(t + 1) * LANES] for n in range(G)])
            at = first // G * LANES
            for n in range(G):
                y, o = divmod(t * G + n, O)
                V[0, y + 1, o * Cw:(o + 1) * Cw, at:at + LANES] = blocks[n]
    halo = halo_field(0)

    arrived(coef_copies)
    for first in range(0, S, G):
        blocks = butterfly([CR[first + n] for n in range(G)])
        at = first // G * LANES
        for n in range(G):
            jl, y = divmod(n, Y)
            M[jl, y + 1, :, at:at + LANES] = blocks[n]
    coef_halo = []
    for n, (run, y_from, y_to_slot, way) in enumerate(
            [(run, Y, 0, 1) for run in ahead_runs] + [(run, 1, Y + 1, -1) for run in behind_runs]):
        rows = pl.ds(run[0] * ROWS, run[1] * ROWS)
        coef_halo.append(send(
            M.at[:, y_from, rows], M.at[:, y_to_slot, rows], hm_s.at[n], hm_r.at[n], along(way)))

    HALFJ = O // p.JT
    diag_rows = [(i % p.JT, NB * ROWS + i * HALFJ + i // p.JT) for i in range(O)]
    part = jnp.zeros((1, L), f32)
    for y in range(1, Y + 1):
        for jl, row in diag_rows:
            part = part + M[jl, y, row:row + 1, :]
    TG[ay] = jnp.broadcast_to(jnp.sum(part, axis=1, keepdims=True), (ROWS, LANES))
    theta_copies = [
        send(TG.at[ay], TG.at[ay], th_s.at[r - 1], th_r.at[r - 1], along(r)) for r in range(1, p.ny)]

    def inside(y):
        return 0 <= y < Y

    def mirror(within):
        groups = {}
        for k, o in enumerate(bonds):
            for y in range(Y):
                if inside(y - o[1]) == within:
                    groups.setdefault((-o[0], -o[2]), []).extend((k, jl, y) for jl in range(p.JT))
        for (sx, sz), members in groups.items():
            blocks = [M[jl, y + 1 - bonds[k][1], k * ROWS:(k + 1) * ROWS, :] for k, jl, y in members]
            if (sx, sz) != (0, 0):
                at = place(sx, sz) * L
                moved = jnp.dot(halves(jnp.concatenate(blocks, axis=0)), PM[:, at:at + L], preferred_element_type=f32)
                blocks = [moved[n * ROWS:(n + 1) * ROWS] for n in range(len(members))]
            for (k, jl, y), block in zip(members, blocks):
                MB[k, jl, y] = block

    mirror(True)

    def spread_field(m, slots):
        rows = len(slots) * OC
        for n, slot in enumerate(slots):
            LH[n * OC:(n + 1) * OC, :] = halves(V[m, slot])
        for n in range(0, 8, 2):
            at = slice(n * L, (n + 2) * L)
            moved = jnp.dot(LH[0:rows, :], PM[:, at], preferred_element_type=f32)
            for q, slot in enumerate(slots):
                VS[slot, :, at] = moved[q * OC:(q + 1) * OC]

    def add_bonds(acc, m, y, steps):
        for k, o in enumerate(bonds):
            for sign in (1, -1):
                if sign * o[1] not in steps:
                    continue
                slot = y + 1 + sign * o[1]
                sx, sz = sign * o[0], sign * o[2]
                for j in range(O):
                    rows = slice(j * Cw, (j + 1) * Cw)
                    at = place(sx, sz) * L
                    v = V[m, slot, rows, :] if (sx, sz) == (0, 0) else VS[slot, rows, at:at + L]
                    for i in range(O):
                        if sign > 0:
                            row = k * ROWS + i * HALFJ + j // p.JT
                            c = M[j % p.JT, y + 1, row:row + 1, :]
                        else:
                            row = j * HALFJ + i // p.JT
                            c = MB[k, i % p.JT, y, row:row + 1, :]
                        acc[i] = acc[i] + c * v

    def add_onsite(acc, m, y, theta):
        for j in range(O):
            v = V[m, y + 1, j * Cw:(j + 1) * Cw, :]
            for i in range(O):
                row = NB * ROWS + i * HALFJ + j // p.JT
                c = M[j % p.JT, y + 1, row:row + 1, :]
                if i == j:
                    c = c - theta
                acc[i] = acc[i] + c * v

    def put(acc, m, y):
        for i in range(O):
            V[m, y + 1, i * Cw:(i + 1) * Cw, :] = acc[i]

    def take(m, y):
        return [V[m, y + 1, i * Cw:(i + 1) * Cw, :] for i in range(O)]

    def zeros():
        return [jnp.zeros((Cw, L), f32) for _ in range(O)]

    def moment(a, b):
        total = jnp.zeros((Cw, L), f32)
        for y in range(Y):
            for i in range(O):
                rows = slice(i * Cw, (i + 1) * Cw)
                total = total + V[a, y + 1, rows, :] * V[b, y + 1, rows, :]
        return jnp.sum(total, axis=1, keepdims=True)

    moments = []
    home_copies = []

    everyone = [(g, r) for g in range(p.ny) for r in range(S) if (g, r) != (0, 0)]

    def tell(part, values):
        table = jnp.zeros((Cw, LANES), f32)
        for n, value in enumerate(values):
            table = jnp.where(lane128 == n, value, table)
        if Cw < LANES:
            table = jnp.concatenate([table, jnp.zeros((LANES - Cw, LANES), f32)], axis=0)
        table = jnp.transpose(table)
        line = table[0:1]
        for n in range(1, len(values)):
            line = line + roll(table[n:n + 1], n * Cw)
        EM[part, ay, me] = line
        SR[part] = line
        copies = []
        for n, (g, r) in enumerate(everyone):
            d = lax.rem(me + r, S)
            device = (lax.div(d, p.nz), lax.rem(ay + g, p.ny), lax.rem(d, p.nz))
            copies.append(send(SR.at[part], EM.at[part, ay, me], e_s.at[part, n], e_r.at[part, n], device))
        return copies

    def go_home(m):
        for t in range(p.HT):
            for first in range(0, S, G):
                at = first // G * LANES
                blocks = []
                for n in range(G):
                    y, o = divmod(t * G + n, O)
                    blocks.append(V[m, y + 1, o * Cw:(o + 1) * Cw, at:at + LANES])
                blocks = butterfly(blocks)
                for n in range(G):
                    SB[m - 1, first + n, :, t * LANES:(t + 1) * LANES] = blocks[n]
        mine = pl.ds(pl.multiple_of(me * Cw, ROWS), Cw)
        for r in range(1, S):
            d, device = mate(r)
            home_copies.append(send(
                SB.at[m - 1, d], YB.at[m - 1, mine], y_s.at[m - 1, r - 1], y_r.at[m - 1, r - 1], device))
        YB[m - 1, mine] = SB[m - 1, me]

    theta = None
    for m in range(ITERS):
        spread_field(m, range(1, Y + 1))
        for y in range(Y):
            acc = zeros()
            add_bonds(acc, m, y, [s for s in (-1, 0, 1) if inside(y + s)])
            put(acc, m + 1, y)
        if m == 0:
            moments.append(moment(0, 0))
            arrived(theta_copies)
            theta = TG[0][0:1, 0:1]
            for n in range(1, p.ny):
                theta = theta + TG[n][0:1, 0:1]
            theta = theta * (1.0 / (p.ny * Y * L * O))
        arrived(halo)
        if m == 0:
            arrived(coef_halo)
            mirror(False)
        spread_field(m, (0, Y + 1))
        for y, s in ((0, -1), (Y - 1, 1)):
            acc = take(m + 1, y)
            add_bonds(acc, m, y, [s])
            add_onsite(acc, m, y, theta)
            put(acc, m + 1, y)
        if m + 1 < ITERS:
            halo = halo_field(m + 1)
        for y in range(1, Y - 1):
            acc = take(m + 1, y)
            add_onsite(acc, m, y, theta)
            put(acc, m + 1, y)
        go_home(m + 1)
        moments.append(moment(m, m + 1))
        if m + 1 < ITERS:
            moments.append(moment(m + 1, m + 1))
        if m + 2 == ITERS:
            early = len(moments) - 1
            told = tell(0, moments[:early])
    told = told + tell(1, moments[early:])

    shift = jnp.concatenate([
        roll(shift_ref[:, d * Cw // LANES * LANES:(d * Cw // LANES + 1) * LANES], -(d * Cw % LANES)) for d in range(S)
    ], axis=0) + theta
    arrived(told)

    def total(part):
        rows = []
        for d in range(S):
            line = EM[part, 0, d]
            for n in range(1, p.ny):
                line = line + EM[part, n, d]
            rows.append(line)
        return jnp.concatenate(rows, axis=0)

    sums = [total(0), total(1)]
    m_of = [roll(sums[n >= early], -(n - early * (n >= early)) * Cw) for n in range(2 * ITERS)]

    def inner(u, v):
        out = None
        for a, first in enumerate(u):
            for b, second in enumerate(v):
                term = first * second * m_of[a + b]
                out = term if out is None else out + term
        return out

    def plus(u, v, factor):
        n = max(len(u), len(v))
        out = []
        for a in range(n):
            if a < len(v):
                term = factor * v[a]
                out.append(u[a] + term if a < len(u) else term)
            else:
                out.append(u[a])
        return out

    one = jnp.ones((S, LANES), f32)
    answer, residual, direction, norm = [], [one], [one], m_of[0]
    for turn in range(ITERS):
        image = [shift * direction[0]]
        for a in range(1, len(direction)):
            image.append(direction[a - 1] + shift * direction[a])
        image.append(direction[-1])
        alpha = norm / inner(direction, image)
        answer = plus(answer, direction, alpha)
        residual = plus(residual, image, -alpha)
        if turn + 1 < ITERS:
            fresh = inner(residual, residual)
            direction = plus(residual, direction, fresh / norm)
            norm = fresh
    factors = answer + residual
    lines = jnp.concatenate(factors, axis=0)
    spare = -lines.shape[0] % LANES
    if spare:
        lines = jnp.concatenate([lines, jnp.zeros((spare, LANES), f32)], axis=0)
    column = jnp.transpose(lines)
    arrived(home_copies)

    outs = []
    for which, hbm in ((0, sol_hbm), (1, res_hbm)):
        for h in range(H):
            fields = []
            for d in range(h * LANES // Cw, (h + 1) * LANES // Cw):
                rows = slice(d * Cw, (d + 1) * Cw)
                field = None
                for n in range(ITERS + which):
                    at = (which * ITERS + n) * S + d
                    term = column[0:Cw, at:at + 1] * (T[rows, :] if n == 0 else YB[n - 1, rows, :])
                    field = term if field is None else field + term
                fields.append(field)
            field = jnp.transpose(jnp.concatenate(fields, axis=0))
            for y in range(Y):
                for o in range(O):
                    n = (y * O + o) * l
                    OS[which, pl.ds(y * X * Z * step + h * O + o, l, stride=step), :] = field[n:n + l, :]
        for x in range(X):
            for y in range(Y):
                n = Z * H * O
                copy = pltpu.make_async_copy(
                    OS.at[which, pl.ds((y * X + x) * n, n)], hbm.at[x, y], in_sem.at[(which * X + x) * Y + y])
                copy.start()
                outs.append(copy)
    for copy in outs:
        copy.wait()
    for copy in pending:
        copy.wait_send()


def per_device(peers, right_side, bond_blocks, bond_open, onsite_blocks, orbital_levels, column_shift):
    block, orb, cols = right_side.shape[:3], right_side.shape[3], right_side.shape[4]
    p = Plan(block, orb, cols, peers)
    X, Y, Z, O, S, L, H = p.X, p.Y, p.Z, p.O, p.S, p.L, p.H
    f32 = jnp.float32
    right = right_side.reshape(X, Y, Z, O, H, LANES).transpose(0, 1, 2, 4, 3, 5).reshape(X, Y, Z * H * O, LANES)
    blocks = jnp.transpose(bond_blocks, (1, 2, 3, 4, 5, 0)).reshape(O * O * X * Y * Z, NB)
    opened = jnp.transpose(bond_open, (1, 2, 3, 0)).reshape(X * Y * Z, NB)
    onsite = onsite_blocks.reshape(O * O * X * Y, Z)
    levels = orbital_levels.reshape(O * X * Y, Z)
    dma = pltpu.SemaphoreType.DMA
    anywhere = pl.BlockSpec(memory_space=pl.ANY)

    def scratch(*shape):
        return pltpu.VMEM(shape, f32)

    outs = pl.pallas_call(
        functools.partial(kernel, p),
        out_shape=(jax.ShapeDtypeStruct(right.shape, f32),) * 2,
        in_specs=[anywhere] * 6,
        out_specs=(anywhere, anywhere),
        scratch_shapes=[
            scratch(X * Y * Z * H * O, LANES),
            scratch(O * O * X * Y * Z, NB),
            pltpu.VMEM(opened.shape, jnp.int32),
            scratch(*onsite.shape),
            scratch(*levels.shape),
            scratch(1, cols),
            pltpu.VMEM((2 * L, 8 * L), jnp.bfloat16),
            pltpu.VMEM((Y * p.OC, 2 * L), jnp.bfloat16),
            scratch(cols, p.HL),
            scratch(S, p.Cw, p.HL),
            scratch(p.CR, LANES),
            scratch(S, p.CR, LANES),
            scratch(p.JT, Y + 2, p.CR, L),
            scratch(NB, p.JT, Y, ROWS, L),
            scratch(ITERS + 1, Y + 2, p.OC, L),
            scratch(Y + 2, p.OC, 8 * L),
            scratch(ITERS, S, p.Cw, p.HL),
            scratch(ITERS, cols, p.HL),
            scratch(2, p.ny, S, 1, LANES),
            scratch(2, 1, LANES),
            scratch(p.ny, ROWS, LANES),
            scratch(2, X * Y * Z * H * O, LANES),
            dma((2 * X * Y,)),
            dma((S - 1,)), dma((S - 1,)), dma((S - 1,)), dma((S - 1,)),
            dma((ITERS, 2)), dma((ITERS, 2)), dma((3,)), dma((3,)),
            dma((p.ny - 1,)), dma((p.ny - 1,)),
            dma((ITERS, S - 1)), dma((ITERS, S - 1)),
            dma((2, p.ny * S - 1)), dma((2, p.ny * S - 1)),
        ],
        compiler_params=pltpu.CompilerParams(
            collective_id=0, has_side_effects=True, vmem_limit_bytes=60 * 1024 * 1024
        ),
    )(right, blocks, opened, onsite, levels, column_shift[None])

    def back(v):
        return v.reshape(X, Y, Z, H, O, LANES).transpose(0, 1, 2, 4, 3, 5).reshape(right_side.shape)

    return back(outs[0]), back(outs[1])


def solution(mesh):
    field = P("gx", "gy", "gz", None, None)
    placed = (
        field,
        P(None, None, None, "gx", "gy", "gz"),
        P(None, "gx", "gy", "gz"),
        P(None, None, "gx", "gy", "gz"),
        P(None, "gx", "gy", "gz"),
        P(),
    )
    return jax.shard_map(
        functools.partial(per_device, tuple(mesh.shape[name] for name in AXES)),
        mesh=mesh,
        in_specs=placed,
        out_specs=(field, field),
        check_vma=False,
    )
```

```python
import functools
import itertools

import jax
import jax.numpy as jnp
from jax import lax
from jax.experimental import pallas as pl
from jax.experimental.pallas import tpu as pltpu
from jax.sharding import PartitionSpec as P

ITERS = 3
LANES = 128
ROWS = 8
AXES = ("gx", "gy", "gz")
MESH = pl.DeviceIdType.MESH

bonds = [o for o in itertools.product((-1, 0, 1), repeat=3) if o > (0, 0, 0)]
NB = len(bonds)
ahead_runs = [(1, 3), (10, 3)]
behind_runs = [(4, 3)]
assert all(bonds[k][1] == 1 for at, n in ahead_runs for k in range(at, at + n))
assert all(bonds[k][1] == -1 for at, n in behind_runs for k in range(at, at + n))


class Plan:
    def __init__(self, block, orb, cols, peers):
        self.X, self.Y, self.Z = block
        self.O, self.cols = orb, cols
        self.nx, self.ny, self.nz = peers
        self.S = self.nx * self.nz
        self.l = self.X * self.Z
        self.L = self.S * self.l
        self.G = LANES // self.l
        self.Cw = cols // self.S
        self.YO = self.Y * orb
        self.HL = self.YO * self.l
        self.HT = self.HL // LANES
        self.H = cols // LANES
        self.JT = LANES // (self.Y * self.l)
        self.tiles = orb * orb // self.JT
        self.CR = (NB + 1) * self.tiles
        self.OC = orb * self.Cw
        assert self.tiles == ROWS and self.S % self.G == 0 and self.Cw % ROWS == 0


def kernel(plan, rs_hbm, bb_hbm, open_hbm, onsite_hbm, level_hbm, shift_hbm, T, YB, FX,
           RS, BB, open_ref, onsite_ref, level_ref, shift_ref, PM, LH, RB, CS, CR, M, MB, V, VS, SB, EM, SR, TG,
           in_sem, a_s, a_r, c_s, c_r, hv_s, hv_r, hm_s, hm_r, th_s, th_r, y_s, y_r, e_s, e_r):
    p = plan
    X, Y, Z, O, S, L, l, G, Cw, H, OC = p.X, p.Y, p.Z, p.O, p.S, p.L, p.l, p.G, p.Cw, p.H, p.OC
    f32 = jnp.float32
    ax, ay, az = (lax.axis_index(name) for name in AXES)
    me = ax * p.nz + az
    pending = []

    def mate(r):
        d = lax.rem(me + r, S)
        return d, (lax.div(d, p.nz), ay, lax.rem(d, p.nz))

    def source(r):
        return lax.rem(me + (S - r), S)

    def along(r):
        return (ax, lax.rem(ay + (r % p.ny), p.ny), az)

    def send(src, dst, ssem, rsem, device):
        copy = pltpu.make_async_remote_copy(
            src_ref=src, dst_ref=dst, send_sem=ssem, recv_sem=rsem, device_id=device, device_id_type=MESH
        )
        copy.start()
        pending.append(copy)
        return copy

    barrier = pltpu.get_barrier_semaphore()
    for r in range(1, S):
        pl.semaphore_signal(barrier, inc=1, device_id=mate(r)[1], device_id_type=MESH)
    for r in range(1, p.ny):
        pl.semaphore_signal(barrier, inc=1, device_id=along(r), device_id_type=MESH)

    loads = []
    for x in range(X):
        for y in range(Y):
            n = Z * H * O
            copy = pltpu.make_async_copy(
                rs_hbm.at[x, y], RS.at[pl.ds((y * X + x) * n, n)], in_sem.at[x * Y + y])
            copy.start()
            loads.append(copy)
    small_loads = []
    for n, (src, dst) in enumerate(((onsite_hbm, onsite_ref), (level_hbm, level_ref), (bb_hbm, BB),
                                    (open_hbm, open_ref), (shift_hbm, shift_ref))):
        copy = pltpu.make_async_copy(src, dst, in_sem.at[X * Y + n])
        copy.start()
        small_loads.append(copy)

    lane = lax.broadcasted_iota(jnp.int32, (1, L), 1)
    lane128 = lax.broadcasted_iota(jnp.int32, (1, LANES), 1)

    def roll(v, by):
        by = by % v.shape[1]
        return v if by == 0 else pltpu.roll(v, by, 1)

    zg = ((lane // l) & (p.nz - 1)) * Z + (lane & (Z - 1))
    xg = (lane // (l * p.nz)) * X + ((lane // Z) & (X - 1))
    row_of = lax.broadcasted_iota(jnp.int32, (L, L), 0)

    def place(sx, sz):
        n = (sx + 1) * 3 + sz + 1
        return n - (n > 4)

    def make_shifts():
        for sx in (-1, 0, 1):
            for sz in (-1, 0, 1):
                if (sx, sz) == (0, 0):
                    continue
                x_to, z_to = (xg + sx) & (p.nx * X - 1), (zg + sz) & (p.nz * Z - 1)
                from_lane = ((x_to // X) * p.nz + z_to // Z) * l + (x_to & (X - 1)) * Z + (z_to & (Z - 1))
                matrix = jnp.where(row_of == from_lane, 1.0, 0.0).astype(jnp.bfloat16)
                at = place(sx, sz) * L
                PM[0:L, at:at + L] = matrix
                PM[L:2 * L, at:at + L] = matrix

    def halves(v):
        high = v.astype(jnp.bfloat16)
        low = (v - high.astype(f32)).astype(jnp.bfloat16)
        return jnp.concatenate([high, low], axis=1)

    block_of = lane128 // l

    def butterfly(arrays):
        arrays = list(arrays)
        m = 1
        while m < G:
            low = (block_of & m) == 0
            for a in range(G):
                if a & m == 0:
                    b = a | m
                    first, second = arrays[a], arrays[b]
                    arrays[a] = jnp.where(low, first, roll(second, m * l))
                    arrays[b] = jnp.where(low, roll(first, -m * l), second)
            m *= 2
        return arrays

    for copy in loads:
        copy.wait()
    step = H * O
    for h in range(H):
        rows = jnp.concatenate([
            RS[pl.ds(y * X * Z * step + h * O + o, l, stride=step), :] for y in range(Y) for o in range(O)
        ], axis=0)
        T[h * LANES:(h + 1) * LANES, :] = jnp.transpose(rows)
    make_shifts()
    pl.semaphore_wait(barrier, S - 1 + p.ny - 1)
    field_copies = []
    for r in range(1, S):
        d, device = mate(r)
        field_copies.append(send(
            T.at[pl.ds(pl.multiple_of(d * Cw, ROWS), Cw)], RB.at[me], a_s.at[r - 1], a_r.at[r - 1], device))
    RB[me] = T[pl.ds(pl.multiple_of(me * Cw, ROWS), Cw), :]

    def spread_z(block):
        n = block.shape[0]
        out = jnp.zeros((n, LANES), f32)
        for z in range(Z):
            out = jnp.where((lane128 & (Z - 1)) == z, block[:, z:z + 1], out)
        row = lax.broadcasted_iota(jnp.int32, (n, LANES), 0)
        col = lax.broadcasted_iota(jnp.int32, (n, LANES), 1)
        x_row, y_row = (row // Y) & (X - 1), row & (Y - 1)
        x_col, y_col = (col // Z) & (X - 1), (col // l) & (Y - 1)
        return jnp.where((x_row == x_col) & (y_row == y_col), out, 0.0)

    for copy in small_loads[0:2]:
        copy.wait()
    onsite = spread_z(onsite_ref[...])
    level = spread_z(level_ref[...])
    XY = X * Y
    pair = [jnp.sum(onsite[n * XY:(n + 1) * XY], axis=0, keepdims=True) for n in range(O * O)]
    diagonal = [jnp.sum(level[n * XY:(n + 1) * XY], axis=0, keepdims=True) for n in range(O)]
    j_low = lane128 // (Y * l)
    for i in range(O):
        for jh in range(O // p.JT):
            line = jnp.zeros((1, LANES), f32)
            for jl in range(p.JT):
                j = jh * p.JT + jl
                term = 0.5 * (pair[i * O + j] + pair[j * O + i])
                if i == j:
                    term = term + diagonal[i]
                line = jnp.where(j_low == jl, term, line)
            row = NB * ROWS + i * (O // p.JT) + jh
            CS[row:row + 1, :] = line

    for copy in small_loads[2:]:
        copy.wait()
    is_open = open_ref[...].astype(f32)
    is_open = jnp.concatenate([is_open] * p.JT, axis=0)
    x_of, y_of = (lane128 // (Y * Z)) & (X - 1), (lane128 // Z) & (Y - 1)
    x_to, y_to = (lane128 // Z) & (X - 1), (lane128 // (X * Z)) & (Y - 1)
    source_lane = (lane128 & (Z - 1)) + x_to * (Y * Z) + y_to * Z + j_low * (Y * l)
    gaps = sorted({(x * Y * Z + y * Z) - (y * X * Z + x * Z) for x in range(X) for y in range(Y)})
    for t in range(p.tiles):
        block = BB[t * LANES:(t + 1) * LANES, :] * is_open
        block = jnp.concatenate([block, jnp.zeros((LANES, LANES - NB), f32)], axis=1)
        block = jnp.transpose(block)[0:2 * ROWS, :]
        out = block
        for gap in gaps:
            if gap:
                out = jnp.where(source_lane - lane128 == gap, roll(block, -gap), out)
        CS[pl.ds(t, NB, stride=ROWS), :] = out[0:NB, :]
    coef_copies = []
    for r in range(1, S):
        d, device = mate(r)
        coef_copies.append(send(CS, CR.at[me], c_s.at[r - 1], c_r.at[r - 1], device))
    CR[me] = CS[...]

    def halo_field(m):
        return [
            send(V.at[m, 1], V.at[m, Y + 1], hv_s.at[m, 0], hv_r.at[m, 0], along(-1)),
            send(V.at[m, Y], V.at[m, 0], hv_s.at[m, 1], hv_r.at[m, 1], along(1)),
        ]

    def arrived(copies):
        for copy in copies:
            copy.wait_recv()

    arrived(field_copies)
    for t in range(p.HT):
        for first in range(0, S, G):
            blocks = butterfly([RB[first + n, :, t * LANES:(t + 1) * LANES] for n in range(G)])
            at = first // G * LANES
            for n in range(G):
                y, o = divmod(t * G + n, O)
                V[0, y + 1, o * Cw:(o + 1) * Cw, at:at + LANES] = blocks[n]
    halo = halo_field(0)

    arrived(coef_copies)
    for first in range(0, S, G):
        blocks = butterfly([CR[first + n] for n in range(G)])
        at = first // G * LANES
        for n in range(G):
            jl, y = divmod(n, Y)
            M[jl, y + 1, :, at:at + LANES] = blocks[n]
    coef_halo = []
    for n, (run, y_from, y_to_slot, way) in enumerate(
            [(run, Y, 0, 1) for run in ahead_runs] + [(run, 1, Y + 1, -1) for run in behind_runs]):
        rows = pl.ds(run[0] * ROWS, run[1] * ROWS)
        coef_halo.append(send(
            M.at[:, y_from, rows], M.at[:, y_to_slot, rows], hm_s.at[n], hm_r.at[n], along(way)))

    HALFJ = O // p.JT
    diag_rows = [(i % p.JT, NB * ROWS + i * HALFJ + i // p.JT) for i in range(O)]
    part = jnp.zeros((1, L), f32)
    for y in range(1, Y + 1):
        for jl, row in diag_rows:
            part = part + M[jl, y, row:row + 1, :]
    TG[ay] = jnp.broadcast_to(jnp.sum(part, axis=1, keepdims=True), (ROWS, LANES))
    theta_copies = [
        send(TG.at[ay], TG.at[ay], th_s.at[r - 1], th_r.at[r - 1], along(r)) for r in range(1, p.ny)]

    def inside(y):
        return 0 <= y < Y

    def mirror(within):
        groups = {}
        for k, o in enumerate(bonds):
            for y in range(Y):
                if inside(y - o[1]) == within:
                    groups.setdefault((-o[0], -o[2]), []).extend((k, jl, y) for jl in range(p.JT))
        for (sx, sz), members in groups.items():
            blocks = [M[jl, y + 1 - bonds[k][1], k * ROWS:(k + 1) * ROWS, :] for k, jl, y in members]
            if (sx, sz) != (0, 0):
                at = place(sx, sz) * L
                moved = jnp.dot(halves(jnp.concatenate(blocks, axis=0)), PM[:, at:at + L], preferred_element_type=f32)
                blocks = [moved[n * ROWS:(n + 1) * ROWS] for n in range(len(members))]
            for (k, jl, y), block in zip(members, blocks):
                MB[k, jl, y] = block

    mirror(True)

    def spread_field(m, slots):
        rows = len(slots) * OC
        for n, slot in enumerate(slots):
            LH[n * OC:(n + 1) * OC, :] = halves(V[m, slot])
        for n in range(0, 8, 2):
            at = slice(n * L, (n + 2) * L)
            moved = jnp.dot(LH[0:rows, :], PM[:, at], preferred_element_type=f32)
            for q, slot in enumerate(slots):
                VS[slot, :, at] = moved[q * OC:(q + 1) * OC]

    def add_bonds(acc, m, y, steps):
        for k, o in enumerate(bonds):
            for sign in (1, -1):
                if sign * o[1] not in steps:
                    continue
                slot = y + 1 + sign * o[1]
                sx, sz = sign * o[0], sign * o[2]
                for j in range(O):
                    rows = slice(j * Cw, (j + 1) * Cw)
                    at = place(sx, sz) * L
                    v = V[m, slot, rows, :] if (sx, sz) == (0, 0) else VS[slot, rows, at:at + L]
                    for i in range(O):
                        if sign > 0:
                            row = k * ROWS + i * HALFJ + j // p.JT
                            c = M[j % p.JT, y + 1, row:row + 1, :]
                        else:
                            row = j * HALFJ + i // p.JT
                            c = MB[k, i % p.JT, y, row:row + 1, :]
                        acc[i] = acc[i] + c * v

    def add_onsite(acc, m, y, theta):
        for j in range(O):
            v = V[m, y + 1, j * Cw:(j + 1) * Cw, :]
            for i in range(O):
                row = NB * ROWS + i * HALFJ + j // p.JT
                c = M[j % p.JT, y + 1, row:row + 1, :]
                if i == j:
                    c = c - theta
                acc[i] = acc[i] + c * v

    def put(acc, m, y):
        for i in range(O):
            V[m, y + 1, i * Cw:(i + 1) * Cw, :] = acc[i]

    def take(m, y):
        return [V[m, y + 1, i * Cw:(i + 1) * Cw, :] for i in range(O)]

    def zeros():
        return [jnp.zeros((Cw, L), f32) for _ in range(O)]

    def moment(a, b):
        total = jnp.zeros((Cw, L), f32)
        for y in range(Y):
            for i in range(O):
                rows = slice(i * Cw, (i + 1) * Cw)
                total = total + V[a, y + 1, rows, :] * V[b, y + 1, rows, :]
        return jnp.sum(total, axis=1, keepdims=True)

    moments = []
    home_copies = []

    everyone = [(g, r) for g in range(p.ny) for r in range(S) if (g, r) != (0, 0)]

    def tell(part, values):
        table = jnp.zeros((Cw, LANES), f32)
        for n, value in enumerate(values):
            table = jnp.where(lane128 == n, value, table)
        if Cw < LANES:
            table = jnp.concatenate([table, jnp.zeros((LANES - Cw, LANES), f32)], axis=0)
        table = jnp.transpose(table)
        line = table[0:1]
        for n in range(1, len(values)):
            line = line + roll(table[n:n + 1], n * Cw)
        EM[part, ay, me] = line
        SR[part] = line
        copies = []
        for n, (g, r) in enumerate(everyone):
            d = lax.rem(me + r, S)
            device = (lax.div(d, p.nz), lax.rem(ay + g, p.ny), lax.rem(d, p.nz))
            copies.append(send(SR.at[part], EM.at[part, ay, me], e_s.at[part, n], e_r.at[part, n], device))
        return copies

    def go_home(m):
        for t in range(p.HT):
            for first in range(0, S, G):
                at = first // G * LANES
                blocks = []
                for n in range(G):
                    y, o = divmod(t * G + n, O)
                    blocks.append(V[m, y + 1, o * Cw:(o + 1) * Cw, at:at + LANES])
                blocks = butterfly(blocks)
                for n in range(G):
                    SB[m - 1, first + n, :, t * LANES:(t + 1) * LANES] = blocks[n]
        mine = pl.ds(pl.multiple_of(me * Cw, ROWS), Cw)
        for r in range(1, S):
            d, device = mate(r)
            home_copies.append(send(
                SB.at[m - 1, d], YB.at[m - 1, mine], y_s.at[m - 1, r - 1], y_r.at[m - 1, r - 1], device))
        YB[m - 1, mine] = SB[m - 1, me]

    theta = None
    for m in range(ITERS):
        spread_field(m, range(1, Y + 1))
        for y in range(Y):
            acc = zeros()
            add_bonds(acc, m, y, [s for s in (-1, 0, 1) if inside(y + s)])
            put(acc, m + 1, y)
        if m == 0:
            moments.append(moment(0, 0))
            arrived(theta_copies)
            theta = TG[0][0:1, 0:1]
            for n in range(1, p.ny):
                theta = theta + TG[n][0:1, 0:1]
            theta = theta * (1.0 / (p.ny * Y * L * O))
        arrived(halo)
        if m == 0:
            arrived(coef_halo)
            mirror(False)
        spread_field(m, (0, Y + 1))
        for y, s in ((0, -1), (Y - 1, 1)):
            acc = take(m + 1, y)
            add_bonds(acc, m, y, [s])
            add_onsite(acc, m, y, theta)
            put(acc, m + 1, y)
        if m + 1 < ITERS:
            halo = halo_field(m + 1)
        for y in range(1, Y - 1):
            acc = take(m + 1, y)
            add_onsite(acc, m, y, theta)
            put(acc, m + 1, y)
        go_home(m + 1)
        moments.append(moment(m, m + 1))
        if m + 1 < ITERS:
            moments.append(moment(m + 1, m + 1))
        if m + 2 == ITERS:
            early = len(moments) - 1
            told = tell(0, moments[:early])
    told = told + tell(1, moments[early:])

    shift = jnp.concatenate([
        roll(shift_ref[:, d * Cw // LANES * LANES:(d * Cw // LANES + 1) * LANES], -(d * Cw % LANES)) for d in range(S)
    ], axis=0) + theta
    arrived(told)

    def total(part):
        rows = []
        for d in range(S):
            line = EM[part, 0, d]
            for n in range(1, p.ny):
                line = line + EM[part, n, d]
            rows.append(line)
        return jnp.concatenate(rows, axis=0)

    sums = [total(0), total(1)]
    m_of = [roll(sums[n >= early], -(n - early * (n >= early)) * Cw) for n in range(2 * ITERS)]

    def inner(u, v):
        out = None
        for a, first in enumerate(u):
            for b, second in enumerate(v):
                term = first * second * m_of[a + b]
                out = term if out is None else out + term
        return out

    def plus(u, v, factor):
        n = max(len(u), len(v))
        out = []
        for a in range(n):
            if a < len(v):
                term = factor * v[a]
                out.append(u[a] + term if a < len(u) else term)
            else:
                out.append(u[a])
        return out

    one = jnp.ones((S, LANES), f32)
    answer, residual, direction, norm = [], [one], [one], m_of[0]
    for turn in range(ITERS):
        image = [shift * direction[0]]
        for a in range(1, len(direction)):
            image.append(direction[a - 1] + shift * direction[a])
        image.append(direction[-1])
        alpha = norm / inner(direction, image)
        answer = plus(answer, direction, alpha)
        residual = plus(residual, image, -alpha)
        if turn + 1 < ITERS:
            fresh = inner(residual, residual)
            direction = plus(residual, direction, fresh / norm)
            norm = fresh
    factors = answer + residual
    lines = jnp.concatenate(factors, axis=0)
    spare = -lines.shape[0] % LANES
    if spare:
        lines = jnp.concatenate([lines, jnp.zeros((spare, LANES), f32)], axis=0)
    for at in range(0, lines.shape[0], LANES):
        FX[:, at:at + LANES] = jnp.transpose(lines[at:at + LANES])
    arrived(home_copies)
    for copy in pending:
        copy.wait_send()


def combine(plan, T, YB, FX, sol_hbm, res_hbm, OS, sem):
    p = plan
    X, Y, Z, O, S, l, Cw, H = p.X, p.Y, p.Z, p.O, p.S, p.l, p.Cw, p.H
    step = H * O
    outs = []
    for which, hbm in ((0, sol_hbm), (1, res_hbm)):
        for h in range(H):
            fields = []
            for d in range(h * LANES // Cw, (h + 1) * LANES // Cw):
                rows = slice(d * Cw, (d + 1) * Cw)
                field = None
                for n in range(ITERS + which):
                    at = (which * ITERS + n) * S + d
                    term = FX[0:Cw, at:at + 1] * (T[rows, :] if n == 0 else YB[n - 1, rows, :])
                    field = term if field is None else field + term
                fields.append(field)
            field = jnp.transpose(jnp.concatenate(fields, axis=0))
            for y in range(Y):
                for o in range(O):
                    n = (y * O + o) * l
                    OS[which, pl.ds(y * X * Z * step + h * O + o, l, stride=step), :] = field[n:n + l, :]
        for x in range(X):
            for y in range(Y):
                n = Z * H * O
                copy = pltpu.make_async_copy(
                    OS.at[which, pl.ds((y * X + x) * n, n)], hbm.at[x, y], sem.at[(which * X + x) * Y + y])
                copy.start()
                outs.append(copy)
    for copy in outs:
        copy.wait()


def per_device(peers, right_side, bond_blocks, bond_open, onsite_blocks, orbital_levels, column_shift):
    block, orb, cols = right_side.shape[:3], right_side.shape[3], right_side.shape[4]
    p = Plan(block, orb, cols, peers)
    X, Y, Z, O, S, L, H = p.X, p.Y, p.Z, p.O, p.S, p.L, p.H
    f32 = jnp.float32
    right = right_side.reshape(X, Y, Z, O, H, LANES).transpose(0, 1, 2, 4, 3, 5).reshape(X, Y, Z * H * O, LANES)
    blocks = jnp.transpose(bond_blocks, (1, 2, 3, 4, 5, 0)).reshape(O * O * X * Y * Z, NB)
    opened = jnp.transpose(bond_open, (1, 2, 3, 0)).reshape(X * Y * Z, NB)
    onsite = onsite_blocks.reshape(O * O * X * Y, Z)
    levels = orbital_levels.reshape(O * X * Y, Z)
    dma = pltpu.SemaphoreType.DMA
    vmem, anywhere = pl.BlockSpec(memory_space=pltpu.VMEM), pl.BlockSpec(memory_space=pl.ANY)

    def scratch(*shape):
        return pltpu.VMEM(shape, f32)

    flat = (p.cols, p.HL)
    width = -(-(2 * ITERS + 1) * S // LANES) * LANES
    made = pl.pallas_call(
        functools.partial(kernel, p),
        out_shape=(scratch(*flat), scratch(ITERS, *flat), scratch(LANES, width)),
        in_specs=[pl.BlockSpec(memory_space=pltpu.HBM)] * 6,
        out_specs=(vmem,) * 3,
        scratch_shapes=[
            scratch(X * Y * Z * H * O, LANES),
            scratch(O * O * X * Y * Z, NB),
            pltpu.VMEM(opened.shape, jnp.int32),
            scratch(*onsite.shape),
            scratch(*levels.shape),
            scratch(1, cols),
            pltpu.VMEM((2 * L, 8 * L), jnp.bfloat16),
            pltpu.VMEM((Y * p.OC, 2 * L), jnp.bfloat16),
            scratch(S, p.Cw, p.HL),
            scratch(p.CR, LANES),
            scratch(S, p.CR, LANES),
            scratch(p.JT, Y + 2, p.CR, L),
            scratch(NB, p.JT, Y, ROWS, L),
            scratch(ITERS + 1, Y + 2, p.OC, L),
            scratch(Y + 2, p.OC, 8 * L),
            scratch(ITERS, S, p.Cw, p.HL),
            scratch(2, p.ny, S, 1, LANES),
            scratch(2, 1, LANES),
            scratch(p.ny, ROWS, LANES),
            dma((X * Y + 5,)),
            dma((S - 1,)), dma((S - 1,)), dma((S - 1,)), dma((S - 1,)),
            dma((ITERS, 2)), dma((ITERS, 2)), dma((3,)), dma((3,)),
            dma((p.ny - 1,)), dma((p.ny - 1,)),
            dma((ITERS, S - 1)), dma((ITERS, S - 1)),
            dma((2, p.ny * S - 1)), dma((2, p.ny * S - 1)),
        ],
        compiler_params=pltpu.CompilerParams(
            collective_id=0, has_side_effects=True, vmem_limit_bytes=40 * 1024 * 1024
        ),
    )(*(pltpu.with_memory_space_constraint(v, pltpu.HBM)
        for v in (right, blocks, opened, onsite, levels, column_shift[None])))
    outs = pl.pallas_call(
        functools.partial(combine, p),
        out_shape=(jax.ShapeDtypeStruct(right.shape, f32),) * 2,
        in_specs=[vmem] * 3,
        out_specs=(anywhere, anywhere),
        scratch_shapes=[scratch(2, X * Y * Z * H * O, LANES), dma((2 * X * Y,))],
        compiler_params=pltpu.CompilerParams(vmem_limit_bytes=16 * 1024 * 1024),
    )(*made)

    def back(v):
        return v.reshape(X, Y, Z, H, O, LANES).transpose(0, 1, 2, 4, 3, 5).reshape(right_side.shape)

    return back(outs[0]), back(outs[1])


def solution(mesh):
    field = P("gx", "gy", "gz", None, None)
    placed = (
        field,
        P(None, None, None, "gx", "gy", "gz"),
        P(None, "gx", "gy", "gz"),
        P(None, None, "gx", "gy", "gz"),
        P(None, "gx", "gy", "gz"),
        P(),
    )
    return jax.shard_map(
        functools.partial(per_device, tuple(mesh.shape[name] for name in AXES)),
        mesh=mesh,
        in_specs=placed,
        out_specs=(field, field),
        check_vma=False,
    )
```

```python
import functools
import itertools

import jax
import jax.numpy as jnp
from jax import lax
from jax.experimental import pallas as pl
from jax.experimental.pallas import tpu as pltpu
from jax.sharding import PartitionSpec as P

ITERS = 3
LANES = 128
ROWS = 8
AXES = ("gx", "gy", "gz")
MESH = pl.DeviceIdType.MESH

bonds = [o for o in itertools.product((-1, 0, 1), repeat=3) if o > (0, 0, 0)]
NB = len(bonds)
ahead_runs = [(1, 3), (10, 3)]
behind_runs = [(4, 3)]
assert all(bonds[k][1] == 1 for at, n in ahead_runs for k in range(at, at + n))
assert all(bonds[k][1] == -1 for at, n in behind_runs for k in range(at, at + n))


class Plan:
    def __init__(self, block, orb, cols, peers):
        self.X, self.Y, self.Z = block
        self.O, self.cols = orb, cols
        self.nx, self.ny, self.nz = peers
        self.S = self.nx * self.nz
        self.l = self.X * self.Z
        self.L = self.S * self.l
        self.G = LANES // self.l
        self.Cw = cols // self.S
        self.YO = self.Y * orb
        self.HL = self.YO * self.l
        self.HT = self.HL // LANES
        self.H = cols // LANES
        self.JT = LANES // (self.Y * self.l)
        self.tiles = orb * orb // self.JT
        self.CR = (NB + 1) * self.tiles
        self.OC = orb * self.Cw
        edge = sum(n for _, n in ahead_runs + behind_runs)
        self.HR = (-(-edge // (LANES // (self.JT * self.l))) + 1) * ROWS
        assert self.H * orb == ROWS
        assert self.tiles == ROWS and self.S % self.G == 0 and self.Cw % ROWS == 0


def kernel(plan, rs_hbm, bb_hbm, open_hbm, onsite_hbm, level_hbm, shift_hbm, BT, FX,
           RS, BB, open_ref, onsite_ref, level_ref, shift_ref, PM, LH, T, YB, ZC, HS, HC, RB, CS, CR, M, MB, V, VS, SB, EM, SR, TG,
           in_sem, a_s, a_r, c_s, c_r, hv_s, hv_r, hm_s, hm_r, ho_s, ho_r, th_s, th_r, y_s, y_r, e_s, e_r):
    p = plan
    X, Y, Z, O, S, L, l, G, Cw, H, OC = p.X, p.Y, p.Z, p.O, p.S, p.L, p.l, p.G, p.Cw, p.H, p.OC
    f32 = jnp.float32
    ax, ay, az = (lax.axis_index(name) for name in AXES)
    me = ax * p.nz + az
    pending = []

    def mate(r):
        d = lax.rem(me + r, S)
        return d, (lax.div(d, p.nz), ay, lax.rem(d, p.nz))

    def source(r):
        return lax.rem(me + (S - r), S)

    def along(r):
        return (ax, lax.rem(ay + (r % p.ny), p.ny), az)

    def send(src, dst, ssem, rsem, device):
        copy = pltpu.make_async_remote_copy(
            src_ref=src, dst_ref=dst, send_sem=ssem, recv_sem=rsem, device_id=device, device_id_type=MESH
        )
        copy.start()
        pending.append(copy)
        return copy

    barrier = pltpu.get_barrier_semaphore()
    for r in range(1, S):
        pl.semaphore_signal(barrier, inc=1, device_id=mate(r)[1], device_id_type=MESH)
    for r in range(1, p.ny):
        pl.semaphore_signal(barrier, inc=1, device_id=along(r), device_id_type=MESH)

    loads = []
    for x in range(X):
        for y in range(Y):
            n = Z * H * O
            copy = pltpu.make_async_copy(
                rs_hbm.at[x, y], RS.at[pl.ds((y * X + x) * n, n)], in_sem.at[x * Y + y])
            copy.start()
            loads.append(copy)
    small_loads = []
    for n, (src, dst) in enumerate(((onsite_hbm, onsite_ref), (level_hbm, level_ref), (bb_hbm, BB),
                                    (open_hbm, open_ref), (shift_hbm, shift_ref))):
        copy = pltpu.make_async_copy(src, dst, in_sem.at[X * Y + n])
        copy.start()
        small_loads.append(copy)

    lane = lax.broadcasted_iota(jnp.int32, (1, L), 1)
    lane128 = lax.broadcasted_iota(jnp.int32, (1, LANES), 1)

    def roll(v, by):
        by = by % v.shape[1]
        return v if by == 0 else pltpu.roll(v, by, 1)

    zg = ((lane // l) & (p.nz - 1)) * Z + (lane & (Z - 1))
    xg = (lane // (l * p.nz)) * X + ((lane // Z) & (X - 1))
    row_of = lax.broadcasted_iota(jnp.int32, (L, L), 0)

    def place(sx, sz):
        n = (sx + 1) * 3 + sz + 1
        return n - (n > 4)

    def make_shifts():
        for sx in (-1, 0, 1):
            for sz in (-1, 0, 1):
                if (sx, sz) == (0, 0):
                    continue
                x_to, z_to = (xg + sx) & (p.nx * X - 1), (zg + sz) & (p.nz * Z - 1)
                from_lane = ((x_to // X) * p.nz + z_to // Z) * l + (x_to & (X - 1)) * Z + (z_to & (Z - 1))
                matrix = jnp.where(row_of == from_lane, 1.0, 0.0).astype(jnp.bfloat16)
                at = place(sx, sz) * L
                PM[0:L, at:at + L] = matrix
                PM[L:2 * L, at:at + L] = matrix

    def halves(v):
        high = v.astype(jnp.bfloat16)
        low = (v - high.astype(f32)).astype(jnp.bfloat16)
        return jnp.concatenate([high, low], axis=1)

    block_of = lane128 // l

    def butterfly(arrays):
        arrays = list(arrays)
        m = 1
        while m < G:
            low = (block_of & m) == 0
            for a in range(G):
                if a & m == 0:
                    b = a | m
                    first, second = arrays[a], arrays[b]
                    arrays[a] = jnp.where(low, first, roll(second, m * l))
                    arrays[b] = jnp.where(low, roll(first, -m * l), second)
            m *= 2
        return arrays

    for copy in loads:
        copy.wait()
    step = H * O
    for h in range(H):
        rows = jnp.concatenate([
            RS[pl.ds(y * X * Z * step + h * O + o, l, stride=step), :] for y in range(Y) for o in range(O)
        ], axis=0)
        T[h * LANES:(h + 1) * LANES, :] = jnp.transpose(rows)
    BT[0] = RS[...]
    make_shifts()
    pl.semaphore_wait(barrier, S - 1 + p.ny - 1)
    field_copies = []
    for r in range(1, S):
        d, device = mate(r)
        field_copies.append(send(
            T.at[pl.ds(pl.multiple_of(d * Cw, ROWS), Cw)], RB.at[me], a_s.at[r - 1], a_r.at[r - 1], device))
    RB[me] = T[pl.ds(pl.multiple_of(me * Cw, ROWS), Cw), :]

    def spread_z(block):
        n = block.shape[0]
        out = jnp.zeros((n, LANES), f32)
        for z in range(Z):
            out = jnp.where((lane128 & (Z - 1)) == z, block[:, z:z + 1], out)
        row = lax.broadcasted_iota(jnp.int32, (n, LANES), 0)
        col = lax.broadcasted_iota(jnp.int32, (n, LANES), 1)
        x_row, y_row = (row // Y) & (X - 1), row & (Y - 1)
        x_col, y_col = (col // Z) & (X - 1), (col // l) & (Y - 1)
        return jnp.where((x_row == x_col) & (y_row == y_col), out, 0.0)

    for copy in small_loads[0:2]:
        copy.wait()
    onsite = spread_z(onsite_ref[...])
    level = spread_z(level_ref[...])
    XY = X * Y
    pair = [jnp.sum(onsite[n * XY:(n + 1) * XY], axis=0, keepdims=True) for n in range(O * O)]
    diagonal = [jnp.sum(level[n * XY:(n + 1) * XY], axis=0, keepdims=True) for n in range(O)]
    j_low = lane128 // (Y * l)
    diagonal_sum = jnp.zeros((1, LANES), f32)
    for i in range(O):
        for jh in range(O // p.JT):
            line = jnp.zeros((1, LANES), f32)
            for jl in range(p.JT):
                j = jh * p.JT + jl
                term = 0.5 * (pair[i * O + j] + pair[j * O + i])
                if i == j:
                    term = term + diagonal[i]
                    diagonal_sum = diagonal_sum + jnp.where(j_low == 0, term, 0.0)
                line = jnp.where(j_low == jl, term, line)
            row = NB * ROWS + i * (O // p.JT) + jh
            CS[row:row + 1, :] = line

    diagonal_sum = jnp.sum(diagonal_sum, axis=1, keepdims=True)
    for copy in small_loads[2:]:
        copy.wait()
    is_open = open_ref[...].astype(f32)
    is_open = jnp.concatenate([is_open] * p.JT, axis=0)
    x_of, y_of = (lane128 // (Y * Z)) & (X - 1), (lane128 // Z) & (Y - 1)
    x_to, y_to = (lane128 // Z) & (X - 1), (lane128 // (X * Z)) & (Y - 1)
    source_lane = (lane128 & (Z - 1)) + x_to * (Y * Z) + y_to * Z + j_low * (Y * l)
    gaps = sorted({(x * Y * Z + y * Z) - (y * X * Z + x * Z) for x in range(X) for y in range(Y)})
    for t in range(p.tiles):
        block = BB[t * LANES:(t + 1) * LANES, :] * is_open
        block = jnp.concatenate([block, jnp.zeros((LANES, LANES - NB), f32)], axis=1)
        block = jnp.transpose(block)[0:2 * ROWS, :]
        out = block
        for gap in gaps:
            if gap:
                out = jnp.where(source_lane - lane128 == gap, roll(block, -gap), out)
        CS[pl.ds(t, NB, stride=ROWS), :] = out[0:NB, :]
    early_halo = []
    for n, (run, way) in enumerate([(run, 1) for run in ahead_runs] + [(run, -1) for run in behind_runs]):
        early_halo.append(send(
            CS.at[pl.ds(run[0] * ROWS, run[1] * ROWS)], ZC.at[n], hm_s.at[n], hm_r.at[n], along(way)))
    TG[ay] = jnp.broadcast_to(diagonal_sum, (ROWS, LANES))
    early_halo += [
        send(TG.at[ay], TG.at[ay], th_s.at[r - 1], th_r.at[r - 1], along(r)) for r in range(1, p.ny)]
    coef_copies = []
    for r in range(1, S):
        d, device = mate(r)
        coef_copies.append(send(CS, CR.at[me], c_s.at[r - 1], c_r.at[r - 1], device))
    CR[me] = CS[...]

    def halo_field(m):
        return [
            send(V.at[m, 1], V.at[m, Y + 1], hv_s.at[m, 0], hv_r.at[m, 0], along(-1)),
            send(V.at[m, Y], V.at[m, 0], hv_s.at[m, 1], hv_r.at[m, 1], along(1)),
        ]

    def arrived(copies):
        for copy in copies:
            copy.wait_recv()

    def spread_field(m, slots):
        rows = len(slots) * OC
        for n, slot in enumerate(slots):
            LH[n * OC:(n + 1) * OC, :] = halves(V[m, slot])
        for n in range(0, 8, 2):
            at = slice(n * L, (n + 2) * L)
            moved = jnp.dot(LH[0:rows, :], PM[:, at], preferred_element_type=f32)
            for q, slot in enumerate(slots):
                VS[slot, :, at] = moved[q * OC:(q + 1) * OC]

    arrived(field_copies)
    for t in range(p.HT):
        for first in range(0, S, G):
            blocks = butterfly([RB[first + n, :, t * LANES:(t + 1) * LANES] for n in range(G)])
            at = first // G * LANES
            for n in range(G):
                y, o = divmod(t * G + n, O)
                V[0, y + 1, o * Cw:(o + 1) * Cw, at:at + LANES] = blocks[n]
    halo = halo_field(0)

    arrived(early_halo)
    outer = [(n, q, run[0] + q, slot, y) for n, (run, slot, y) in enumerate(
        [(run, 0, Y - 1) for run in ahead_runs] + [(run, Y + 1, 0) for run in behind_runs]) for q in range(run[1])]
    unit = p.JT * l
    U = LANES // unit
    for v in range(0, len(outer), U):
        packed = jnp.zeros((ROWS, LANES), f32)
        for q, (n, at, k, slot, y) in enumerate(outer[v:v + U]):
            block = ZC[n, at * ROWS:(at + 1) * ROWS, :]
            for jl in range(p.JT):
                to = q * unit + jl * l
                packed = jnp.where(block_of == to // l, roll(block, to - jl * Y * l - y * l), packed)
        HS[v // U * ROWS:(v // U + 1) * ROWS, :] = packed
    part = TG[0]
    for n in range(1, p.ny):
        part = part + TG[n]
    HS[p.HR - ROWS:p.HR, :] = part
    outer_copies = []
    for r in range(1, S):
        d, device = mate(r)
        outer_copies.append(send(HS, HC.at[me], ho_s.at[r - 1], ho_r.at[r - 1], device))
    HC[me] = HS[...]
    spread_field(0, range(1, Y + 1))

    def take_outer():
        arrived(outer_copies)
        for first in range(0, S, G):
            blocks = butterfly([HC[first + n, 0:p.HR - ROWS, :] for n in range(G)])
            at = first // G * LANES
            for n, (_, _, k, slot, y) in enumerate(outer):
                v, q = divmod(n, U)
                for jl in range(p.JT):
                    M[jl, slot, k * ROWS:(k + 1) * ROWS, at:at + LANES] = (
                        blocks[q * p.JT + jl][v * ROWS:(v + 1) * ROWS])
        mirror(False)
        total = HC[0, p.HR - ROWS:p.HR - ROWS + 1, 0:1]
        for n in range(1, S):
            total = total + HC[n, p.HR - ROWS:p.HR - ROWS + 1, 0:1]
        return total * (1.0 / (p.ny * Y * L * O))

    arrived(coef_copies)
    for first in range(0, S, G):
        blocks = butterfly([CR[first + n] for n in range(G)])
        at = first // G * LANES
        for n in range(G):
            jl, y = divmod(n, Y)
            M[jl, y + 1, :, at:at + LANES] = blocks[n]
    HALFJ = O // p.JT

    def inside(y):
        return 0 <= y < Y

    def mirror(within):
        groups = {}
        for k, o in enumerate(bonds):
            for y in range(Y):
                if inside(y - o[1]) == within:
                    groups.setdefault((-o[0], -o[2]), []).extend((k, jl, y) for jl in range(p.JT))
        for (sx, sz), members in groups.items():
            blocks = [M[jl, y + 1 - bonds[k][1], k * ROWS:(k + 1) * ROWS, :] for k, jl, y in members]
            if (sx, sz) != (0, 0):
                at = place(sx, sz) * L
                moved = jnp.dot(halves(jnp.concatenate(blocks, axis=0)), PM[:, at:at + L], preferred_element_type=f32)
                blocks = [moved[n * ROWS:(n + 1) * ROWS] for n in range(len(members))]
            for (k, jl, y), block in zip(members, blocks):
                MB[k, jl, y] = block

    mirror(True)

    def add_bonds(acc, m, y, steps):
        for k, o in enumerate(bonds):
            for sign in (1, -1):
                if sign * o[1] not in steps:
                    continue
                slot = y + 1 + sign * o[1]
                sx, sz = sign * o[0], sign * o[2]
                for j in range(O):
                    rows = slice(j * Cw, (j + 1) * Cw)
                    at = place(sx, sz) * L
                    v = V[m, slot, rows, :] if (sx, sz) == (0, 0) else VS[slot, rows, at:at + L]
                    for i in range(O):
                        if sign > 0:
                            row = k * ROWS + i * HALFJ + j // p.JT
                            c = M[j % p.JT, y + 1, row:row + 1, :]
                        else:
                            row = j * HALFJ + i // p.JT
                            c = MB[k, i % p.JT, y, row:row + 1, :]
                        acc[i] = acc[i] + c * v

    def add_onsite(acc, m, y, theta):
        for j in range(O):
            v = V[m, y + 1, j * Cw:(j + 1) * Cw, :]
            for i in range(O):
                row = NB * ROWS + i * HALFJ + j // p.JT
                c = M[j % p.JT, y + 1, row:row + 1, :]
                if i == j:
                    c = c - theta
                acc[i] = acc[i] + c * v

    def put(acc, m, y):
        for i in range(O):
            V[m, y + 1, i * Cw:(i + 1) * Cw, :] = acc[i]

    def take(m, y):
        return [V[m, y + 1, i * Cw:(i + 1) * Cw, :] for i in range(O)]

    def zeros():
        return [jnp.zeros((Cw, L), f32) for _ in range(O)]

    def moment(a, b):
        total = jnp.zeros((Cw, L), f32)
        for y in range(Y):
            for i in range(O):
                rows = slice(i * Cw, (i + 1) * Cw)
                total = total + V[a, y + 1, rows, :] * V[b, y + 1, rows, :]
        return jnp.sum(total, axis=1, keepdims=True)

    moments = []
    home_copies = []

    everyone = [(g, r) for g in range(p.ny) for r in range(S) if (g, r) != (0, 0)]

    def tell(part, values):
        sublane = lax.broadcasted_iota(jnp.int32, (Cw, LANES), 0)
        spot = lax.broadcasted_iota(jnp.int32, (Cw, LANES), 1)
        table = jnp.zeros((Cw, LANES), f32)
        for n, value in enumerate(values):
            table = jnp.where(spot == sublane + n * Cw, value, table)
        line = jnp.sum(table, axis=0, keepdims=True)
        EM[part, ay, me] = line
        SR[part] = line
        copies = []
        for n, (g, r) in enumerate(everyone):
            d = lax.rem(me + r, S)
            device = (lax.div(d, p.nz), lax.rem(ay + g, p.ny), lax.rem(d, p.nz))
            copies.append(send(SR.at[part], EM.at[part, ay, me], e_s.at[part, n], e_r.at[part, n], device))
        return copies

    def go_home(m):
        for t in range(p.HT):
            for first in range(0, S, G):
                at = first // G * LANES
                blocks = []
                for n in range(G):
                    y, o = divmod(t * G + n, O)
                    blocks.append(V[m, y + 1, o * Cw:(o + 1) * Cw, at:at + LANES])
                blocks = butterfly(blocks)
                for n in range(G):
                    SB[m - 1, first + n, :, t * LANES:(t + 1) * LANES] = blocks[n]
        mine = pl.ds(pl.multiple_of(me * Cw, ROWS), Cw)
        for r in range(1, S):
            d, device = mate(r)
            home_copies.append(send(
                SB.at[m - 1, d], YB.at[m - 1, mine], y_s.at[m - 1, r - 1], y_r.at[m - 1, r - 1], device))
        YB[m - 1, mine] = SB[m - 1, me]

    theta = None
    for m in range(ITERS):
        if m > 0:
            spread_field(m, range(1, Y + 1))
        for y in range(Y):
            acc = zeros()
            add_bonds(acc, m, y, [s for s in (-1, 0, 1) if inside(y + s)])
            put(acc, m + 1, y)
        if m == 0:
            moments.append(moment(0, 0))
            theta = take_outer()
        arrived(halo)
        spread_field(m, (0, Y + 1))
        for y, s in ((0, -1), (Y - 1, 1)):
            acc = take(m + 1, y)
            add_bonds(acc, m, y, [s])
            add_onsite(acc, m, y, theta)
            put(acc, m + 1, y)
        if m + 1 < ITERS:
            halo = halo_field(m + 1)
        for y in range(1, Y - 1):
            acc = take(m + 1, y)
            add_onsite(acc, m, y, theta)
            put(acc, m + 1, y)
        if m + 1 < ITERS:
            go_home(m + 1)
        moments.append(moment(m, m + 1))
        if m + 1 < ITERS:
            moments.append(moment(m + 1, m + 1))
        if m + 2 == ITERS:
            early = len(moments) - 1
            told = tell(0, moments[:early])
    told = told + tell(1, moments[early:])
    go_home(ITERS)

    shift = jnp.concatenate([
        roll(shift_ref[:, d * Cw // LANES * LANES:(d * Cw // LANES + 1) * LANES], -(d * Cw % LANES)) for d in range(S)
    ], axis=0) + theta

    def turn_home(n):
        arrived(home_copies[n * (S - 1):(n + 1) * (S - 1)])
        for h in range(H):
            field = jnp.transpose(YB[n, h * LANES:(h + 1) * LANES, :])
            for y in range(Y):
                for o in range(O):
                    at = (y * O + o) * l
                    BT[n + 1, pl.ds(y * X * Z * step + h * O + o, l, stride=step), :] = field[at:at + l, :]

    for n in range(ITERS):
        turn_home(n)
    arrived(told)

    def total(part):
        rows = []
        for d in range(S):
            line = EM[part, 0, d]
            for n in range(1, p.ny):
                line = line + EM[part, n, d]
            rows.append(line)
        return jnp.concatenate(rows, axis=0)

    sums = [total(0), total(1)]
    m_of = [roll(sums[n >= early], -(n - early * (n >= early)) * Cw) for n in range(2 * ITERS)]

    def inner(u, v):
        out = None
        for a, first in enumerate(u):
            for b, second in enumerate(v):
                term = first * second * m_of[a + b]
                out = term if out is None else out + term
        return out

    def plus(u, v, factor):
        n = max(len(u), len(v))
        out = []
        for a in range(n):
            if a < len(v):
                term = factor * v[a]
                out.append(u[a] + term if a < len(u) else term)
            else:
                out.append(u[a])
        return out

    one = jnp.ones((S, LANES), f32)
    answer, residual, direction, norm = [], [one], [one], m_of[0]
    for turn in range(ITERS):
        image = [shift * direction[0]]
        for a in range(1, len(direction)):
            image.append(direction[a - 1] + shift * direction[a])
        image.append(direction[-1])
        alpha = norm / inner(direction, image)
        answer = plus(answer, direction, alpha)
        residual = plus(residual, image, -alpha)
        if turn + 1 < ITERS:
            fresh = inner(residual, residual)
            direction = plus(residual, direction, fresh / norm)
            norm = fresh
    factors = answer + residual
    per = LANES // Cw
    half = lax.broadcasted_iota(jnp.int32, (H * O, LANES), 0) // O
    for n, factor in enumerate(factors):
        turned = [roll(factor, q * Cw) for q in range(per)]
        block = jnp.zeros((H * O, LANES), f32)
        for h in range(H):
            line = turned[0][h * per:h * per + 1]
            for q in range(1, per):
                line = jnp.where(lane128 // Cw == q, turned[q][h * per + q:h * per + q + 1], line)
            block = jnp.where(half == h, line, block)
        FX[n] = block
    for copy in pending:
        copy.wait_send()


def combine(plan, BT, FX, sol_hbm, res_hbm, OS, sem):
    p = plan
    X, Y, n = p.X, p.Y, p.Z * p.H * p.O
    group = p.H * p.O
    outs = []
    for which, hbm in ((0, sol_hbm), (1, res_hbm)):
        for y in range(Y):
            for x in range(X):
                base = (y * X + x) * n
                for at in range(base, base + n, group):
                    rows = slice(at, at + group)
                    field = FX[which * ITERS] * BT[0, rows, :]
                    for q in range(1, ITERS + which):
                        field = field + FX[which * ITERS + q] * BT[q, rows, :]
                    OS[which, rows, :] = field
        for x in range(X):
            for y in range(Y):
                copy = pltpu.make_async_copy(
                    OS.at[which, pl.ds((y * X + x) * n, n)], hbm.at[x, y], sem.at[(which * X + x) * Y + y])
                copy.start()
                outs.append(copy)
    for copy in outs:
        copy.wait()


def per_device(peers, right_side, bond_blocks, bond_open, onsite_blocks, orbital_levels, column_shift):
    block, orb, cols = right_side.shape[:3], right_side.shape[3], right_side.shape[4]
    p = Plan(block, orb, cols, peers)
    X, Y, Z, O, S, L, H = p.X, p.Y, p.Z, p.O, p.S, p.L, p.H
    f32 = jnp.float32
    right = right_side.reshape(X, Y, Z, O, H, LANES).transpose(0, 1, 2, 4, 3, 5).reshape(X, Y, Z * H * O, LANES)
    blocks = jnp.transpose(bond_blocks, (1, 2, 3, 4, 5, 0)).reshape(O * O * X * Y * Z, NB)
    opened = jnp.transpose(bond_open, (1, 2, 3, 0)).reshape(X * Y * Z, NB)
    onsite = onsite_blocks.reshape(O * O * X * Y, Z)
    levels = orbital_levels.reshape(O * X * Y, Z)
    dma = pltpu.SemaphoreType.DMA
    vmem, anywhere = pl.BlockSpec(memory_space=pltpu.VMEM), pl.BlockSpec(memory_space=pl.ANY)

    def scratch(*shape):
        return pltpu.VMEM(shape, f32)

    flat = (p.cols, p.HL)
    made = pl.pallas_call(
        functools.partial(kernel, p),
        out_shape=(scratch(ITERS + 1, X * Y * Z * H * O, LANES), scratch(2 * ITERS + 1, H * O, LANES)),
        in_specs=[pl.BlockSpec(memory_space=pltpu.HBM)] * 6,
        out_specs=(vmem,) * 2,
        scratch_shapes=[
            scratch(X * Y * Z * H * O, LANES),
            scratch(O * O * X * Y * Z, NB),
            pltpu.VMEM(opened.shape, jnp.int32),
            scratch(*onsite.shape),
            scratch(*levels.shape),
            scratch(1, cols),
            pltpu.VMEM((2 * L, 8 * L), jnp.bfloat16),
            pltpu.VMEM((Y * p.OC, 2 * L), jnp.bfloat16),
            scratch(*flat),
            scratch(ITERS, *flat),
            scratch(3, 3 * ROWS, LANES),
            scratch(p.HR, LANES),
            scratch(S, p.HR, LANES),
            scratch(S, p.Cw, p.HL),
            scratch(p.CR, LANES),
            scratch(S, p.CR, LANES),
            scratch(p.JT, Y + 2, p.CR, L),
            scratch(NB, p.JT, Y, ROWS, L),
            scratch(ITERS + 1, Y + 2, p.OC, L),
            scratch(Y + 2, p.OC, 8 * L),
            scratch(ITERS, S, p.Cw, p.HL),
            scratch(2, p.ny, S, 1, LANES),
            scratch(2, 1, LANES),
            scratch(p.ny, ROWS, LANES),
            dma((X * Y + 5,)),
            dma((S - 1,)), dma((S - 1,)), dma((S - 1,)), dma((S - 1,)),
            dma((ITERS, 2)), dma((ITERS, 2)), dma((3,)), dma((3,)),
            dma((S - 1,)), dma((S - 1,)),
            dma((p.ny - 1,)), dma((p.ny - 1,)),
            dma((ITERS, S - 1)), dma((ITERS, S - 1)),
            dma((2, p.ny * S - 1)), dma((2, p.ny * S - 1)),
        ],
        compiler_params=pltpu.CompilerParams(
            collective_id=0, has_side_effects=True, vmem_limit_bytes=40 * 1024 * 1024
        ),
    )(*(pltpu.with_memory_space_constraint(v, pltpu.HBM)
        for v in (right, blocks, opened, onsite, levels, column_shift[None])))
    outs = pl.pallas_call(
        functools.partial(combine, p),
        out_shape=(jax.ShapeDtypeStruct(right.shape, f32),) * 2,
        in_specs=[vmem] * 2,
        out_specs=(anywhere, anywhere),
        scratch_shapes=[scratch(2, X * Y * Z * H * O, LANES), dma((2 * X * Y,))],
        compiler_params=pltpu.CompilerParams(vmem_limit_bytes=16 * 1024 * 1024),
    )(*made)

    def back(v):
        return v.reshape(X, Y, Z, H, O, LANES).transpose(0, 1, 2, 4, 3, 5).reshape(right_side.shape)

    return back(outs[0]), back(outs[1])


def solution(mesh):
    field = P("gx", "gy", "gz", None, None)
    placed = (
        field,
        P(None, None, None, "gx", "gy", "gz"),
        P(None, "gx", "gy", "gz"),
        P(None, None, "gx", "gy", "gz"),
        P(None, "gx", "gy", "gz"),
        P(),
    )
    return jax.shard_map(
        functools.partial(per_device, tuple(mesh.shape[name] for name in AXES)),
        mesh=mesh,
        in_specs=placed,
        out_specs=(field, field),
        check_vma=False,
    )
```

```python
import functools
import itertools

import jax
import jax.numpy as jnp
from jax import lax
from jax.experimental import pallas as pl
from jax.experimental.pallas import tpu as pltpu
from jax.sharding import PartitionSpec as P

ITERS = 3
LANES = 128
ROWS = 8
AXES = ("gx", "gy", "gz")
MESH = pl.DeviceIdType.MESH

bonds = [o for o in itertools.product((-1, 0, 1), repeat=3) if o > (0, 0, 0)]
NB = len(bonds)
ahead_runs = [(1, 3), (10, 3)]
behind_runs = [(4, 3)]
assert all(bonds[k][1] == 1 for at, n in ahead_runs for k in range(at, at + n))
assert all(bonds[k][1] == -1 for at, n in behind_runs for k in range(at, at + n))


class Plan:
    def __init__(self, block, orb, cols, peers):
        self.X, self.Y, self.Z = block
        self.O, self.cols = orb, cols
        self.nx, self.ny, self.nz = peers
        self.S = self.nx * self.nz
        self.l = self.X * self.Z
        self.L = self.S * self.l
        self.G = LANES // self.l
        self.Cw = cols // self.S
        self.YO = self.Y * orb
        self.HL = self.YO * self.l
        self.HT = self.HL // LANES
        self.H = cols // LANES
        self.JT = LANES // (self.Y * self.l)
        self.tiles = orb * orb // self.JT
        self.CR = (NB + 1) * self.tiles
        self.OC = orb * self.Cw
        edge = sum(n for _, n in ahead_runs + behind_runs)
        self.HR = (-(-edge // (LANES // (self.JT * self.l))) + 1) * ROWS
        assert self.H * orb == ROWS
        assert self.tiles == ROWS and self.S % self.G == 0 and self.Cw % ROWS == 0


def kernel(plan, rs_hbm, bb_hbm, open_hbm, onsite_hbm, level_hbm, shift_hbm, BT, FX,
           RS, BB, open_ref, onsite_ref, level_ref, shift_ref, PM, LH, T, YB, ZC, HS, HC, RB, CS, CR, M, MB, V, VS, SB, EM, SR, TG,
           in_sem, a_s, a_r, c_s, c_r, hv_s, hv_r, hm_s, hm_r, ho_s, ho_r, th_s, th_r, y_s, y_r, e_s, e_r):
    p = plan
    X, Y, Z, O, S, L, l, G, Cw, H, OC = p.X, p.Y, p.Z, p.O, p.S, p.L, p.l, p.G, p.Cw, p.H, p.OC
    f32 = jnp.float32
    ax, ay, az = (lax.axis_index(name) for name in AXES)
    me = ax * p.nz + az
    pending = []

    def mate(r):
        d = lax.rem(me + r, S)
        return d, (lax.div(d, p.nz), ay, lax.rem(d, p.nz))

    def source(r):
        return lax.rem(me + (S - r), S)

    def along(r):
        return (ax, lax.rem(ay + (r % p.ny), p.ny), az)

    def send(src, dst, ssem, rsem, device):
        copy = pltpu.make_async_remote_copy(
            src_ref=src, dst_ref=dst, send_sem=ssem, recv_sem=rsem, device_id=device, device_id_type=MESH
        )
        copy.start()
        pending.append(copy)
        return copy

    barrier = pltpu.get_barrier_semaphore()
    for r in range(1, S):
        pl.semaphore_signal(barrier, inc=1, device_id=mate(r)[1], device_id_type=MESH)
    for r in range(1, p.ny):
        pl.semaphore_signal(barrier, inc=1, device_id=along(r), device_id_type=MESH)

    loads = []
    for x in range(X):
        for y in range(Y):
            n = Z * H * O
            copy = pltpu.make_async_copy(
                rs_hbm.at[x, y], RS.at[pl.ds((y * X + x) * n, n)], in_sem.at[x * Y + y])
            copy.start()
            loads.append(copy)
    small_loads = []
    for n, (src, dst) in enumerate(((onsite_hbm, onsite_ref), (level_hbm, level_ref), (bb_hbm, BB),
                                    (open_hbm, open_ref), (shift_hbm, shift_ref))):
        copy = pltpu.make_async_copy(src, dst, in_sem.at[X * Y + n])
        copy.start()
        small_loads.append(copy)

    lane = lax.broadcasted_iota(jnp.int32, (1, L), 1)
    lane128 = lax.broadcasted_iota(jnp.int32, (1, LANES), 1)

    def roll(v, by):
        by = by % v.shape[1]
        return v if by == 0 else pltpu.roll(v, by, 1)

    zg = ((lane // l) & (p.nz - 1)) * Z + (lane & (Z - 1))
    xg = (lane // (l * p.nz)) * X + ((lane // Z) & (X - 1))
    row_of = lax.broadcasted_iota(jnp.int32, (L, L), 0)

    def place(sx, sz):
        n = (sx + 1) * 3 + sz + 1
        return n - (n > 4)

    def make_shifts():
        for sx in (-1, 0, 1):
            for sz in (-1, 0, 1):
                if (sx, sz) == (0, 0):
                    continue
                x_to, z_to = (xg + sx) & (p.nx * X - 1), (zg + sz) & (p.nz * Z - 1)
                from_lane = ((x_to // X) * p.nz + z_to // Z) * l + (x_to & (X - 1)) * Z + (z_to & (Z - 1))
                matrix = jnp.where(row_of == from_lane, 1.0, 0.0).astype(jnp.bfloat16)
                at = place(sx, sz) * L
                PM[0:L, at:at + L] = matrix
                PM[L:2 * L, at:at + L] = matrix

    def halves(v):
        high = v.astype(jnp.bfloat16)
        low = (v - high.astype(f32)).astype(jnp.bfloat16)
        return jnp.concatenate([high, low], axis=1)

    block_of = lane128 // l

    def butterfly(arrays):
        arrays = list(arrays)
        m = 1
        while m < G:
            low = (block_of & m) == 0
            for a in range(G):
                if a & m == 0:
                    b = a | m
                    first, second = arrays[a], arrays[b]
                    arrays[a] = jnp.where(low, first, roll(second, m * l))
                    arrays[b] = jnp.where(low, roll(first, -m * l), second)
            m *= 2
        return arrays

    for copy in loads:
        copy.wait()
    step = H * O
    order = list(range(1, Y - 1)) + [0, Y - 1]

    def group(n):
        return order[n // O], n % O

    for h in range(H):
        rows = jnp.concatenate([
            RS[pl.ds(y * X * Z * step + h * O + o, l, stride=step), :] for y in order for o in range(O)
        ], axis=0)
        T[h * LANES:(h + 1) * LANES, :] = jnp.transpose(rows)
    BT[0] = RS[...]
    make_shifts()
    pl.semaphore_wait(barrier, S - 1 + p.ny - 1)
    field_copies = []
    for r in range(1, S):
        d, device = mate(r)
        field_copies.append(send(
            T.at[pl.ds(pl.multiple_of(d * Cw, ROWS), Cw)], RB.at[me], a_s.at[r - 1], a_r.at[r - 1], device))
    RB[me] = T[pl.ds(pl.multiple_of(me * Cw, ROWS), Cw), :]

    def spread_z(block):
        n = block.shape[0]
        out = jnp.zeros((n, LANES), f32)
        for z in range(Z):
            out = jnp.where((lane128 & (Z - 1)) == z, block[:, z:z + 1], out)
        row = lax.broadcasted_iota(jnp.int32, (n, LANES), 0)
        col = lax.broadcasted_iota(jnp.int32, (n, LANES), 1)
        x_row, y_row = (row // Y) & (X - 1), row & (Y - 1)
        x_col, y_col = (col // Z) & (X - 1), (col // l) & (Y - 1)
        return jnp.where((x_row == x_col) & (y_row == y_col), out, 0.0)

    for copy in small_loads[0:2]:
        copy.wait()
    onsite = spread_z(onsite_ref[...])
    level = spread_z(level_ref[...])
    XY = X * Y
    pair = [jnp.sum(onsite[n * XY:(n + 1) * XY], axis=0, keepdims=True) for n in range(O * O)]
    diagonal = [jnp.sum(level[n * XY:(n + 1) * XY], axis=0, keepdims=True) for n in range(O)]
    j_low = lane128 // (Y * l)
    diagonal_sum = jnp.zeros((1, LANES), f32)
    for i in range(O):
        for jh in range(O // p.JT):
            line = jnp.zeros((1, LANES), f32)
            for jl in range(p.JT):
                j = jh * p.JT + jl
                term = 0.5 * (pair[i * O + j] + pair[j * O + i])
                if i == j:
                    term = term + diagonal[i]
                    diagonal_sum = diagonal_sum + jnp.where(j_low == 0, term, 0.0)
                line = jnp.where(j_low == jl, term, line)
            row = NB * ROWS + i * (O // p.JT) + jh
            CS[row:row + 1, :] = line

    diagonal_sum = jnp.sum(diagonal_sum, axis=1, keepdims=True)
    for copy in small_loads[2:]:
        copy.wait()
    is_open = open_ref[...].astype(f32)
    is_open = jnp.concatenate([is_open] * p.JT, axis=0)
    x_of, y_of = (lane128 // (Y * Z)) & (X - 1), (lane128 // Z) & (Y - 1)
    x_to, y_to = (lane128 // Z) & (X - 1), (lane128 // (X * Z)) & (Y - 1)
    source_lane = (lane128 & (Z - 1)) + x_to * (Y * Z) + y_to * Z + j_low * (Y * l)
    gaps = sorted({(x * Y * Z + y * Z) - (y * X * Z + x * Z) for x in range(X) for y in range(Y)})
    for t in range(p.tiles):
        block = BB[t * LANES:(t + 1) * LANES, :] * is_open
        block = jnp.concatenate([block, jnp.zeros((LANES, LANES - NB), f32)], axis=1)
        block = jnp.transpose(block)[0:2 * ROWS, :]
        out = block
        for gap in gaps:
            if gap:
                out = jnp.where(source_lane - lane128 == gap, roll(block, -gap), out)
        CS[pl.ds(t, NB, stride=ROWS), :] = out[0:NB, :]
    early_halo = []
    for n, (run, way) in enumerate([(run, 1) for run in ahead_runs] + [(run, -1) for run in behind_runs]):
        early_halo.append(send(
            CS.at[pl.ds(run[0] * ROWS, run[1] * ROWS)], ZC.at[n], hm_s.at[n], hm_r.at[n], along(way)))
    TG[ay] = jnp.broadcast_to(diagonal_sum, (ROWS, LANES))
    early_halo += [
        send(TG.at[ay], TG.at[ay], th_s.at[r - 1], th_r.at[r - 1], along(r)) for r in range(1, p.ny)]
    partner = (ax + 1 - 2 * lax.rem(ax, 2), ay, az)
    even = [(dx, dz) for dz in range(p.nz) for dx in range(0, p.nx, 2) if (dx, dz) != (0, 0)]
    coef_copies = []
    for n, (dx, dz) in enumerate(even):
        device = (lax.rem(ax + dx, p.nx), ay, lax.rem(az + dz, p.nz))
        coef_copies.append(send(CS, CR.at[me], c_s.at[n], c_r.at[n], device))
    relays = [send(CS, CR.at[me], c_s.at[len(even)], c_r.at[len(even)], partner)]
    CR[me] = CS[...]

    def halo_field(m):
        return [
            send(V.at[m, 1], V.at[m, Y + 1], hv_s.at[m, 0], hv_r.at[m, 0], along(-1)),
            send(V.at[m, Y], V.at[m, 0], hv_s.at[m, 1], hv_r.at[m, 1], along(1)),
        ]

    def arrived(copies):
        for copy in copies:
            copy.wait_recv()

    def spread_field(m, slots):
        rows = len(slots) * OC
        for n, slot in enumerate(slots):
            LH[n * OC:(n + 1) * OC, :] = halves(V[m, slot])
        for n in range(0, 8, 2):
            at = slice(n * L, (n + 2) * L)
            moved = jnp.dot(LH[0:rows, :], PM[:, at], preferred_element_type=f32)
            for q, slot in enumerate(slots):
                VS[slot, :, at] = moved[q * OC:(q + 1) * OC]

    arrived(field_copies)
    for t in range(p.HT):
        for first in range(0, S, G):
            blocks = butterfly([RB[first + n, :, t * LANES:(t + 1) * LANES] for n in range(G)])
            at = first // G * LANES
            for n in range(G):
                y, o = group(t * G + n)
                V[0, y + 1, o * Cw:(o + 1) * Cw, at:at + LANES] = blocks[n]
    halo = halo_field(0)

    arrived(early_halo)
    outer = [(n, q, run[0] + q, slot, y) for n, (run, slot, y) in enumerate(
        [(run, 0, Y - 1) for run in ahead_runs] + [(run, Y + 1, 0) for run in behind_runs]) for q in range(run[1])]
    unit = p.JT * l
    U = LANES // unit
    for v in range(0, len(outer), U):
        packed = jnp.zeros((ROWS, LANES), f32)
        for q, (n, at, k, slot, y) in enumerate(outer[v:v + U]):
            block = ZC[n, at * ROWS:(at + 1) * ROWS, :]
            for jl in range(p.JT):
                to = q * unit + jl * l
                packed = jnp.where(block_of == to // l, roll(block, to - jl * Y * l - y * l), packed)
        HS[v // U * ROWS:(v // U + 1) * ROWS, :] = packed
    part = TG[0]
    for n in range(1, p.ny):
        part = part + TG[n]
    HS[p.HR - ROWS:p.HR, :] = part
    outer_copies = []
    for r in range(1, S):
        d, device = mate(r)
        outer_copies.append(send(HS, HC.at[me], ho_s.at[r - 1], ho_r.at[r - 1], device))
    HC[me] = HS[...]
    spread_field(0, range(1, Y + 1))

    def take_outer():
        arrived(outer_copies)
        for first in range(0, S, G):
            blocks = butterfly([HC[first + n, 0:p.HR - ROWS, :] for n in range(G)])
            at = first // G * LANES
            for n, (_, _, k, slot, y) in enumerate(outer):
                v, q = divmod(n, U)
                for jl in range(p.JT):
                    M[jl, slot, k * ROWS:(k + 1) * ROWS, at:at + LANES] = (
                        blocks[q * p.JT + jl][v * ROWS:(v + 1) * ROWS])
        mirror(False)
        total = HC[0, p.HR - ROWS:p.HR - ROWS + 1, 0:1]
        for n in range(1, S):
            total = total + HC[n, p.HR - ROWS:p.HR - ROWS + 1, 0:1]
        return total * (1.0 / (p.ny * Y * L * O))

    for n, (dx, dz) in enumerate(even):
        coef_copies[n].wait_recv()
        s = lax.rem(ax + (p.nx - dx), p.nx) * p.nz + lax.rem(az + (p.nz - dz), p.nz)
        at = len(even) + 1 + n
        relays.append(send(CR.at[s], CR.at[s], c_s.at[at], c_r.at[at], partner))
    arrived(relays)
    for first in range(0, S, G):
        blocks = butterfly([CR[first + n] for n in range(G)])
        at = first // G * LANES
        for n in range(G):
            jl, y = divmod(n, Y)
            M[jl, y + 1, :, at:at + LANES] = blocks[n]
    HALFJ = O // p.JT

    def inside(y):
        return 0 <= y < Y

    def mirror(within):
        groups = {}
        for k, o in enumerate(bonds):
            for y in range(Y):
                if inside(y - o[1]) == within:
                    groups.setdefault((-o[0], -o[2]), []).extend((k, jl, y) for jl in range(p.JT))
        for (sx, sz), members in groups.items():
            blocks = [M[jl, y + 1 - bonds[k][1], k * ROWS:(k + 1) * ROWS, :] for k, jl, y in members]
            if (sx, sz) != (0, 0):
                at = place(sx, sz) * L
                moved = jnp.dot(halves(jnp.concatenate(blocks, axis=0)), PM[:, at:at + L], preferred_element_type=f32)
                blocks = [moved[n * ROWS:(n + 1) * ROWS] for n in range(len(members))]
            for (k, jl, y), block in zip(members, blocks):
                MB[k, jl, y] = block

    mirror(True)

    def add_bonds(acc, m, y, steps):
        for k, o in enumerate(bonds):
            for sign in (1, -1):
                if sign * o[1] not in steps:
                    continue
                slot = y + 1 + sign * o[1]
                sx, sz = sign * o[0], sign * o[2]
                for j in range(O):
                    rows = slice(j * Cw, (j + 1) * Cw)
                    at = place(sx, sz) * L
                    v = V[m, slot, rows, :] if (sx, sz) == (0, 0) else VS[slot, rows, at:at + L]
                    for i in range(O):
                        if sign > 0:
                            row = k * ROWS + i * HALFJ + j // p.JT
                            c = M[j % p.JT, y + 1, row:row + 1, :]
                        else:
                            row = j * HALFJ + i // p.JT
                            c = MB[k, i % p.JT, y, row:row + 1, :]
                        acc[i] = acc[i] + c * v

    def add_onsite(acc, m, y, theta):
        for j in range(O):
            v = V[m, y + 1, j * Cw:(j + 1) * Cw, :]
            for i in range(O):
                row = NB * ROWS + i * HALFJ + j // p.JT
                c = M[j % p.JT, y + 1, row:row + 1, :]
                if i == j:
                    c = c - theta
                acc[i] = acc[i] + c * v

    def put(acc, m, y):
        for i in range(O):
            V[m, y + 1, i * Cw:(i + 1) * Cw, :] = acc[i]

    def take(m, y):
        return [V[m, y + 1, i * Cw:(i + 1) * Cw, :] for i in range(O)]

    def zeros():
        return [jnp.zeros((Cw, L), f32) for _ in range(O)]

    def moment(a, b):
        total = jnp.zeros((Cw, L), f32)
        for y in range(Y):
            for i in range(O):
                rows = slice(i * Cw, (i + 1) * Cw)
                total = total + V[a, y + 1, rows, :] * V[b, y + 1, rows, :]
        return jnp.sum(total, axis=1, keepdims=True)

    moments = []
    home_copies = {}

    everyone = [(g, r) for g in range(p.ny) for r in range(S) if (g, r) != (0, 0)]

    def tell(part, values):
        sublane = lax.broadcasted_iota(jnp.int32, (Cw, LANES), 0)
        spot = lax.broadcasted_iota(jnp.int32, (Cw, LANES), 1)
        table = jnp.zeros((Cw, LANES), f32)
        for n, value in enumerate(values):
            table = jnp.where(spot == sublane + n * Cw, value, table)
        line = jnp.sum(table, axis=0, keepdims=True)
        EM[part, ay, me] = line
        SR[part] = line
        copies = []
        for n, (g, r) in enumerate(everyone):
            d = lax.rem(me + r, S)
            device = (lax.div(d, p.nz), lax.rem(ay + g, p.ny), lax.rem(d, p.nz))
            copies.append(send(SR.at[part], EM.at[part, ay, me], e_s.at[part, n], e_r.at[part, n], device))
        return copies

    def go_home(m, t):
        for first in range(0, S, G):
            at = first // G * LANES
            blocks = []
            for n in range(G):
                y, o = group(t * G + n)
                blocks.append(V[m, y + 1, o * Cw:(o + 1) * Cw, at:at + LANES])
            blocks = butterfly(blocks)
            for n in range(G):
                SB[m - 1, t, first + n] = blocks[n]
        mine = pl.ds(pl.multiple_of(me * Cw, ROWS), Cw)
        copies = home_copies.setdefault(m, [])
        for r in range(1, S):
            d, device = mate(r)
            copies.append(send(SB.at[m - 1, t, d], YB.at[m - 1, t, mine],
                               y_s.at[m - 1, t, r - 1], y_r.at[m - 1, t, r - 1], device))
        YB[m - 1, t, mine] = SB[m - 1, t, me]

    theta = None
    for m in range(ITERS):
        if m > 0:
            M[0, 0, 0:ROWS, :] = jnp.zeros((ROWS, L), f32)
            MB[NB, 0, 0] = jnp.zeros((ROWS, L), f32)
            spread_field(m, range(1, Y + 1))
        for y in range(Y):
            acc = zeros()
            add_bonds(acc, m, y, [s for s in (-1, 0, 1) if inside(y + s)])
            put(acc, m + 1, y)
        if m == 0:
            moments.append(moment(0, 0))
            theta = take_outer()
        for y in range(1, Y - 1):
            acc = take(m + 1, y)
            add_onsite(acc, m, y, theta)
            put(acc, m + 1, y)
        if m + 1 == ITERS:
            go_home(ITERS, 0)
        arrived(halo)
        spread_field(m, (0, Y + 1))
        for y, s in ((0, -1), (Y - 1, 1)):
            acc = take(m + 1, y)
            add_bonds(acc, m, y, [s])
            add_onsite(acc, m, y, theta)
            put(acc, m + 1, y)
        if m + 1 < ITERS:
            halo = halo_field(m + 1)
        for t in range(1 if m + 1 == ITERS else 0, p.HT if m + 1 < ITERS else 1):
            go_home(m + 1, t)
        moments.append(moment(m, m + 1))
        if m + 1 < ITERS:
            moments.append(moment(m + 1, m + 1))
        if m + 2 == ITERS:
            early = len(moments) - 1
            told = tell(0, moments[:early])
    told = told + tell(1, moments[early:])
    for t in range(1, p.HT):
        go_home(ITERS, t)

    shift = jnp.concatenate([
        roll(shift_ref[:, d * Cw // LANES * LANES:(d * Cw // LANES + 1) * LANES], -(d * Cw % LANES)) for d in range(S)
    ], axis=0) + theta

    def turn_home(n):
        arrived(home_copies[n + 1])
        for h in range(H):
            for t in range(p.HT):
                field = jnp.transpose(YB[n, t, h * LANES:(h + 1) * LANES, :])
                for q in range(G):
                    y, o = group(t * G + q)
                    BT[n + 1, pl.ds(y * X * Z * step + h * O + o, l, stride=step), :] = field[q * l:(q + 1) * l, :]

    for n in range(ITERS):
        turn_home(n)
    arrived(told)

    def total(part):
        rows = []
        for d in range(S):
            line = EM[part, 0, d]
            for n in range(1, p.ny):
                line = line + EM[part, n, d]
            rows.append(line)
        return jnp.concatenate(rows, axis=0)

    sums = [total(0), total(1)]
    m_of = [roll(sums[n >= early], -(n - early * (n >= early)) * Cw) for n in range(2 * ITERS)]

    def inner(u, v):
        out = None
        for a, first in enumerate(u):
            for b, second in enumerate(v):
                term = first * second * m_of[a + b]
                out = term if out is None else out + term
        return out

    def plus(u, v, factor):
        n = max(len(u), len(v))
        out = []
        for a in range(n):
            if a < len(v):
                term = factor * v[a]
                out.append(u[a] + term if a < len(u) else term)
            else:
                out.append(u[a])
        return out

    one = jnp.ones((S, LANES), f32)
    answer, residual, direction, norm = [], [one], [one], m_of[0]
    for turn in range(ITERS):
        image = [shift * direction[0]]
        for a in range(1, len(direction)):
            image.append(direction[a - 1] + shift * direction[a])
        image.append(direction[-1])
        alpha = norm / inner(direction, image)
        answer = plus(answer, direction, alpha)
        residual = plus(residual, image, -alpha)
        if turn + 1 < ITERS:
            fresh = inner(residual, residual)
            direction = plus(residual, direction, fresh / norm)
            norm = fresh
    factors = answer + residual
    per = LANES // Cw
    half = lax.broadcasted_iota(jnp.int32, (H * O, LANES), 0) // O
    for n, factor in enumerate(factors):
        turned = [roll(factor, q * Cw) for q in range(per)]
        block = jnp.zeros((H * O, LANES), f32)
        for h in range(H):
            line = turned[0][h * per:h * per + 1]
            for q in range(1, per):
                line = jnp.where(lane128 // Cw == q, turned[q][h * per + q:h * per + q + 1], line)
            block = jnp.where(half == h, line, block)
        FX[n] = block
    for copy in pending:
        copy.wait_send()


def combine(plan, BT, FX, sol_hbm, res_hbm, OS, sem):
    p = plan
    X, Y, n = p.X, p.Y, p.Z * p.H * p.O
    group = p.H * p.O
    outs = []
    for which, hbm in ((0, sol_hbm), (1, res_hbm)):
        for y in range(Y):
            for x in range(X):
                base = (y * X + x) * n
                for at in range(base, base + n, group):
                    rows = slice(at, at + group)
                    field = FX[which * ITERS] * BT[0, rows, :]
                    for q in range(1, ITERS + which):
                        field = field + FX[which * ITERS + q] * BT[q, rows, :]
                    OS[which, rows, :] = field
        for x in range(X):
            for y in range(Y):
                copy = pltpu.make_async_copy(
                    OS.at[which, pl.ds((y * X + x) * n, n)], hbm.at[x, y], sem.at[(which * X + x) * Y + y])
                copy.start()
                outs.append(copy)
    for copy in outs:
        copy.wait()


def per_device(peers, right_side, bond_blocks, bond_open, onsite_blocks, orbital_levels, column_shift):
    block, orb, cols = right_side.shape[:3], right_side.shape[3], right_side.shape[4]
    p = Plan(block, orb, cols, peers)
    X, Y, Z, O, S, L, H = p.X, p.Y, p.Z, p.O, p.S, p.L, p.H
    f32 = jnp.float32
    right = right_side.reshape(X, Y, Z, O, H, LANES).transpose(0, 1, 2, 4, 3, 5).reshape(X, Y, Z * H * O, LANES)
    blocks = jnp.transpose(bond_blocks, (1, 2, 3, 4, 5, 0)).reshape(O * O * X * Y * Z, NB)
    opened = jnp.transpose(bond_open, (1, 2, 3, 0)).reshape(X * Y * Z, NB)
    onsite = onsite_blocks.reshape(O * O * X * Y, Z)
    levels = orbital_levels.reshape(O * X * Y, Z)
    dma = pltpu.SemaphoreType.DMA
    vmem, anywhere = pl.BlockSpec(memory_space=pltpu.VMEM), pl.BlockSpec(memory_space=pl.ANY)

    def scratch(*shape):
        return pltpu.VMEM(shape, f32)

    flat = (p.cols, p.HL)
    made = pl.pallas_call(
        functools.partial(kernel, p),
        out_shape=(scratch(ITERS + 1, X * Y * Z * H * O, LANES), scratch(2 * ITERS + 1, H * O, LANES)),
        in_specs=[pl.BlockSpec(memory_space=pltpu.HBM)] * 6,
        out_specs=(vmem,) * 2,
        scratch_shapes=[
            scratch(X * Y * Z * H * O, LANES),
            scratch(O * O * X * Y * Z, NB),
            pltpu.VMEM(opened.shape, jnp.int32),
            scratch(*onsite.shape),
            scratch(*levels.shape),
            scratch(1, cols),
            pltpu.VMEM((2 * L, 8 * L), jnp.bfloat16),
            pltpu.VMEM((Y * p.OC, 2 * L), jnp.bfloat16),
            scratch(*flat),
            scratch(ITERS, p.HT, cols, LANES),
            scratch(3, 3 * ROWS, LANES),
            scratch(p.HR, LANES),
            scratch(S, p.HR, LANES),
            scratch(S, p.Cw, p.HL),
            scratch(p.CR, LANES),
            scratch(S, p.CR, LANES),
            scratch(p.JT, Y + 2, p.CR, L),
            scratch(NB + 1, p.JT, Y, ROWS, L),
            scratch(ITERS + 1, Y + 2, p.OC, L),
            scratch(Y + 2, p.OC, 8 * L),
            scratch(ITERS, p.HT, S, p.Cw, LANES),
            scratch(2, p.ny, S, 1, LANES),
            scratch(2, 1, LANES),
            scratch(p.ny, ROWS, LANES),
            dma((X * Y + 5,)),
            dma((S - 1,)), dma((S - 1,)), dma((S - 1,)), dma((S - 1,)),
            dma((ITERS, 2)), dma((ITERS, 2)), dma((3,)), dma((3,)),
            dma((S - 1,)), dma((S - 1,)),
            dma((p.ny - 1,)), dma((p.ny - 1,)),
            dma((ITERS, p.HT, S - 1)), dma((ITERS, p.HT, S - 1)),
            dma((2, p.ny * S - 1)), dma((2, p.ny * S - 1)),
        ],
        compiler_params=pltpu.CompilerParams(
            collective_id=0, has_side_effects=True, vmem_limit_bytes=40 * 1024 * 1024
        ),
    )(*(pltpu.with_memory_space_constraint(v, pltpu.HBM)
        for v in (right, blocks, opened, onsite, levels, column_shift[None])))
    outs = pl.pallas_call(
        functools.partial(combine, p),
        out_shape=(jax.ShapeDtypeStruct(right.shape, f32),) * 2,
        in_specs=[vmem] * 2,
        out_specs=(anywhere, anywhere),
        scratch_shapes=[scratch(2, X * Y * Z * H * O, LANES), dma((2 * X * Y,))],
        compiler_params=pltpu.CompilerParams(vmem_limit_bytes=16 * 1024 * 1024),
    )(*made)

    def back(v):
        return v.reshape(X, Y, Z, H, O, LANES).transpose(0, 1, 2, 4, 3, 5).reshape(right_side.shape)

    return back(outs[0]), back(outs[1])


def solution(mesh):
    field = P("gx", "gy", "gz", None, None)
    placed = (
        field,
        P(None, None, None, "gx", "gy", "gz"),
        P(None, "gx", "gy", "gz"),
        P(None, None, "gx", "gy", "gz"),
        P(None, "gx", "gy", "gz"),
        P(),
    )
    return jax.shard_map(
        functools.partial(per_device, tuple(mesh.shape[name] for name in AXES)),
        mesh=mesh,
        in_specs=placed,
        out_specs=(field, field),
        check_vma=False,
    )
```

```python
import functools
import itertools

import jax
import jax.numpy as jnp
from jax import lax
from jax.experimental import pallas as pl
from jax.experimental.pallas import tpu as pltpu
from jax.sharding import PartitionSpec as P

ITERS = 3
LANES = 128
ROWS = 8
AXES = ("gx", "gy", "gz")
MESH = pl.DeviceIdType.MESH

bonds = [o for o in itertools.product((-1, 0, 1), repeat=3) if o > (0, 0, 0)]
NB = len(bonds)
ahead_runs = [(1, 3), (10, 3)]
behind_runs = [(4, 3)]
assert all(bonds[k][1] == 1 for at, n in ahead_runs for k in range(at, at + n))
assert all(bonds[k][1] == -1 for at, n in behind_runs for k in range(at, at + n))


class Plan:
    def __init__(self, block, orb, cols, peers):
        self.X, self.Y, self.Z = block
        self.O, self.cols = orb, cols
        self.nx, self.ny, self.nz = peers
        self.S = self.nx * self.nz
        self.l = self.X * self.Z
        self.L = self.S * self.l
        self.G = LANES // self.l
        self.Cw = cols // self.S
        self.YO = self.Y * orb
        self.HL = self.YO * self.l
        self.HT = self.HL // LANES
        self.H = cols // LANES
        self.JT = LANES // (self.Y * self.l)
        self.tiles = orb * orb // self.JT
        self.CR = (NB + 1) * self.tiles
        self.NG = 2 if self.Cw % (2 * ROWS) == 0 else 1
        self.Cg = self.Cw // self.NG
        self.OC = orb * self.Cg
        edge = sum(n for _, n in ahead_runs + behind_runs)
        self.HR = (-(-edge // (LANES // (self.JT * self.l))) + 1) * ROWS
        assert self.H * orb == ROWS
        assert self.tiles == ROWS and self.S % self.G == 0 and self.Cw % ROWS == 0


def kernel(plan, rs_hbm, bb_hbm, open_hbm, onsite_hbm, level_hbm, shift_hbm, BT, FX,
           RS, BB, open_ref, onsite_ref, level_ref, shift_ref, PM, LH, T, YB, ZC, HS, HC, RB, CS, CR, M, MB, V, VS, SB, EM, SR, TG,
           in_sem, a_s, a_r, c_s, c_r, hv_s, hv_r, hm_s, hm_r, ho_s, ho_r, th_s, th_r, y_s, y_r, e_s, e_r):
    p = plan
    X, Y, Z, O, S, L, l, G, Cw, H, OC = p.X, p.Y, p.Z, p.O, p.S, p.L, p.l, p.G, p.Cw, p.H, p.OC
    NG, Cg = p.NG, p.Cg
    f32 = jnp.float32
    ax, ay, az = (lax.axis_index(name) for name in AXES)
    me = ax * p.nz + az
    pending = []

    def mate(r):
        d = lax.rem(me + r, S)
        return d, (lax.div(d, p.nz), ay, lax.rem(d, p.nz))

    def source(r):
        return lax.rem(me + (S - r), S)

    def along(r):
        return (ax, lax.rem(ay + (r % p.ny), p.ny), az)

    def send(src, dst, ssem, rsem, device):
        copy = pltpu.make_async_remote_copy(
            src_ref=src, dst_ref=dst, send_sem=ssem, recv_sem=rsem, device_id=device, device_id_type=MESH
        )
        copy.start()
        pending.append(copy)
        return copy

    barrier = pltpu.get_barrier_semaphore()
    for r in range(1, S):
        pl.semaphore_signal(barrier, inc=1, device_id=mate(r)[1], device_id_type=MESH)
    for r in range(1, p.ny):
        pl.semaphore_signal(barrier, inc=1, device_id=along(r), device_id_type=MESH)

    loads = []
    for x in range(X):
        for y in range(Y):
            n = Z * H * O
            copy = pltpu.make_async_copy(
                rs_hbm.at[x, y], RS.at[pl.ds((y * X + x) * n, n)], in_sem.at[x * Y + y])
            copy.start()
            loads.append(copy)
    small_loads = []
    for n, (src, dst) in enumerate(((onsite_hbm, onsite_ref), (level_hbm, level_ref), (bb_hbm, BB),
                                    (open_hbm, open_ref), (shift_hbm, shift_ref))):
        copy = pltpu.make_async_copy(src, dst, in_sem.at[X * Y + n])
        copy.start()
        small_loads.append(copy)

    lane = lax.broadcasted_iota(jnp.int32, (1, L), 1)
    lane128 = lax.broadcasted_iota(jnp.int32, (1, LANES), 1)

    def roll(v, by):
        by = by % v.shape[1]
        return v if by == 0 else pltpu.roll(v, by, 1)

    zg = ((lane // l) & (p.nz - 1)) * Z + (lane & (Z - 1))
    xg = (lane // (l * p.nz)) * X + ((lane // Z) & (X - 1))
    row_of = lax.broadcasted_iota(jnp.int32, (L, L), 0)

    def place(sx, sz):
        n = (sx + 1) * 3 + sz + 1
        return n - (n > 4)

    def make_shifts():
        for sx in (-1, 0, 1):
            for sz in (-1, 0, 1):
                if (sx, sz) == (0, 0):
                    continue
                x_to, z_to = (xg + sx) & (p.nx * X - 1), (zg + sz) & (p.nz * Z - 1)
                from_lane = ((x_to // X) * p.nz + z_to // Z) * l + (x_to & (X - 1)) * Z + (z_to & (Z - 1))
                matrix = jnp.where(row_of == from_lane, 1.0, 0.0).astype(jnp.bfloat16)
                at = place(sx, sz) * L
                PM[0:L, at:at + L] = matrix
                PM[L:2 * L, at:at + L] = matrix

    def halves(v):
        high = v.astype(jnp.bfloat16)
        low = (v - high.astype(f32)).astype(jnp.bfloat16)
        return jnp.concatenate([high, low], axis=1)

    block_of = lane128 // l

    def butterfly(arrays):
        arrays = list(arrays)
        m = 1
        while m < G:
            low = (block_of & m) == 0
            for a in range(G):
                if a & m == 0:
                    b = a | m
                    first, second = arrays[a], arrays[b]
                    arrays[a] = jnp.where(low, first, roll(second, m * l))
                    arrays[b] = jnp.where(low, roll(first, -m * l), second)
            m *= 2
        return arrays

    for copy in loads:
        copy.wait()
    step = H * O
    order = list(range(1, Y - 1)) + [0, Y - 1]

    def group(n):
        return order[n // O], n % O

    for h in range(H):
        rows = jnp.concatenate([
            RS[pl.ds(y * X * Z * step + h * O + o, l, stride=step), :] for y in order for o in range(O)
        ], axis=0)
        T[h * LANES:(h + 1) * LANES, :] = jnp.transpose(rows)
    BT[0] = RS[...]
    make_shifts()
    pl.semaphore_wait(barrier, S - 1 + p.ny - 1)
    field_copies = []
    for r in range(1, S):
        d, device = mate(r)
        field_copies.append(send(
            T.at[pl.ds(pl.multiple_of(d * Cw, ROWS), Cw)], RB.at[me], a_s.at[r - 1], a_r.at[r - 1], device))
    RB[me] = T[pl.ds(pl.multiple_of(me * Cw, ROWS), Cw), :]

    def spread_z(block):
        n = block.shape[0]
        out = jnp.zeros((n, LANES), f32)
        for z in range(Z):
            out = jnp.where((lane128 & (Z - 1)) == z, block[:, z:z + 1], out)
        row = lax.broadcasted_iota(jnp.int32, (n, LANES), 0)
        col = lax.broadcasted_iota(jnp.int32, (n, LANES), 1)
        x_row, y_row = (row // Y) & (X - 1), row & (Y - 1)
        x_col, y_col = (col // Z) & (X - 1), (col // l) & (Y - 1)
        return jnp.where((x_row == x_col) & (y_row == y_col), out, 0.0)

    for copy in small_loads[0:2]:
        copy.wait()
    onsite = spread_z(onsite_ref[...])
    level = spread_z(level_ref[...])
    XY = X * Y
    pair = [jnp.sum(onsite[n * XY:(n + 1) * XY], axis=0, keepdims=True) for n in range(O * O)]
    diagonal = [jnp.sum(level[n * XY:(n + 1) * XY], axis=0, keepdims=True) for n in range(O)]
    j_low = lane128 // (Y * l)
    diagonal_sum = jnp.zeros((1, LANES), f32)
    for i in range(O):
        for jh in range(O // p.JT):
            line = jnp.zeros((1, LANES), f32)
            for jl in range(p.JT):
                j = jh * p.JT + jl
                term = 0.5 * (pair[i * O + j] + pair[j * O + i])
                if i == j:
                    term = term + diagonal[i]
                    diagonal_sum = diagonal_sum + jnp.where(j_low == 0, term, 0.0)
                line = jnp.where(j_low == jl, term, line)
            row = NB * ROWS + i * (O // p.JT) + jh
            CS[row:row + 1, :] = line

    diagonal_sum = jnp.sum(diagonal_sum, axis=1, keepdims=True)
    for copy in small_loads[2:]:
        copy.wait()
    is_open = open_ref[...].astype(f32)
    is_open = jnp.concatenate([is_open] * p.JT, axis=0)
    x_of, y_of = (lane128 // (Y * Z)) & (X - 1), (lane128 // Z) & (Y - 1)
    x_to, y_to = (lane128 // Z) & (X - 1), (lane128 // (X * Z)) & (Y - 1)
    source_lane = (lane128 & (Z - 1)) + x_to * (Y * Z) + y_to * Z + j_low * (Y * l)
    gaps = sorted({(x * Y * Z + y * Z) - (y * X * Z + x * Z) for x in range(X) for y in range(Y)})
    for t in range(p.tiles):
        block = BB[t * LANES:(t + 1) * LANES, :] * is_open
        block = jnp.concatenate([block, jnp.zeros((LANES, LANES - NB), f32)], axis=1)
        block = jnp.transpose(block)[0:2 * ROWS, :]
        out = block
        for gap in gaps:
            if gap:
                out = jnp.where(source_lane - lane128 == gap, roll(block, -gap), out)
        CS[pl.ds(t, NB, stride=ROWS), :] = out[0:NB, :]
    early_halo = []
    for n, (run, way) in enumerate([(run, 1) for run in ahead_runs] + [(run, -1) for run in behind_runs]):
        early_halo.append(send(
            CS.at[pl.ds(run[0] * ROWS, run[1] * ROWS)], ZC.at[n], hm_s.at[n], hm_r.at[n], along(way)))
    TG[ay] = jnp.broadcast_to(diagonal_sum, (ROWS, LANES))
    early_halo += [
        send(TG.at[ay], TG.at[ay], th_s.at[r - 1], th_r.at[r - 1], along(r)) for r in range(1, p.ny)]
    partner = (ax + 1 - 2 * lax.rem(ax, 2), ay, az)
    even = [(dx, dz) for dz in range(p.nz) for dx in range(0, p.nx, 2) if (dx, dz) != (0, 0)]
    coef_copies = []
    for n, (dx, dz) in enumerate(even):
        device = (lax.rem(ax + dx, p.nx), ay, lax.rem(az + dz, p.nz))
        coef_copies.append(send(CS, CR.at[me], c_s.at[n], c_r.at[n], device))
    relays = [send(CS, CR.at[me], c_s.at[len(even)], c_r.at[len(even)], partner)]
    CR[me] = CS[...]

    def halo_field(m, g):
        return [
            send(V.at[m, 1, g], V.at[m, Y + 1, g], hv_s.at[m, g, 0], hv_r.at[m, g, 0], along(-1)),
            send(V.at[m, Y, g], V.at[m, 0, g], hv_s.at[m, g, 1], hv_r.at[m, g, 1], along(1)),
        ]

    def arrived(copies):
        for copy in copies:
            copy.wait_recv()

    def spread_field(m, slots, g):
        rows = len(slots) * OC
        for n, slot in enumerate(slots):
            LH[g, n * OC:(n + 1) * OC, :] = halves(V[m, slot, g])
        for n in range(0, 8, 2):
            at = slice(n * L, (n + 2) * L)
            moved = jnp.dot(LH[g, 0:rows, :], PM[:, at], preferred_element_type=f32)
            for q, slot in enumerate(slots):
                VS[slot, g, :, at] = moved[q * OC:(q + 1) * OC]

    arrived(field_copies)
    for t in range(p.HT):
        for first in range(0, S, G):
            blocks = butterfly([RB[first + n, :, t * LANES:(t + 1) * LANES] for n in range(G)])
            at = first // G * LANES
            for n in range(G):
                y, o = group(t * G + n)
                for g in range(NG):
                    V[0, y + 1, g, o * Cg:(o + 1) * Cg, at:at + LANES] = blocks[n][g * Cg:(g + 1) * Cg]
    halo = [halo_field(0, g) for g in range(NG)]

    arrived(early_halo)
    outer = [(n, q, run[0] + q, slot, y) for n, (run, slot, y) in enumerate(
        [(run, 0, Y - 1) for run in ahead_runs] + [(run, Y + 1, 0) for run in behind_runs]) for q in range(run[1])]
    unit = p.JT * l
    U = LANES // unit
    for v in range(0, len(outer), U):
        packed = jnp.zeros((ROWS, LANES), f32)
        for q, (n, at, k, slot, y) in enumerate(outer[v:v + U]):
            block = ZC[n, at * ROWS:(at + 1) * ROWS, :]
            for jl in range(p.JT):
                to = q * unit + jl * l
                packed = jnp.where(block_of == to // l, roll(block, to - jl * Y * l - y * l), packed)
        HS[v // U * ROWS:(v // U + 1) * ROWS, :] = packed
    part = TG[0]
    for n in range(1, p.ny):
        part = part + TG[n]
    HS[p.HR - ROWS:p.HR, :] = part
    outer_copies = []
    for r in range(1, S):
        d, device = mate(r)
        outer_copies.append(send(HS, HC.at[me], ho_s.at[r - 1], ho_r.at[r - 1], device))
    HC[me] = HS[...]
    for g in range(NG):
        spread_field(0, range(1, Y + 1), g)

    def take_outer():
        arrived(outer_copies)
        for first in range(0, S, G):
            blocks = butterfly([HC[first + n, 0:p.HR - ROWS, :] for n in range(G)])
            at = first // G * LANES
            for n, (_, _, k, slot, y) in enumerate(outer):
                v, q = divmod(n, U)
                for jl in range(p.JT):
                    M[jl, slot, k * ROWS:(k + 1) * ROWS, at:at + LANES] = (
                        blocks[q * p.JT + jl][v * ROWS:(v + 1) * ROWS])
        mirror(False)
        total = HC[0, p.HR - ROWS:p.HR - ROWS + 1, 0:1]
        for n in range(1, S):
            total = total + HC[n, p.HR - ROWS:p.HR - ROWS + 1, 0:1]
        return total * (1.0 / (p.ny * Y * L * O))

    for n, (dx, dz) in enumerate(even):
        coef_copies[n].wait_recv()
        s = lax.rem(ax + (p.nx - dx), p.nx) * p.nz + lax.rem(az + (p.nz - dz), p.nz)
        at = len(even) + 1 + n
        relays.append(send(CR.at[s], CR.at[s], c_s.at[at], c_r.at[at], partner))
    arrived(relays)
    for first in range(0, S, G):
        blocks = butterfly([CR[first + n] for n in range(G)])
        at = first // G * LANES
        for n in range(G):
            jl, y = divmod(n, Y)
            M[jl, y + 1, :, at:at + LANES] = blocks[n]
    HALFJ = O // p.JT

    def inside(y):
        return 0 <= y < Y

    def mirror(within):
        groups = {}
        for k, o in enumerate(bonds):
            for y in range(Y):
                if inside(y - o[1]) == within:
                    groups.setdefault((-o[0], -o[2]), []).extend((k, jl, y) for jl in range(p.JT))
        for (sx, sz), members in groups.items():
            blocks = [M[jl, y + 1 - bonds[k][1], k * ROWS:(k + 1) * ROWS, :] for k, jl, y in members]
            if (sx, sz) != (0, 0):
                at = place(sx, sz) * L
                moved = jnp.dot(halves(jnp.concatenate(blocks, axis=0)), PM[:, at:at + L], preferred_element_type=f32)
                blocks = [moved[n * ROWS:(n + 1) * ROWS] for n in range(len(members))]
            for (k, jl, y), block in zip(members, blocks):
                MB[k, jl, y] = block

    mirror(True)

    zero = [0, lax.div(ax, p.nx), lax.div(ay, p.ny)]

    def add_bonds(acc, m, y, steps, g):
        for k, o in enumerate(bonds):
            for sign in (1, -1):
                if sign * o[1] not in steps:
                    continue
                slot = y + 1 + sign * o[1]
                sx, sz = sign * o[0], sign * o[2]
                for j in range(O):
                    rows = slice(j * Cg, (j + 1) * Cg)
                    at = place(sx, sz) * L
                    v = V[m, slot, g, rows, :] if (sx, sz) == (0, 0) else VS[slot, g, rows, at:at + L]
                    for i in range(O):
                        if sign > 0:
                            row = k * ROWS + i * HALFJ + j // p.JT
                            c = M[zero[m] + j % p.JT, y + 1, row:row + 1, :]
                        else:
                            row = j * HALFJ + i // p.JT
                            c = MB[zero[m] + k, i % p.JT, y, row:row + 1, :]
                        acc[i] = acc[i] + c * v

    def add_onsite(acc, m, y, theta, g):
        for j in range(O):
            v = V[m, y + 1, g, j * Cg:(j + 1) * Cg, :]
            for i in range(O):
                row = NB * ROWS + i * HALFJ + j // p.JT
                c = M[zero[m] + j % p.JT, y + 1, row:row + 1, :]
                if i == j:
                    c = c - theta
                acc[i] = acc[i] + c * v

    def put(acc, m, y, g):
        for i in range(O):
            V[m, y + 1, g, i * Cg:(i + 1) * Cg, :] = acc[i]

    def take(m, y, g):
        return [V[m, y + 1, g, i * Cg:(i + 1) * Cg, :] for i in range(O)]

    def zeros():
        return [jnp.zeros((Cg, L), f32) for _ in range(O)]

    def moment(a, b):
        sums = []
        for g in range(NG):
            total = jnp.zeros((Cg, L), f32)
            for y in range(Y):
                for i in range(O):
                    rows = slice(i * Cg, (i + 1) * Cg)
                    total = total + V[a, y + 1, g, rows, :] * V[b, y + 1, g, rows, :]
            sums.append(jnp.sum(total, axis=1, keepdims=True))
        return jnp.concatenate(sums, axis=0)

    moments = []
    home_copies = {}

    everyone = [(g, r) for g in range(p.ny) for r in range(S) if (g, r) != (0, 0)]

    def tell(part, values):
        sublane = lax.broadcasted_iota(jnp.int32, (Cw, LANES), 0)
        spot = lax.broadcasted_iota(jnp.int32, (Cw, LANES), 1)
        table = jnp.zeros((Cw, LANES), f32)
        for n, value in enumerate(values):
            table = jnp.where(spot == sublane + n * Cw, value, table)
        line = jnp.sum(table, axis=0, keepdims=True)
        EM[part, ay, me] = line
        SR[part] = line
        copies = []
        for n, (g, r) in enumerate(everyone):
            d = lax.rem(me + r, S)
            device = (lax.div(d, p.nz), lax.rem(ay + g, p.ny), lax.rem(d, p.nz))
            copies.append(send(SR.at[part], EM.at[part, ay, me], e_s.at[part, n], e_r.at[part, n], device))
        return copies

    def go_home(m, tiles):
        for t in tiles:
            for first in range(0, S, G):
                at = first // G * LANES
                blocks = []
                for n in range(G):
                    y, o = group(t * G + n)
                    blocks.append(jnp.concatenate(
                        [V[m, y + 1, g, o * Cg:(o + 1) * Cg, at:at + LANES] for g in range(NG)], axis=0))
                blocks = butterfly(blocks)
                for n in range(G):
                    SB[m - 1, t, first + n] = blocks[n]
        mine = pl.ds(pl.multiple_of(me * Cw, ROWS), Cw)
        copies = home_copies.setdefault(m, [])
        at, n = tiles[0], len(tiles)
        for r in range(1, S):
            d, device = mate(r)
            copies.append(send(SB.at[m - 1, pl.ds(at, n), d], YB.at[m - 1, pl.ds(at, n), mine],
                               y_s.at[m - 1, at, r - 1], y_r.at[m - 1, at, r - 1], device))
        for t in tiles:
            YB[m - 1, t, mine] = SB[m - 1, t, me]

    theta = None
    for m in range(ITERS):
        last = m + 1 == ITERS
        for g in range(NG):
            if m > 0:
                spread_field(m, range(1, Y + 1), g)
            for y in range(Y):
                acc = zeros()
                if m > 0 and 0 < y < Y - 1:
                    add_onsite(acc, m, y, theta, g)
                add_bonds(acc, m, y, [s for s in (-1, 0, 1) if inside(y + s)], g)
                put(acc, m + 1, y, g)
        if m == 0:
            moments.append(moment(0, 0))
            theta = take_outer()
            for g in range(NG):
                for y in range(1, Y - 1):
                    acc = take(m + 1, y, g)
                    add_onsite(acc, m, y, theta, g)
                    put(acc, m + 1, y, g)
        if last:
            go_home(ITERS, [0])
            early = len(moments) - 1
            told = tell(0, moments[:early])
        for g in range(NG):
            arrived(halo[g])
            spread_field(m, (0, Y + 1), g)
            for y, s in ((0, -1), (Y - 1, 1)):
                acc = take(m + 1, y, g)
                add_bonds(acc, m, y, [s], g)
                add_onsite(acc, m, y, theta, g)
                put(acc, m + 1, y, g)
            if not last:
                halo[g] = halo_field(m + 1, g)
        if not last:
            go_home(m + 1, list(range(p.HT)))
        moments.append(moment(m, m + 1))
        if not last:
            moments.append(moment(m + 1, m + 1))
    told = told + tell(1, moments[early:])
    go_home(ITERS, list(range(1, p.HT)))

    shift = jnp.concatenate([
        roll(shift_ref[:, d * Cw // LANES * LANES:(d * Cw // LANES + 1) * LANES], -(d * Cw % LANES)) for d in range(S)
    ], axis=0) + theta

    def turn_home(n):
        arrived(home_copies[n + 1])
        for h in range(H):
            for t in range(p.HT):
                field = jnp.transpose(YB[n, t, h * LANES:(h + 1) * LANES, :])
                for q in range(G):
                    y, o = group(t * G + q)
                    BT[n + 1, pl.ds(y * X * Z * step + h * O + o, l, stride=step), :] = field[q * l:(q + 1) * l, :]

    for n in range(ITERS):
        turn_home(n)
    arrived(told)

    def total(part):
        rows = []
        for d in range(S):
            line = EM[part, 0, d]
            for n in range(1, p.ny):
                line = line + EM[part, n, d]
            rows.append(line)
        return jnp.concatenate(rows, axis=0)

    sums = [total(0), total(1)]
    m_of = [roll(sums[n >= early], -(n - early * (n >= early)) * Cw) for n in range(2 * ITERS)]

    def inner(u, v):
        out = None
        for a, first in enumerate(u):
            for b, second in enumerate(v):
                term = first * second * m_of[a + b]
                out = term if out is None else out + term
        return out

    def plus(u, v, factor):
        n = max(len(u), len(v))
        out = []
        for a in range(n):
            if a < len(v):
                term = factor * v[a]
                out.append(u[a] + term if a < len(u) else term)
            else:
                out.append(u[a])
        return out

    one = jnp.ones((S, LANES), f32)
    answer, residual, direction, norm = [], [one], [one], m_of[0]
    for turn in range(ITERS):
        image = [shift * direction[0]]
        for a in range(1, len(direction)):
            image.append(direction[a - 1] + shift * direction[a])
        image.append(direction[-1])
        alpha = norm / inner(direction, image)
        answer = plus(answer, direction, alpha)
        residual = plus(residual, image, -alpha)
        if turn + 1 < ITERS:
            fresh = inner(residual, residual)
            direction = plus(residual, direction, fresh / norm)
            norm = fresh
    factors = answer + residual
    per = LANES // Cw
    half = lax.broadcasted_iota(jnp.int32, (H * O, LANES), 0) // O
    for n, factor in enumerate(factors):
        turned = [roll(factor, q * Cw) for q in range(per)]
        block = jnp.zeros((H * O, LANES), f32)
        for h in range(H):
            line = turned[0][h * per:h * per + 1]
            for q in range(1, per):
                line = jnp.where(lane128 // Cw == q, turned[q][h * per + q:h * per + q + 1], line)
            block = jnp.where(half == h, line, block)
        FX[n] = block
    for copy in pending:
        copy.wait_send()


def combine(plan, BT, FX, sol_hbm, res_hbm, OS, sem):
    p = plan
    X, Y, n = p.X, p.Y, p.Z * p.H * p.O
    group = p.H * p.O
    outs = []
    for which, hbm in ((0, sol_hbm), (1, res_hbm)):
        for y in range(Y):
            for x in range(X):
                base = (y * X + x) * n
                for at in range(base, base + n, group):
                    rows = slice(at, at + group)
                    field = FX[which * ITERS] * BT[0, rows, :]
                    for q in range(1, ITERS + which):
                        field = field + FX[which * ITERS + q] * BT[q, rows, :]
                    OS[which, rows, :] = field
        for x in range(X):
            for y in range(Y):
                copy = pltpu.make_async_copy(
                    OS.at[which, pl.ds((y * X + x) * n, n)], hbm.at[x, y], sem.at[(which * X + x) * Y + y])
                copy.start()
                outs.append(copy)
    for copy in outs:
        copy.wait()


def per_device(peers, right_side, bond_blocks, bond_open, onsite_blocks, orbital_levels, column_shift):
    block, orb, cols = right_side.shape[:3], right_side.shape[3], right_side.shape[4]
    p = Plan(block, orb, cols, peers)
    X, Y, Z, O, S, L, H = p.X, p.Y, p.Z, p.O, p.S, p.L, p.H
    f32 = jnp.float32
    right = right_side.reshape(X, Y, Z, O, H, LANES).transpose(0, 1, 2, 4, 3, 5).reshape(X, Y, Z * H * O, LANES)
    blocks = jnp.transpose(bond_blocks, (1, 2, 3, 4, 5, 0)).reshape(O * O * X * Y * Z, NB)
    opened = jnp.transpose(bond_open, (1, 2, 3, 0)).reshape(X * Y * Z, NB)
    onsite = onsite_blocks.reshape(O * O * X * Y, Z)
    levels = orbital_levels.reshape(O * X * Y, Z)
    dma = pltpu.SemaphoreType.DMA
    vmem, anywhere = pl.BlockSpec(memory_space=pltpu.VMEM), pl.BlockSpec(memory_space=pl.ANY)

    def scratch(*shape):
        return pltpu.VMEM(shape, f32)

    flat = (p.cols, p.HL)
    made = pl.pallas_call(
        functools.partial(kernel, p),
        out_shape=(scratch(ITERS + 1, X * Y * Z * H * O, LANES), scratch(2 * ITERS + 1, H * O, LANES)),
        in_specs=[pl.BlockSpec(memory_space=pltpu.HBM)] * 6,
        out_specs=(vmem,) * 2,
        scratch_shapes=[
            scratch(X * Y * Z * H * O, LANES),
            scratch(O * O * X * Y * Z, NB),
            pltpu.VMEM(opened.shape, jnp.int32),
            scratch(*onsite.shape),
            scratch(*levels.shape),
            scratch(1, cols),
            pltpu.VMEM((2 * L, 8 * L), jnp.bfloat16),
            pltpu.VMEM((p.NG, Y * p.OC, 2 * L), jnp.bfloat16),
            scratch(*flat),
            scratch(ITERS, p.HT, cols, LANES),
            scratch(3, 3 * ROWS, LANES),
            scratch(p.HR, LANES),
            scratch(S, p.HR, LANES),
            scratch(S, p.Cw, p.HL),
            scratch(p.CR, LANES),
            scratch(S, p.CR, LANES),
            scratch(p.JT, Y + 2, p.CR, L),
            scratch(NB, p.JT, Y, ROWS, L),
            scratch(ITERS + 1, Y + 2, p.NG, p.OC, L),
            scratch(Y + 2, p.NG, p.OC, 8 * L),
            scratch(ITERS, p.HT, S, p.Cw, LANES),
            scratch(2, p.ny, S, 1, LANES),
            scratch(2, 1, LANES),
            scratch(p.ny, ROWS, LANES),
            dma((X * Y + 5,)),
            dma((S - 1,)), dma((S - 1,)), dma((S - 1,)), dma((S - 1,)),
            dma((ITERS, p.NG, 2)), dma((ITERS, p.NG, 2)), dma((3,)), dma((3,)),
            dma((S - 1,)), dma((S - 1,)),
            dma((p.ny - 1,)), dma((p.ny - 1,)),
            dma((ITERS, p.HT, S - 1)), dma((ITERS, p.HT, S - 1)),
            dma((2, p.ny * S - 1)), dma((2, p.ny * S - 1)),
        ],
        compiler_params=pltpu.CompilerParams(
            collective_id=0, has_side_effects=True, vmem_limit_bytes=40 * 1024 * 1024
        ),
    )(*(pltpu.with_memory_space_constraint(v, pltpu.HBM)
        for v in (right, blocks, opened, onsite, levels, column_shift[None])))
    outs = pl.pallas_call(
        functools.partial(combine, p),
        out_shape=(jax.ShapeDtypeStruct(right.shape, f32),) * 2,
        in_specs=[vmem] * 2,
        out_specs=(anywhere, anywhere),
        scratch_shapes=[scratch(2, X * Y * Z * H * O, LANES), dma((2 * X * Y,))],
        compiler_params=pltpu.CompilerParams(vmem_limit_bytes=16 * 1024 * 1024),
    )(*made)

    def back(v):
        return v.reshape(X, Y, Z, H, O, LANES).transpose(0, 1, 2, 4, 3, 5).reshape(right_side.shape)

    return back(outs[0]), back(outs[1])


def solution(mesh):
    field = P("gx", "gy", "gz", None, None)
    placed = (
        field,
        P(None, None, None, "gx", "gy", "gz"),
        P(None, "gx", "gy", "gz"),
        P(None, None, "gx", "gy", "gz"),
        P(None, "gx", "gy", "gz"),
        P(),
    )
    return jax.shard_map(
        functools.partial(per_device, tuple(mesh.shape[name] for name in AXES)),
        mesh=mesh,
        in_specs=placed,
        out_specs=(field, field),
        check_vma=False,
    )
```

```python
import functools
import itertools

import jax
import jax.numpy as jnp
from jax import lax
from jax.experimental import pallas as pl
from jax.experimental.pallas import tpu as pltpu
from jax.sharding import PartitionSpec as P

ITERS = 3
LANES = 128
ROWS = 8
AXES = ("gx", "gy", "gz")
MESH = pl.DeviceIdType.MESH

bonds = [o for o in itertools.product((-1, 0, 1), repeat=3) if o > (0, 0, 0)]
NB = len(bonds)
ahead_runs = [(1, 3), (10, 3)]
behind_runs = [(4, 3)]
assert all(bonds[k][1] == 1 for at, n in ahead_runs for k in range(at, at + n))
assert all(bonds[k][1] == -1 for at, n in behind_runs for k in range(at, at + n))


class Plan:
    def __init__(self, block, orb, cols, peers):
        self.X, self.Y, self.Z = block
        self.O, self.cols = orb, cols
        self.nx, self.ny, self.nz = peers
        self.S = self.nx * self.nz
        self.l = self.X * self.Z
        self.L = self.S * self.l
        self.G = LANES // self.l
        self.Cw = cols // self.S
        self.YO = self.Y * orb
        self.HL = self.YO * self.l
        self.HT = self.HL // LANES
        self.H = cols // LANES
        self.JT = LANES // (self.Y * self.l)
        self.tiles = orb * orb // self.JT
        self.CR = (NB + 1) * self.tiles
        self.NG = 2 if self.Cw % (2 * ROWS) == 0 else 1
        self.Cg = self.Cw // self.NG
        self.OC = orb * self.Cg
        edge = sum(n for _, n in ahead_runs + behind_runs)
        self.HR = (-(-edge // (LANES // (self.JT * self.l))) + 1) * ROWS
        assert self.H * orb == ROWS
        assert self.tiles == ROWS and self.S % self.G == 0 and self.Cw % ROWS == 0


def kernel(plan, rs_hbm, bb_hbm, open_hbm, onsite_hbm, level_hbm, shift_hbm, BT, FX,
           RS, BB, open_ref, onsite_ref, level_ref, shift_ref, PM, LH, T, YB, ZC, HS, HC, RB, CS, CR, M, MB, V, VS, SB, EM, SR, TG,
           in_sem, a_s, a_r, c_s, c_r, hv_s, hv_r, hm_s, hm_r, ho_s, ho_r, th_s, th_r, y_s, y_r, e_s, e_r):
    p = plan
    X, Y, Z, O, S, L, l, G, Cw, H, OC = p.X, p.Y, p.Z, p.O, p.S, p.L, p.l, p.G, p.Cw, p.H, p.OC
    NG, Cg = p.NG, p.Cg
    f32 = jnp.float32
    ax, ay, az = (lax.axis_index(name) for name in AXES)
    me = ax * p.nz + az
    pending = []

    def mate(r):
        d = lax.rem(me + r, S)
        return d, (lax.div(d, p.nz), ay, lax.rem(d, p.nz))

    def source(r):
        return lax.rem(me + (S - r), S)

    def along(r):
        return (ax, lax.rem(ay + (r % p.ny), p.ny), az)

    def send(src, dst, ssem, rsem, device):
        copy = pltpu.make_async_remote_copy(
            src_ref=src, dst_ref=dst, send_sem=ssem, recv_sem=rsem, device_id=device, device_id_type=MESH
        )
        copy.start()
        pending.append(copy)
        return copy

    barrier = pltpu.get_barrier_semaphore()
    for r in range(1, S):
        pl.semaphore_signal(barrier, inc=1, device_id=mate(r)[1], device_id_type=MESH)
    for r in range(1, p.ny):
        pl.semaphore_signal(barrier, inc=1, device_id=along(r), device_id_type=MESH)

    loads = []
    for x in range(X):
        for y in range(Y):
            n = Z * H * O
            copy = pltpu.make_async_copy(
                rs_hbm.at[x, y], RS.at[pl.ds((y * X + x) * n, n)], in_sem.at[x * Y + y])
            copy.start()
            loads.append(copy)
    small_loads = []
    for n, (src, dst) in enumerate(((onsite_hbm, onsite_ref), (level_hbm, level_ref), (bb_hbm, BB),
                                    (open_hbm, open_ref), (shift_hbm, shift_ref))):
        copy = pltpu.make_async_copy(src, dst, in_sem.at[X * Y + n])
        copy.start()
        small_loads.append(copy)

    lane = lax.broadcasted_iota(jnp.int32, (1, L), 1)
    lane128 = lax.broadcasted_iota(jnp.int32, (1, LANES), 1)

    def roll(v, by):
        by = by % v.shape[1]
        return v if by == 0 else pltpu.roll(v, by, 1)

    zg = ((lane // l) & (p.nz - 1)) * Z + (lane & (Z - 1))
    xg = (lane // (l * p.nz)) * X + ((lane // Z) & (X - 1))
    row_of = lax.broadcasted_iota(jnp.int32, (L, L), 0)

    def place(sx, sz):
        n = (sx + 1) * 3 + sz + 1
        return n - (n > 4)

    def make_shifts():
        for sx in (-1, 0, 1):
            for sz in (-1, 0, 1):
                if (sx, sz) == (0, 0):
                    continue
                x_to, z_to = (xg + sx) & (p.nx * X - 1), (zg + sz) & (p.nz * Z - 1)
                from_lane = ((x_to // X) * p.nz + z_to // Z) * l + (x_to & (X - 1)) * Z + (z_to & (Z - 1))
                matrix = jnp.where(row_of == from_lane, 1.0, 0.0).astype(jnp.bfloat16)
                at = place(sx, sz) * L
                PM[0:L, at:at + L] = matrix
                PM[L:2 * L, at:at + L] = matrix

    def halves(v):
        high = v.astype(jnp.bfloat16)
        low = (v - high.astype(f32)).astype(jnp.bfloat16)
        return jnp.concatenate([high, low], axis=1)

    block_of = lane128 // l

    def butterfly(arrays):
        arrays = list(arrays)
        m = 1
        while m < G:
            low = (block_of & m) == 0
            for a in range(G):
                if a & m == 0:
                    b = a | m
                    first, second = arrays[a], arrays[b]
                    arrays[a] = jnp.where(low, first, roll(second, m * l))
                    arrays[b] = jnp.where(low, roll(first, -m * l), second)
            m *= 2
        return arrays

    for copy in loads:
        copy.wait()
    step = H * O
    order = list(range(1, Y - 1)) + [0, Y - 1]

    def group(n):
        return order[n // O], n % O

    for h in range(H):
        rows = jnp.concatenate([
            RS[pl.ds(y * X * Z * step + h * O + o, l, stride=step), :] for y in order for o in range(O)
        ], axis=0)
        T[h * LANES:(h + 1) * LANES, :] = jnp.transpose(rows)
    BT[0] = RS[...]
    make_shifts()
    pl.semaphore_wait(barrier, S - 1 + p.ny - 1)
    field_copies = []
    for r in range(1, S):
        d, device = mate(r)
        field_copies.append(send(
            T.at[pl.ds(pl.multiple_of(d * Cw, ROWS), Cw)], RB.at[me], a_s.at[r - 1], a_r.at[r - 1], device))
    RB[me] = T[pl.ds(pl.multiple_of(me * Cw, ROWS), Cw), :]

    def spread_z(block):
        n = block.shape[0]
        out = jnp.zeros((n, LANES), f32)
        for z in range(Z):
            out = jnp.where((lane128 & (Z - 1)) == z, block[:, z:z + 1], out)
        row = lax.broadcasted_iota(jnp.int32, (n, LANES), 0)
        col = lax.broadcasted_iota(jnp.int32, (n, LANES), 1)
        x_row, y_row = (row // Y) & (X - 1), row & (Y - 1)
        x_col, y_col = (col // Z) & (X - 1), (col // l) & (Y - 1)
        return jnp.where((x_row == x_col) & (y_row == y_col), out, 0.0)

    for copy in small_loads[0:2]:
        copy.wait()
    onsite = spread_z(onsite_ref[...])
    level = spread_z(level_ref[...])
    XY = X * Y
    pair = [jnp.sum(onsite[n * XY:(n + 1) * XY], axis=0, keepdims=True) for n in range(O * O)]
    diagonal = [jnp.sum(level[n * XY:(n + 1) * XY], axis=0, keepdims=True) for n in range(O)]
    j_low = lane128 // (Y * l)
    diagonal_sum = jnp.zeros((1, LANES), f32)
    for i in range(O):
        for jh in range(O // p.JT):
            line = jnp.zeros((1, LANES), f32)
            for jl in range(p.JT):
                j = jh * p.JT + jl
                term = 0.5 * (pair[i * O + j] + pair[j * O + i])
                if i == j:
                    term = term + diagonal[i]
                    diagonal_sum = diagonal_sum + jnp.where(j_low == 0, term, 0.0)
                line = jnp.where(j_low == jl, term, line)
            row = NB * ROWS + i * (O // p.JT) + jh
            CS[row:row + 1, :] = line

    diagonal_sum = jnp.sum(diagonal_sum, axis=1, keepdims=True)
    for copy in small_loads[2:]:
        copy.wait()
    is_open = open_ref[...].astype(f32)
    is_open = jnp.concatenate([is_open] * p.JT, axis=0)
    x_of, y_of = (lane128 // (Y * Z)) & (X - 1), (lane128 // Z) & (Y - 1)
    x_to, y_to = (lane128 // Z) & (X - 1), (lane128 // (X * Z)) & (Y - 1)
    source_lane = (lane128 & (Z - 1)) + x_to * (Y * Z) + y_to * Z + j_low * (Y * l)
    gaps = sorted({(x * Y * Z + y * Z) - (y * X * Z + x * Z) for x in range(X) for y in range(Y)})
    for t in range(p.tiles):
        block = BB[t * LANES:(t + 1) * LANES, :] * is_open
        block = jnp.concatenate([block, jnp.zeros((LANES, LANES - NB), f32)], axis=1)
        block = jnp.transpose(block)[0:2 * ROWS, :]
        out = block
        for gap in gaps:
            if gap:
                out = jnp.where(source_lane - lane128 == gap, roll(block, -gap), out)
        CS[pl.ds(t, NB, stride=ROWS), :] = out[0:NB, :]
    early_halo = []
    for n, (run, way) in enumerate([(run, 1) for run in ahead_runs] + [(run, -1) for run in behind_runs]):
        early_halo.append(send(
            CS.at[pl.ds(run[0] * ROWS, run[1] * ROWS)], ZC.at[n], hm_s.at[n], hm_r.at[n], along(way)))
    TG[ay] = jnp.broadcast_to(diagonal_sum, (ROWS, LANES))
    early_halo += [
        send(TG.at[ay], TG.at[ay], th_s.at[r - 1], th_r.at[r - 1], along(r)) for r in range(1, p.ny)]
    partner = (ax + 1 - 2 * lax.rem(ax, 2), ay, az)
    even = [(dx, dz) for dz in range(p.nz) for dx in range(0, p.nx, 2) if (dx, dz) != (0, 0)]
    coef_copies = []
    for n, (dx, dz) in enumerate(even):
        device = (lax.rem(ax + dx, p.nx), ay, lax.rem(az + dz, p.nz))
        coef_copies.append(send(CS, CR.at[me], c_s.at[n], c_r.at[n], device))
    relays = [send(CS, CR.at[me], c_s.at[len(even)], c_r.at[len(even)], partner)]
    CR[me] = CS[...]

    def halo_field(m, g):
        return [
            send(V.at[m, 1, g], V.at[m, Y + 1, g], hv_s.at[m, g, 0], hv_r.at[m, g, 0], along(-1)),
            send(V.at[m, Y, g], V.at[m, 0, g], hv_s.at[m, g, 1], hv_r.at[m, g, 1], along(1)),
        ]

    def arrived(copies):
        for copy in copies:
            copy.wait_recv()

    def spread_field(m, slots, g):
        rows = len(slots) * OC
        for n, slot in enumerate(slots):
            LH[g, n * OC:(n + 1) * OC, :] = halves(V[m, slot, g])
        for n in range(0, 8, 2):
            at = slice(n * L, (n + 2) * L)
            moved = jnp.dot(LH[g, 0:rows, :], PM[:, at], preferred_element_type=f32)
            for q, slot in enumerate(slots):
                VS[slot, g, :, at] = moved[q * OC:(q + 1) * OC]

    arrived(field_copies)
    for t in range(p.HT):
        for first in range(0, S, G):
            blocks = butterfly([RB[first + n, :, t * LANES:(t + 1) * LANES] for n in range(G)])
            at = first // G * LANES
            for n in range(G):
                y, o = group(t * G + n)
                for g in range(NG):
                    V[0, y + 1, g, o * Cg:(o + 1) * Cg, at:at + LANES] = blocks[n][g * Cg:(g + 1) * Cg]
    halo = [halo_field(0, g) for g in range(NG)]

    arrived(early_halo)
    outer = [(n, q, run[0] + q, slot, y) for n, (run, slot, y) in enumerate(
        [(run, 0, Y - 1) for run in ahead_runs] + [(run, Y + 1, 0) for run in behind_runs]) for q in range(run[1])]
    unit = p.JT * l
    U = LANES // unit
    for v in range(0, len(outer), U):
        packed = jnp.zeros((ROWS, LANES), f32)
        for q, (n, at, k, slot, y) in enumerate(outer[v:v + U]):
            block = ZC[n, at * ROWS:(at + 1) * ROWS, :]
            for jl in range(p.JT):
                to = q * unit + jl * l
                packed = jnp.where(block_of == to // l, roll(block, to - jl * Y * l - y * l), packed)
        HS[v // U * ROWS:(v // U + 1) * ROWS, :] = packed
    part = TG[0]
    for n in range(1, p.ny):
        part = part + TG[n]
    HS[p.HR - ROWS:p.HR, :] = part
    outer_copies = []
    for r in range(1, S):
        d, device = mate(r)
        outer_copies.append(send(HS, HC.at[me], ho_s.at[r - 1], ho_r.at[r - 1], device))
    HC[me] = HS[...]
    for g in range(NG):
        spread_field(0, range(1, Y + 1), g)

    def take_outer():
        arrived(outer_copies)
        for first in range(0, S, G):
            blocks = butterfly([HC[first + n, 0:p.HR - ROWS, :] for n in range(G)])
            at = first // G * LANES
            for n, (_, _, k, slot, y) in enumerate(outer):
                v, q = divmod(n, U)
                for jl in range(p.JT):
                    M[jl, slot, k * ROWS:(k + 1) * ROWS, at:at + LANES] = (
                        blocks[q * p.JT + jl][v * ROWS:(v + 1) * ROWS])
        mirror(False)
        total = HC[0, p.HR - ROWS:p.HR - ROWS + 1, 0:1]
        for n in range(1, S):
            total = total + HC[n, p.HR - ROWS:p.HR - ROWS + 1, 0:1]
        return total * (1.0 / (p.ny * Y * L * O))

    for n, (dx, dz) in enumerate(even):
        coef_copies[n].wait_recv()
        s = lax.rem(ax + (p.nx - dx), p.nx) * p.nz + lax.rem(az + (p.nz - dz), p.nz)
        at = len(even) + 1 + n
        relays.append(send(CR.at[s], CR.at[s], c_s.at[at], c_r.at[at], partner))
    arrived(relays)
    for first in range(0, S, G):
        blocks = butterfly([CR[first + n] for n in range(G)])
        at = first // G * LANES
        for n in range(G):
            jl, y = divmod(n, Y)
            M[jl, y + 1, :, at:at + LANES] = blocks[n]
    HALFJ = O // p.JT

    def inside(y):
        return 0 <= y < Y

    def mirror(within):
        groups = {}
        for k, o in enumerate(bonds):
            for y in range(Y):
                if inside(y - o[1]) == within:
                    groups.setdefault((-o[0], -o[2]), []).extend((k, jl, y) for jl in range(p.JT))
        for (sx, sz), members in groups.items():
            blocks = [M[jl, y + 1 - bonds[k][1], k * ROWS:(k + 1) * ROWS, :] for k, jl, y in members]
            if (sx, sz) != (0, 0):
                at = place(sx, sz) * L
                moved = jnp.dot(halves(jnp.concatenate(blocks, axis=0)), PM[:, at:at + L], preferred_element_type=f32)
                blocks = [moved[n * ROWS:(n + 1) * ROWS] for n in range(len(members))]
            for (k, jl, y), block in zip(members, blocks):
                MB[k, jl, y] = block

    mirror(True)

    def add_bonds(acc, m, y, steps, g):
        for k, o in enumerate(bonds):
            for sign in (1, -1):
                if sign * o[1] not in steps:
                    continue
                slot = y + 1 + sign * o[1]
                sx, sz = sign * o[0], sign * o[2]
                for j in range(O):
                    rows = slice(j * Cg, (j + 1) * Cg)
                    at = place(sx, sz) * L
                    v = V[m, slot, g, rows, :] if (sx, sz) == (0, 0) else VS[slot, g, rows, at:at + L]
                    for i in range(O):
                        if sign > 0:
                            row = k * ROWS + i * HALFJ + j // p.JT
                            c = M[j % p.JT, y + 1, row:row + 1, :]
                        else:
                            row = j * HALFJ + i // p.JT
                            c = MB[k, i % p.JT, y, row:row + 1, :]
                        acc[i] = acc[i] + c * v

    def add_onsite(acc, m, y, theta, g):
        for j in range(O):
            v = V[m, y + 1, g, j * Cg:(j + 1) * Cg, :]
            for i in range(O):
                row = NB * ROWS + i * HALFJ + j // p.JT
                c = M[j % p.JT, y + 1, row:row + 1, :]
                if i == j:
                    c = c - theta
                acc[i] = acc[i] + c * v

    def put(acc, m, y, g):
        for i in range(O):
            V[m, y + 1, g, i * Cg:(i + 1) * Cg, :] = acc[i]

    def take(m, y, g):
        return [V[m, y + 1, g, i * Cg:(i + 1) * Cg, :] for i in range(O)]

    def zeros():
        return [jnp.zeros((Cg, L), f32) for _ in range(O)]

    def moment(a, b):
        sums = []
        for g in range(NG):
            total = jnp.zeros((Cg, L), f32)
            for y in range(Y):
                for i in range(O):
                    rows = slice(i * Cg, (i + 1) * Cg)
                    total = total + V[a, y + 1, g, rows, :] * V[b, y + 1, g, rows, :]
            sums.append(jnp.sum(total, axis=1, keepdims=True))
        return jnp.concatenate(sums, axis=0)

    moments = []
    home_copies = {}

    everyone = [(g, r) for g in range(p.ny) for r in range(S) if (g, r) != (0, 0)]

    def tell(part, values):
        sublane = lax.broadcasted_iota(jnp.int32, (Cw, LANES), 0)
        spot = lax.broadcasted_iota(jnp.int32, (Cw, LANES), 1)
        table = jnp.zeros((Cw, LANES), f32)
        for n, value in enumerate(values):
            table = jnp.where(spot == sublane + n * Cw, value, table)
        line = jnp.sum(table, axis=0, keepdims=True)
        EM[part, ay, me] = line
        SR[part] = line
        copies = []
        for n, (g, r) in enumerate(everyone):
            d = lax.rem(me + r, S)
            device = (lax.div(d, p.nz), lax.rem(ay + g, p.ny), lax.rem(d, p.nz))
            copies.append(send(SR.at[part], EM.at[part, ay, me], e_s.at[part, n], e_r.at[part, n], device))
        return copies

    def go_home(m, tiles):
        for t in tiles:
            for first in range(0, S, G):
                at = first // G * LANES
                blocks = []
                for n in range(G):
                    y, o = group(t * G + n)
                    blocks.append(jnp.concatenate(
                        [V[m, y + 1, g, o * Cg:(o + 1) * Cg, at:at + LANES] for g in range(NG)], axis=0))
                blocks = butterfly(blocks)
                for n in range(G):
                    SB[m - 1, t, first + n] = blocks[n]
        mine = pl.ds(pl.multiple_of(me * Cw, ROWS), Cw)
        copies = home_copies.setdefault(m, [])
        at, n = tiles[0], len(tiles)
        for r in range(1, S):
            d, device = mate(r)
            copies.append(send(SB.at[m - 1, pl.ds(at, n), d], YB.at[m - 1, pl.ds(at, n), mine],
                               y_s.at[m - 1, at, r - 1], y_r.at[m - 1, at, r - 1], device))
        for t in tiles:
            YB[m - 1, t, mine] = SB[m - 1, t, me]

    theta = None
    for m in range(ITERS):
        last = m + 1 == ITERS
        if m > 0:
            for g in range(NG):
                spread_field(m, range(1, Y + 1), g)

        def interior(y, steps, g):
            acc = zeros()
            if m > 0 and len(steps) == 3:
                add_onsite(acc, m, y, theta, g)
            add_bonds(acc, m, y, steps, g)
            put(acc, m + 1, y, g)

        def middle(q, carry):
            interior(1 + lax.div(q, NG), (-1, 0, 1), lax.rem(q, NG))
            return carry

        def first(g, carry):
            interior(0, (0, 1), g)
            return carry

        def final(g, carry):
            interior(Y - 1, (-1, 0), g)
            return carry

        lax.fori_loop(0, NG, first, 0)
        lax.fori_loop(0, (Y - 2) * NG, middle, 0)
        lax.fori_loop(0, NG, final, 0)
        if m == 0:
            moments.append(moment(0, 0))
            theta = take_outer()
            for g in range(NG):
                for y in range(1, Y - 1):
                    acc = take(m + 1, y, g)
                    add_onsite(acc, m, y, theta, g)
                    put(acc, m + 1, y, g)
        if last:
            go_home(ITERS, [0])
            early = len(moments) - 1
            told = tell(0, moments[:early])
        for g in range(NG):
            arrived(halo[g])
            spread_field(m, (0, Y + 1), g)
            for y, s in ((0, -1), (Y - 1, 1)):
                acc = take(m + 1, y, g)
                add_bonds(acc, m, y, [s], g)
                add_onsite(acc, m, y, theta, g)
                put(acc, m + 1, y, g)
            if not last:
                halo[g] = halo_field(m + 1, g)
        if not last:
            go_home(m + 1, list(range(p.HT)))
        moments.append(moment(m, m + 1))
        if not last:
            moments.append(moment(m + 1, m + 1))
    told = told + tell(1, moments[early:])
    go_home(ITERS, list(range(1, p.HT)))

    shift = jnp.concatenate([
        roll(shift_ref[:, d * Cw // LANES * LANES:(d * Cw // LANES + 1) * LANES], -(d * Cw % LANES)) for d in range(S)
    ], axis=0) + theta

    def turn_home(n):
        arrived(home_copies[n + 1])
        for h in range(H):
            for t in range(p.HT):
                field = jnp.transpose(YB[n, t, h * LANES:(h + 1) * LANES, :])
                for q in range(G):
                    y, o = group(t * G + q)
                    BT[n + 1, pl.ds(y * X * Z * step + h * O + o, l, stride=step), :] = field[q * l:(q + 1) * l, :]

    for n in range(ITERS):
        turn_home(n)
    arrived(told)

    def total(part):
        rows = []
        for d in range(S):
            line = EM[part, 0, d]
            for n in range(1, p.ny):
                line = line + EM[part, n, d]
            rows.append(line)
        return jnp.concatenate(rows, axis=0)

    sums = [total(0), total(1)]
    m_of = [roll(sums[n >= early], -(n - early * (n >= early)) * Cw) for n in range(2 * ITERS)]

    def inner(u, v):
        out = None
        for a, first in enumerate(u):
            for b, second in enumerate(v):
                term = first * second * m_of[a + b]
                out = term if out is None else out + term
        return out

    def plus(u, v, factor):
        n = max(len(u), len(v))
        out = []
        for a in range(n):
            if a < len(v):
                term = factor * v[a]
                out.append(u[a] + term if a < len(u) else term)
            else:
                out.append(u[a])
        return out

    one = jnp.ones((S, LANES), f32)
    answer, residual, direction, norm = [], [one], [one], m_of[0]
    for turn in range(ITERS):
        image = [shift * direction[0]]
        for a in range(1, len(direction)):
            image.append(direction[a - 1] + shift * direction[a])
        image.append(direction[-1])
        alpha = norm / inner(direction, image)
        answer = plus(answer, direction, alpha)
        residual = plus(residual, image, -alpha)
        if turn + 1 < ITERS:
            fresh = inner(residual, residual)
            direction = plus(residual, direction, fresh / norm)
            norm = fresh
    factors = answer + residual
    per = LANES // Cw
    half = lax.broadcasted_iota(jnp.int32, (H * O, LANES), 0) // O
    for n, factor in enumerate(factors):
        turned = [roll(factor, q * Cw) for q in range(per)]
        block = jnp.zeros((H * O, LANES), f32)
        for h in range(H):
            line = turned[0][h * per:h * per + 1]
            for q in range(1, per):
                line = jnp.where(lane128 // Cw == q, turned[q][h * per + q:h * per + q + 1], line)
            block = jnp.where(half == h, line, block)
        FX[n] = block
    for copy in pending:
        copy.wait_send()


def combine(plan, BT, FX, sol_hbm, res_hbm, OS, sem):
    p = plan
    X, Y, n = p.X, p.Y, p.Z * p.H * p.O
    group = p.H * p.O
    outs = []
    for which, hbm in ((0, sol_hbm), (1, res_hbm)):
        for y in range(Y):
            for x in range(X):
                base = (y * X + x) * n
                for at in range(base, base + n, group):
                    rows = slice(at, at + group)
                    field = FX[which * ITERS] * BT[0, rows, :]
                    for q in range(1, ITERS + which):
                        field = field + FX[which * ITERS + q] * BT[q, rows, :]
                    OS[which, rows, :] = field
        for x in range(X):
            for y in range(Y):
                copy = pltpu.make_async_copy(
                    OS.at[which, pl.ds((y * X + x) * n, n)], hbm.at[x, y], sem.at[(which * X + x) * Y + y])
                copy.start()
                outs.append(copy)
    for copy in outs:
        copy.wait()


def per_device(peers, right_side, bond_blocks, bond_open, onsite_blocks, orbital_levels, column_shift):
    block, orb, cols = right_side.shape[:3], right_side.shape[3], right_side.shape[4]
    p = Plan(block, orb, cols, peers)
    X, Y, Z, O, S, L, H = p.X, p.Y, p.Z, p.O, p.S, p.L, p.H
    f32 = jnp.float32
    right = right_side.reshape(X, Y, Z, O, H, LANES).transpose(0, 1, 2, 4, 3, 5).reshape(X, Y, Z * H * O, LANES)
    blocks = jnp.transpose(bond_blocks, (1, 2, 3, 4, 5, 0)).reshape(O * O * X * Y * Z, NB)
    opened = jnp.transpose(bond_open, (1, 2, 3, 0)).reshape(X * Y * Z, NB)
    onsite = onsite_blocks.reshape(O * O * X * Y, Z)
    levels = orbital_levels.reshape(O * X * Y, Z)
    dma = pltpu.SemaphoreType.DMA
    vmem, anywhere = pl.BlockSpec(memory_space=pltpu.VMEM), pl.BlockSpec(memory_space=pl.ANY)

    def scratch(*shape):
        return pltpu.VMEM(shape, f32)

    flat = (p.cols, p.HL)
    made = pl.pallas_call(
        functools.partial(kernel, p),
        out_shape=(scratch(ITERS + 1, X * Y * Z * H * O, LANES), scratch(2 * ITERS + 1, H * O, LANES)),
        in_specs=[pl.BlockSpec(memory_space=pltpu.HBM)] * 6,
        out_specs=(vmem,) * 2,
        scratch_shapes=[
            scratch(X * Y * Z * H * O, LANES),
            scratch(O * O * X * Y * Z, NB),
            pltpu.VMEM(opened.shape, jnp.int32),
            scratch(*onsite.shape),
            scratch(*levels.shape),
            scratch(1, cols),
            pltpu.VMEM((2 * L, 8 * L), jnp.bfloat16),
            pltpu.VMEM((p.NG, Y * p.OC, 2 * L), jnp.bfloat16),
            scratch(*flat),
            scratch(ITERS, p.HT, cols, LANES),
            scratch(3, 3 * ROWS, LANES),
            scratch(p.HR, LANES),
            scratch(S, p.HR, LANES),
            scratch(S, p.Cw, p.HL),
            scratch(p.CR, LANES),
            scratch(S, p.CR, LANES),
            scratch(p.JT, Y + 2, p.CR, L),
            scratch(NB, p.JT, Y, ROWS, L),
            scratch(ITERS + 1, Y + 2, p.NG, p.OC, L),
            scratch(Y + 2, p.NG, p.OC, 8 * L),
            scratch(ITERS, p.HT, S, p.Cw, LANES),
            scratch(2, p.ny, S, 1, LANES),
            scratch(2, 1, LANES),
            scratch(p.ny, ROWS, LANES),
            dma((X * Y + 5,)),
            dma((S - 1,)), dma((S - 1,)), dma((S - 1,)), dma((S - 1,)),
            dma((ITERS, p.NG, 2)), dma((ITERS, p.NG, 2)), dma((3,)), dma((3,)),
            dma((S - 1,)), dma((S - 1,)),
            dma((p.ny - 1,)), dma((p.ny - 1,)),
            dma((ITERS, p.HT, S - 1)), dma((ITERS, p.HT, S - 1)),
            dma((2, p.ny * S - 1)), dma((2, p.ny * S - 1)),
        ],
        compiler_params=pltpu.CompilerParams(
            collective_id=0, has_side_effects=True, vmem_limit_bytes=40 * 1024 * 1024
        ),
    )(*(pltpu.with_memory_space_constraint(v, pltpu.HBM)
        for v in (right, blocks, opened, onsite, levels, column_shift[None])))
    outs = pl.pallas_call(
        functools.partial(combine, p),
        out_shape=(jax.ShapeDtypeStruct(right.shape, f32),) * 2,
        in_specs=[vmem] * 2,
        out_specs=(anywhere, anywhere),
        scratch_shapes=[scratch(2, X * Y * Z * H * O, LANES), dma((2 * X * Y,))],
        compiler_params=pltpu.CompilerParams(vmem_limit_bytes=16 * 1024 * 1024),
    )(*made)

    def back(v):
        return v.reshape(X, Y, Z, H, O, LANES).transpose(0, 1, 2, 4, 3, 5).reshape(right_side.shape)

    return back(outs[0]), back(outs[1])


def solution(mesh):
    field = P("gx", "gy", "gz", None, None)
    placed = (
        field,
        P(None, None, None, "gx", "gy", "gz"),
        P(None, "gx", "gy", "gz"),
        P(None, None, "gx", "gy", "gz"),
        P(None, "gx", "gy", "gz"),
        P(),
    )
    return jax.shard_map(
        functools.partial(per_device, tuple(mesh.shape[name] for name in AXES)),
        mesh=mesh,
        in_specs=placed,
        out_specs=(field, field),
        check_vma=False,
    )
```

```python
import functools
import itertools

import jax
import jax.numpy as jnp
from jax import lax
from jax.experimental import pallas as pl
from jax.experimental.pallas import tpu as pltpu
from jax.sharding import PartitionSpec as P

ITERS = 3
LANES = 128
ROWS = 8
AXES = ("gx", "gy", "gz")
MESH = pl.DeviceIdType.MESH

bonds = [o for o in itertools.product((-1, 0, 1), repeat=3) if o > (0, 0, 0)]
NB = len(bonds)
ahead_runs = [(1, 3), (10, 3)]
behind_runs = [(4, 3)]
assert all(bonds[k][1] == 1 for at, n in ahead_runs for k in range(at, at + n))
assert all(bonds[k][1] == -1 for at, n in behind_runs for k in range(at, at + n))


class Plan:
    def __init__(self, block, orb, cols, peers):
        self.X, self.Y, self.Z = block
        self.O, self.cols = orb, cols
        self.nx, self.ny, self.nz = peers
        self.S = self.nx * self.nz
        self.l = self.X * self.Z
        self.L = self.S * self.l
        self.G = LANES // self.l
        self.Cw = cols // self.S
        self.YO = self.Y * orb
        self.HL = self.YO * self.l
        self.HT = self.HL // LANES
        self.H = cols // LANES
        self.JT = LANES // (self.Y * self.l)
        self.tiles = orb * orb // self.JT
        self.CR = (NB + 1) * self.tiles
        self.NG = 2 if self.Cw % (2 * ROWS) == 0 else 1
        self.Cg = self.Cw // self.NG
        self.OC = orb * self.Cg
        edge = sum(n for _, n in ahead_runs + behind_runs)
        self.HR = (-(-edge // (LANES // (self.JT * self.l))) + 1) * ROWS
        assert self.H * orb == ROWS
        assert self.tiles == ROWS and self.S % self.G == 0 and self.Cw % ROWS == 0


def kernel(plan, rs_hbm, bb_hbm, open_hbm, onsite_hbm, level_hbm, shift_hbm, BT, FX,
           RS, BB, open_ref, onsite_ref, level_ref, shift_ref, PM, LH, T, YB, ZC, HS, HC, RB, CS, CR, M, MB, V, VS, SB, EM, SR, TG,
           in_sem, a_s, a_r, c_s, c_r, hv_s, hv_r, hm_s, hm_r, ho_s, ho_r, th_s, th_r, y_s, y_r, e_s, e_r):
    p = plan
    X, Y, Z, O, S, L, l, G, Cw, H, OC = p.X, p.Y, p.Z, p.O, p.S, p.L, p.l, p.G, p.Cw, p.H, p.OC
    NG, Cg = p.NG, p.Cg
    f32 = jnp.float32
    ax, ay, az = (lax.axis_index(name) for name in AXES)
    me = ax * p.nz + az
    pending = []

    def mate(r):
        d = lax.rem(me + r, S)
        return d, (lax.div(d, p.nz), ay, lax.rem(d, p.nz))

    def source(r):
        return lax.rem(me + (S - r), S)

    def along(r):
        return (ax, lax.rem(ay + (r % p.ny), p.ny), az)

    def send(src, dst, ssem, rsem, device):
        copy = pltpu.make_async_remote_copy(
            src_ref=src, dst_ref=dst, send_sem=ssem, recv_sem=rsem, device_id=device, device_id_type=MESH
        )
        copy.start()
        pending.append(copy)
        return copy

    barrier = pltpu.get_barrier_semaphore()
    for r in range(1, S):
        pl.semaphore_signal(barrier, inc=1, device_id=mate(r)[1], device_id_type=MESH)
    for r in range(1, p.ny):
        pl.semaphore_signal(barrier, inc=1, device_id=along(r), device_id_type=MESH)

    loads = []
    for x in range(X):
        for y in range(Y):
            n = Z * H * O
            copy = pltpu.make_async_copy(
                rs_hbm.at[x, y], RS.at[pl.ds((y * X + x) * n, n)], in_sem.at[x * Y + y])
            copy.start()
            loads.append(copy)
    small_loads = []
    for n, (src, dst) in enumerate(((onsite_hbm, onsite_ref), (level_hbm, level_ref), (bb_hbm, BB),
                                    (open_hbm, open_ref), (shift_hbm, shift_ref))):
        copy = pltpu.make_async_copy(src, dst, in_sem.at[X * Y + n])
        copy.start()
        small_loads.append(copy)

    lane = lax.broadcasted_iota(jnp.int32, (1, L), 1)
    lane128 = lax.broadcasted_iota(jnp.int32, (1, LANES), 1)

    def roll(v, by):
        by = by % v.shape[1]
        return v if by == 0 else pltpu.roll(v, by, 1)

    zg = ((lane // l) & (p.nz - 1)) * Z + (lane & (Z - 1))
    xg = (lane // (l * p.nz)) * X + ((lane // Z) & (X - 1))
    row_of = lax.broadcasted_iota(jnp.int32, (L, L), 0)

    def place(sx, sz):
        n = (sx + 1) * 3 + sz + 1
        return n - (n > 4)

    def make_shifts():
        for sx in (-1, 0, 1):
            for sz in (-1, 0, 1):
                if (sx, sz) == (0, 0):
                    continue
                x_to, z_to = (xg + sx) & (p.nx * X - 1), (zg + sz) & (p.nz * Z - 1)
                from_lane = ((x_to // X) * p.nz + z_to // Z) * l + (x_to & (X - 1)) * Z + (z_to & (Z - 1))
                matrix = jnp.where(row_of == from_lane, 1.0, 0.0).astype(jnp.bfloat16)
                at = place(sx, sz) * L
                PM[0:L, at:at + L] = matrix
                PM[L:2 * L, at:at + L] = matrix

    def halves(v):
        high = v.astype(jnp.bfloat16)
        low = (v - high.astype(f32)).astype(jnp.bfloat16)
        return jnp.concatenate([high, low], axis=1)

    block_of = lane128 // l

    def butterfly(arrays):
        arrays = list(arrays)
        m = 1
        while m < G:
            low = (block_of & m) == 0
            for a in range(G):
                if a & m == 0:
                    b = a | m
                    first, second = arrays[a], arrays[b]
                    arrays[a] = jnp.where(low, first, roll(second, m * l))
                    arrays[b] = jnp.where(low, roll(first, -m * l), second)
            m *= 2
        return arrays

    for copy in loads:
        copy.wait()
    step = H * O
    order = list(range(1, Y - 1)) + [0, Y - 1]

    def group(n):
        return order[n // O], n % O

    for h in range(H):
        rows = jnp.concatenate([
            RS[pl.ds(y * X * Z * step + h * O + o, l, stride=step), :] for y in order for o in range(O)
        ], axis=0)
        T[h * LANES:(h + 1) * LANES, :] = jnp.transpose(rows)
    BT[0] = RS[...]
    make_shifts()
    pl.semaphore_wait(barrier, S - 1 + p.ny - 1)
    field_copies = []
    for r in range(1, S):
        d, device = mate(r)
        field_copies.append(send(
            T.at[pl.ds(pl.multiple_of(d * Cw, ROWS), Cw)], RB.at[me], a_s.at[r - 1], a_r.at[r - 1], device))
    RB[me] = T[pl.ds(pl.multiple_of(me * Cw, ROWS), Cw), :]

    def spread_z(block):
        n = block.shape[0]
        out = jnp.zeros((n, LANES), f32)
        for z in range(Z):
            out = jnp.where((lane128 & (Z - 1)) == z, block[:, z:z + 1], out)
        row = lax.broadcasted_iota(jnp.int32, (n, LANES), 0)
        col = lax.broadcasted_iota(jnp.int32, (n, LANES), 1)
        x_row, y_row = (row // Y) & (X - 1), row & (Y - 1)
        x_col, y_col = (col // Z) & (X - 1), (col // l) & (Y - 1)
        return jnp.where((x_row == x_col) & (y_row == y_col), out, 0.0)

    for copy in small_loads[0:2]:
        copy.wait()
    onsite = spread_z(onsite_ref[...])
    level = spread_z(level_ref[...])
    XY = X * Y
    pair = [jnp.sum(onsite[n * XY:(n + 1) * XY], axis=0, keepdims=True) for n in range(O * O)]
    diagonal = [jnp.sum(level[n * XY:(n + 1) * XY], axis=0, keepdims=True) for n in range(O)]
    j_low = lane128 // (Y * l)
    diagonal_sum = jnp.zeros((1, LANES), f32)
    for i in range(O):
        for jh in range(O // p.JT):
            line = jnp.zeros((1, LANES), f32)
            for jl in range(p.JT):
                j = jh * p.JT + jl
                term = 0.5 * (pair[i * O + j] + pair[j * O + i])
                if i == j:
                    term = term + diagonal[i]
                    diagonal_sum = diagonal_sum + jnp.where(j_low == 0, term, 0.0)
                line = jnp.where(j_low == jl, term, line)
            row = NB * ROWS + i * (O // p.JT) + jh
            CS[row:row + 1, :] = line

    diagonal_sum = jnp.sum(diagonal_sum, axis=1, keepdims=True)
    for copy in small_loads[2:]:
        copy.wait()
    is_open = open_ref[...].astype(f32)
    is_open = jnp.concatenate([is_open] * p.JT, axis=0)
    x_of, y_of = (lane128 // (Y * Z)) & (X - 1), (lane128 // Z) & (Y - 1)
    x_to, y_to = (lane128 // Z) & (X - 1), (lane128 // (X * Z)) & (Y - 1)
    source_lane = (lane128 & (Z - 1)) + x_to * (Y * Z) + y_to * Z + j_low * (Y * l)
    gaps = sorted({(x * Y * Z + y * Z) - (y * X * Z + x * Z) for x in range(X) for y in range(Y)})
    for t in range(p.tiles):
        block = BB[t * LANES:(t + 1) * LANES, :] * is_open
        block = jnp.concatenate([block, jnp.zeros((LANES, LANES - NB), f32)], axis=1)
        block = jnp.transpose(block)[0:2 * ROWS, :]
        out = block
        for gap in gaps:
            if gap:
                out = jnp.where(source_lane - lane128 == gap, roll(block, -gap), out)
        CS[pl.ds(t, NB, stride=ROWS), :] = out[0:NB, :]
    early_halo = []
    for n, (run, way) in enumerate([(run, 1) for run in ahead_runs] + [(run, -1) for run in behind_runs]):
        early_halo.append(send(
            CS.at[pl.ds(run[0] * ROWS, run[1] * ROWS)], ZC.at[n], hm_s.at[n], hm_r.at[n], along(way)))
    TG[ay] = jnp.broadcast_to(diagonal_sum, (ROWS, LANES))
    early_halo += [
        send(TG.at[ay], TG.at[ay], th_s.at[r - 1], th_r.at[r - 1], along(r)) for r in range(1, p.ny)]
    partner = (ax + 1 - 2 * lax.rem(ax, 2), ay, az)
    even = [(dx, dz) for dz in range(p.nz) for dx in range(0, p.nx, 2) if (dx, dz) != (0, 0)]
    coef_copies = []
    for n, (dx, dz) in enumerate(even):
        device = (lax.rem(ax + dx, p.nx), ay, lax.rem(az + dz, p.nz))
        coef_copies.append(send(CS, CR.at[me], c_s.at[n], c_r.at[n], device))
    relays = [send(CS, CR.at[me], c_s.at[len(even)], c_r.at[len(even)], partner)]
    CR[me] = CS[...]

    def halo_field(m, g):
        return [
            send(V.at[m, 1, g], V.at[m, Y + 1, g], hv_s.at[m, g, 0], hv_r.at[m, g, 0], along(-1)),
            send(V.at[m, Y, g], V.at[m, 0, g], hv_s.at[m, g, 1], hv_r.at[m, g, 1], along(1)),
        ]

    def arrived(copies):
        for copy in copies:
            copy.wait_recv()

    def spread_field(m, slots, g):
        rows = len(slots) * OC
        for n, slot in enumerate(slots):
            LH[g, n * OC:(n + 1) * OC, :] = halves(V[m, slot, g])
        for n in range(0, 8, 2):
            at = slice(n * L, (n + 2) * L)
            moved = jnp.dot(LH[g, 0:rows, :], PM[:, at], preferred_element_type=f32)
            for q, slot in enumerate(slots):
                VS[slot, g, :, at] = moved[q * OC:(q + 1) * OC]

    arrived(field_copies)
    for t in range(p.HT):
        for first in range(0, S, G):
            blocks = butterfly([RB[first + n, :, t * LANES:(t + 1) * LANES] for n in range(G)])
            at = first // G * LANES
            for n in range(G):
                y, o = group(t * G + n)
                for g in range(NG):
                    V[0, y + 1, g, o * Cg:(o + 1) * Cg, at:at + LANES] = blocks[n][g * Cg:(g + 1) * Cg]
    halo = [halo_field(0, g) for g in range(NG)]

    arrived(early_halo)
    outer = [(n, q, run[0] + q, slot, y) for n, (run, slot, y) in enumerate(
        [(run, 0, Y - 1) for run in ahead_runs] + [(run, Y + 1, 0) for run in behind_runs]) for q in range(run[1])]
    unit = p.JT * l
    U = LANES // unit
    for v in range(0, len(outer), U):
        packed = jnp.zeros((ROWS, LANES), f32)
        for q, (n, at, k, slot, y) in enumerate(outer[v:v + U]):
            block = ZC[n, at * ROWS:(at + 1) * ROWS, :]
            for jl in range(p.JT):
                to = q * unit + jl * l
                packed = jnp.where(block_of == to // l, roll(block, to - jl * Y * l - y * l), packed)
        HS[v // U * ROWS:(v // U + 1) * ROWS, :] = packed
    part = TG[0]
    for n in range(1, p.ny):
        part = part + TG[n]
    HS[p.HR - ROWS:p.HR, :] = part
    outer_copies = []
    for r in range(1, S):
        d, device = mate(r)
        outer_copies.append(send(HS, HC.at[me], ho_s.at[r - 1], ho_r.at[r - 1], device))
    HC[me] = HS[...]
    for g in range(NG):
        spread_field(0, range(1, Y + 1), g)

    def take_outer():
        arrived(outer_copies)
        for first in range(0, S, G):
            blocks = butterfly([HC[first + n, 0:p.HR - ROWS, :] for n in range(G)])
            at = first // G * LANES
            for n, (_, _, k, slot, y) in enumerate(outer):
                v, q = divmod(n, U)
                for jl in range(p.JT):
                    M[jl, slot, k * ROWS:(k + 1) * ROWS, at:at + LANES] = (
                        blocks[q * p.JT + jl][v * ROWS:(v + 1) * ROWS])
        mirror(False)
        total = HC[0, p.HR - ROWS:p.HR - ROWS + 1, 0:1]
        for n in range(1, S):
            total = total + HC[n, p.HR - ROWS:p.HR - ROWS + 1, 0:1]
        return total * (1.0 / (p.ny * Y * L * O))

    for n, (dx, dz) in enumerate(even):
        coef_copies[n].wait_recv()
        s = lax.rem(ax + (p.nx - dx), p.nx) * p.nz + lax.rem(az + (p.nz - dz), p.nz)
        at = len(even) + 1 + n
        relays.append(send(CR.at[s], CR.at[s], c_s.at[at], c_r.at[at], partner))
    arrived(relays)
    for first in range(0, S, G):
        blocks = butterfly([CR[first + n] for n in range(G)])
        at = first // G * LANES
        for n in range(G):
            jl, y = divmod(n, Y)
            M[jl, y + 1, :, at:at + LANES] = blocks[n]
    HALFJ = O // p.JT

    def inside(y):
        return 0 <= y < Y

    def mirror(within):
        groups = {}
        for k, o in enumerate(bonds):
            for y in range(Y):
                if inside(y - o[1]) == within:
                    groups.setdefault((-o[0], -o[2]), []).extend((k, jl, y) for jl in range(p.JT))
        for (sx, sz), members in groups.items():
            blocks = [M[jl, y + 1 - bonds[k][1], k * ROWS:(k + 1) * ROWS, :] for k, jl, y in members]
            if (sx, sz) != (0, 0):
                at = place(sx, sz) * L
                moved = jnp.dot(halves(jnp.concatenate(blocks, axis=0)), PM[:, at:at + L], preferred_element_type=f32)
                blocks = [moved[n * ROWS:(n + 1) * ROWS] for n in range(len(members))]
            for (k, jl, y), block in zip(members, blocks):
                MB[k, jl, y] = block

    mirror(True)

    def add_bonds(acc, m, y, steps, g):
        for k, o in enumerate(bonds):
            for sign in (1, -1):
                if sign * o[1] not in steps:
                    continue
                slot = y + 1 + sign * o[1]
                sx, sz = sign * o[0], sign * o[2]
                for j in range(O):
                    rows = slice(j * Cg, (j + 1) * Cg)
                    at = place(sx, sz) * L
                    v = V[m, slot, g, rows, :] if (sx, sz) == (0, 0) else VS[slot, g, rows, at:at + L]
                    for i in range(O):
                        if sign > 0:
                            row = k * ROWS + i * HALFJ + j // p.JT
                            c = M[j % p.JT, y + 1, row:row + 1, :]
                        else:
                            row = j * HALFJ + i // p.JT
                            c = MB[k, i % p.JT, y, row:row + 1, :]
                        acc[i] = acc[i] + c * v

    def add_onsite(acc, m, y, theta, g):
        for j in range(O):
            v = V[m, y + 1, g, j * Cg:(j + 1) * Cg, :]
            for i in range(O):
                row = NB * ROWS + i * HALFJ + j // p.JT
                c = M[j % p.JT, y + 1, row:row + 1, :]
                if i == j:
                    c = c - theta
                acc[i] = acc[i] + c * v

    def put(acc, m, y, g):
        for i in range(O):
            V[m, y + 1, g, i * Cg:(i + 1) * Cg, :] = acc[i]

    def take(m, y, g):
        return [V[m, y + 1, g, i * Cg:(i + 1) * Cg, :] for i in range(O)]

    def zeros():
        return [jnp.zeros((Cg, L), f32) for _ in range(O)]

    def moment(a, b):
        sums = []
        for g in range(NG):
            total = jnp.zeros((Cg, L), f32)
            for y in range(Y):
                for i in range(O):
                    rows = slice(i * Cg, (i + 1) * Cg)
                    total = total + V[a, y + 1, g, rows, :] * V[b, y + 1, g, rows, :]
            sums.append(jnp.sum(total, axis=1, keepdims=True))
        return jnp.concatenate(sums, axis=0)

    nils = [lax.div(ax, p.nx), lax.div(ay, p.ny), lax.div(az, p.nz), lax.div(me, S)]
    moments = []
    home_copies = {}

    everyone = [(g, r) for g in range(p.ny) for r in range(S) if (g, r) != (0, 0)]

    def tell(part, values):
        sublane = lax.broadcasted_iota(jnp.int32, (Cw, LANES), 0)
        spot = lax.broadcasted_iota(jnp.int32, (Cw, LANES), 1)
        table = jnp.zeros((Cw, LANES), f32)
        for n, value in enumerate(values):
            table = jnp.where(spot == sublane + n * Cw, value, table)
        line = jnp.sum(table, axis=0, keepdims=True)
        EM[part, ay, me] = line
        SR[part] = line
        copies = []
        for n, (g, r) in enumerate(everyone):
            d = lax.rem(me + r, S)
            device = (lax.div(d, p.nz), lax.rem(ay + g, p.ny), lax.rem(d, p.nz))
            copies.append(send(SR.at[part], EM.at[part, ay, me], e_s.at[part, n], e_r.at[part, n], device))
        return copies

    def go_home(m, tiles):
        for t in tiles:
            for first in range(0, S, G):
                at = first // G * LANES
                blocks = []
                for n in range(G):
                    y, o = group(t * G + n)
                    blocks.append(jnp.concatenate(
                        [V[m, y + 1, g, o * Cg:(o + 1) * Cg, at:at + LANES] for g in range(NG)], axis=0))
                blocks = butterfly(blocks)
                for n in range(G):
                    SB[m - 1, t, first + n] = blocks[n]
        mine = pl.ds(pl.multiple_of(me * Cw, ROWS), Cw)
        copies = home_copies.setdefault(m, [])
        at, n = tiles[0], len(tiles)
        for r in range(1, S):
            d, device = mate(r)
            copies.append(send(SB.at[m - 1, pl.ds(at, n), d], YB.at[m - 1, pl.ds(at, n), mine],
                               y_s.at[m - 1, at, r - 1], y_r.at[m - 1, at, r - 1], device))
        for t in tiles:
            YB[m - 1, t, mine] = SB[m - 1, t, me]

    theta = None
    for m in range(ITERS):
        last = m + 1 == ITERS
        if m > 0:
            for g in range(NG):
                spread_field(m, range(1, Y + 1), g)

        def interior(y, steps, g):
            acc = zeros()
            if m > 0 and len(steps) == 3:
                add_onsite(acc, m, y, theta, g)
            add_bonds(acc, m, y, steps, g)
            put(acc, m + 1, y, g)

        for g in range(NG):
            for y in range(Y):
                interior(y, [n for n in (-1, 0, 1) if inside(y + n)], g + nils[y])
        if m == 0:
            moments.append(moment(0, 0))
            theta = take_outer()
            for g in range(NG):
                for y in range(1, Y - 1):
                    acc = take(m + 1, y, g)
                    add_onsite(acc, m, y, theta, g)
                    put(acc, m + 1, y, g)
        if last:
            go_home(ITERS, [0])
            early = len(moments) - 1
            told = tell(0, moments[:early])
        for g in range(NG):
            arrived(halo[g])
            spread_field(m, (0, Y + 1), g)
            for y, s in ((0, -1), (Y - 1, 1)):
                acc = take(m + 1, y, g)
                add_bonds(acc, m, y, [s], g)
                add_onsite(acc, m, y, theta, g)
                put(acc, m + 1, y, g)
            if not last:
                halo[g] = halo_field(m + 1, g)
        if not last:
            go_home(m + 1, list(range(p.HT)))
        moments.append(moment(m, m + 1))
        if not last:
            moments.append(moment(m + 1, m + 1))
    told = told + tell(1, moments[early:])
    go_home(ITERS, list(range(1, p.HT)))

    shift = jnp.concatenate([
        roll(shift_ref[:, d * Cw // LANES * LANES:(d * Cw // LANES + 1) * LANES], -(d * Cw % LANES)) for d in range(S)
    ], axis=0) + theta

    def turn_home(n):
        arrived(home_copies[n + 1])
        for h in range(H):
            for t in range(p.HT):
                field = jnp.transpose(YB[n, t, h * LANES:(h + 1) * LANES, :])
                for q in range(G):
                    y, o = group(t * G + q)
                    BT[n + 1, pl.ds(y * X * Z * step + h * O + o, l, stride=step), :] = field[q * l:(q + 1) * l, :]

    for n in range(ITERS):
        turn_home(n)
    arrived(told)

    def total(part):
        rows = []
        for d in range(S):
            line = EM[part, 0, d]
            for n in range(1, p.ny):
                line = line + EM[part, n, d]
            rows.append(line)
        return jnp.concatenate(rows, axis=0)

    sums = [total(0), total(1)]
    m_of = [roll(sums[n >= early], -(n - early * (n >= early)) * Cw) for n in range(2 * ITERS)]

    def inner(u, v):
        out = None
        for a, first in enumerate(u):
            for b, second in enumerate(v):
                term = first * second * m_of[a + b]
                out = term if out is None else out + term
        return out

    def plus(u, v, factor):
        n = max(len(u), len(v))
        out = []
        for a in range(n):
            if a < len(v):
                term = factor * v[a]
                out.append(u[a] + term if a < len(u) else term)
            else:
                out.append(u[a])
        return out

    one = jnp.ones((S, LANES), f32)
    answer, residual, direction, norm = [], [one], [one], m_of[0]
    for turn in range(ITERS):
        image = [shift * direction[0]]
        for a in range(1, len(direction)):
            image.append(direction[a - 1] + shift * direction[a])
        image.append(direction[-1])
        alpha = norm / inner(direction, image)
        answer = plus(answer, direction, alpha)
        residual = plus(residual, image, -alpha)
        if turn + 1 < ITERS:
            fresh = inner(residual, residual)
            direction = plus(residual, direction, fresh / norm)
            norm = fresh
    factors = answer + residual
    per = LANES // Cw
    half = lax.broadcasted_iota(jnp.int32, (H * O, LANES), 0) // O
    for n, factor in enumerate(factors):
        turned = [roll(factor, q * Cw) for q in range(per)]
        block = jnp.zeros((H * O, LANES), f32)
        for h in range(H):
            line = turned[0][h * per:h * per + 1]
            for q in range(1, per):
                line = jnp.where(lane128 // Cw == q, turned[q][h * per + q:h * per + q + 1], line)
            block = jnp.where(half == h, line, block)
        FX[n] = block
    for copy in pending:
        copy.wait_send()


def combine(plan, BT, FX, sol_hbm, res_hbm, OS, sem):
    p = plan
    X, Y, n = p.X, p.Y, p.Z * p.H * p.O
    group = p.H * p.O
    outs = []
    for which, hbm in ((0, sol_hbm), (1, res_hbm)):
        for y in range(Y):
            for x in range(X):
                base = (y * X + x) * n
                for at in range(base, base + n, group):
                    rows = slice(at, at + group)
                    field = FX[which * ITERS] * BT[0, rows, :]
                    for q in range(1, ITERS + which):
                        field = field + FX[which * ITERS + q] * BT[q, rows, :]
                    OS[which, rows, :] = field
        for x in range(X):
            for y in range(Y):
                copy = pltpu.make_async_copy(
                    OS.at[which, pl.ds((y * X + x) * n, n)], hbm.at[x, y], sem.at[(which * X + x) * Y + y])
                copy.start()
                outs.append(copy)
    for copy in outs:
        copy.wait()


def per_device(peers, right_side, bond_blocks, bond_open, onsite_blocks, orbital_levels, column_shift):
    block, orb, cols = right_side.shape[:3], right_side.shape[3], right_side.shape[4]
    p = Plan(block, orb, cols, peers)
    X, Y, Z, O, S, L, H = p.X, p.Y, p.Z, p.O, p.S, p.L, p.H
    f32 = jnp.float32
    right = right_side.reshape(X, Y, Z, O, H, LANES).transpose(0, 1, 2, 4, 3, 5).reshape(X, Y, Z * H * O, LANES)
    blocks = jnp.transpose(bond_blocks, (1, 2, 3, 4, 5, 0)).reshape(O * O * X * Y * Z, NB)
    opened = jnp.transpose(bond_open, (1, 2, 3, 0)).reshape(X * Y * Z, NB)
    onsite = onsite_blocks.reshape(O * O * X * Y, Z)
    levels = orbital_levels.reshape(O * X * Y, Z)
    dma = pltpu.SemaphoreType.DMA
    vmem, anywhere = pl.BlockSpec(memory_space=pltpu.VMEM), pl.BlockSpec(memory_space=pl.ANY)

    def scratch(*shape):
        return pltpu.VMEM(shape, f32)

    flat = (p.cols, p.HL)
    made = pl.pallas_call(
        functools.partial(kernel, p),
        out_shape=(scratch(ITERS + 1, X * Y * Z * H * O, LANES), scratch(2 * ITERS + 1, H * O, LANES)),
        in_specs=[pl.BlockSpec(memory_space=pltpu.HBM)] * 6,
        out_specs=(vmem,) * 2,
        scratch_shapes=[
            scratch(X * Y * Z * H * O, LANES),
            scratch(O * O * X * Y * Z, NB),
            pltpu.VMEM(opened.shape, jnp.int32),
            scratch(*onsite.shape),
            scratch(*levels.shape),
            scratch(1, cols),
            pltpu.VMEM((2 * L, 8 * L), jnp.bfloat16),
            pltpu.VMEM((p.NG, Y * p.OC, 2 * L), jnp.bfloat16),
            scratch(*flat),
            scratch(ITERS, p.HT, cols, LANES),
            scratch(3, 3 * ROWS, LANES),
            scratch(p.HR, LANES),
            scratch(S, p.HR, LANES),
            scratch(S, p.Cw, p.HL),
            scratch(p.CR, LANES),
            scratch(S, p.CR, LANES),
            scratch(p.JT, Y + 2, p.CR, L),
            scratch(NB, p.JT, Y, ROWS, L),
            scratch(ITERS + 1, Y + 2, p.NG, p.OC, L),
            scratch(Y + 2, p.NG, p.OC, 8 * L),
            scratch(ITERS, p.HT, S, p.Cw, LANES),
            scratch(2, p.ny, S, 1, LANES),
            scratch(2, 1, LANES),
            scratch(p.ny, ROWS, LANES),
            dma((X * Y + 5,)),
            dma((S - 1,)), dma((S - 1,)), dma((S - 1,)), dma((S - 1,)),
            dma((ITERS, p.NG, 2)), dma((ITERS, p.NG, 2)), dma((3,)), dma((3,)),
            dma((S - 1,)), dma((S - 1,)),
            dma((p.ny - 1,)), dma((p.ny - 1,)),
            dma((ITERS, p.HT, S - 1)), dma((ITERS, p.HT, S - 1)),
            dma((2, p.ny * S - 1)), dma((2, p.ny * S - 1)),
        ],
        compiler_params=pltpu.CompilerParams(
            collective_id=0, has_side_effects=True, vmem_limit_bytes=40 * 1024 * 1024
        ),
    )(*(pltpu.with_memory_space_constraint(v, pltpu.HBM)
        for v in (right, blocks, opened, onsite, levels, column_shift[None])))
    outs = pl.pallas_call(
        functools.partial(combine, p),
        out_shape=(jax.ShapeDtypeStruct(right.shape, f32),) * 2,
        in_specs=[vmem] * 2,
        out_specs=(anywhere, anywhere),
        scratch_shapes=[scratch(2, X * Y * Z * H * O, LANES), dma((2 * X * Y,))],
        compiler_params=pltpu.CompilerParams(vmem_limit_bytes=16 * 1024 * 1024),
    )(*made)

    def back(v):
        return v.reshape(X, Y, Z, H, O, LANES).transpose(0, 1, 2, 4, 3, 5).reshape(right_side.shape)

    return back(outs[0]), back(outs[1])


def solution(mesh):
    field = P("gx", "gy", "gz", None, None)
    placed = (
        field,
        P(None, None, None, "gx", "gy", "gz"),
        P(None, "gx", "gy", "gz"),
        P(None, None, "gx", "gy", "gz"),
        P(None, "gx", "gy", "gz"),
        P(),
    )
    return jax.shard_map(
        functools.partial(per_device, tuple(mesh.shape[name] for name in AXES)),
        mesh=mesh,
        in_specs=placed,
        out_specs=(field, field),
        check_vma=False,
    )
```
